32 devices in a mesh: dp: 16 (over z, y, x), seq: 2 (over core).
Axes of the slice: x: 2, y: 2, z: 4, core: 2. Of those that a mesh axis runs over, the one named last changes fastest.
Arguments:
- chains_in: bfloat16 [128, 160, 768], P(('dp', 'seq')), may hold values from -6 to 6
- lengths: int32 [128], P(('dp', 'seq')), may hold values from 95 to 160
- d_out: bfloat16 [128, 160, 768], P(('dp', 'seq')), may hold values from -6 to 6
- w_query: bfloat16 [768, 768], replicated, may hold values from -0.21875 to 0.21875
- b_query: float32 [768], replicated, may hold values from -3 to 3
- w_key: bfloat16 [768, 768], replicated, may hold values from -0.21875 to 0.21875
- w_value: bfloat16 [768, 768], replicated, may hold values from -0.21875 to 0.21875
- b_value: float32 [768], replicated, may hold values from -3 to 3
- w_output: bfloat16 [768, 768], replicated, may hold values from -2.5 to 2.5
- b_output: float32 [768], replicated, may hold values from -3 to 3
- gain_one: float32 [768], replicated, may hold values from 0.25 to 1.75
- shift_one: float32 [768], replicated, may hold values from -2 to 2
- w_inner: bfloat16 [768, 3072], replicated, may hold values from -0.21875 to 0.21875
- b_inner: float32 [3072], replicated, may hold values from -3 to 3
- w_outer: bfloat16 [3072, 768], replicated, may hold values from -0.109375 to 0.109375
- b_outer: float32 [768], replicated, may hold values from -3 to 3
- gain_two: float32 [768], replicated, may hold values from 0.25 to 1.75
- shift_two: float32 [768], replicated, may hold values from -2 to 2
Outputs:
- layer_out: bfloat16 [128, 160, 768], P(('dp', 'seq'))
- d_x: float32 [128, 160, 768], P(('dp', 'seq'))
- d_w_query: float32 [768, 768], replicated
- d_b_query: float32 [768], replicated
- d_w_key: float32 [768, 768], replicated
- d_w_value: float32 [768, 768], replicated
- d_b_value: float32 [768], replicated
- d_w_output: float32 [768, 768], replicated
- d_b_output: float32 [768], replicated
- d_gain_one: float32 [768], replicated
- d_shift_one: float32 [768], replicated
- d_w_inner: float32 [768, 3072], replicated
- d_b_inner: float32 [3072], replicated
- d_w_outer: float32 [3072, 768], replicated
- d_b_outer: float32 [768], replicated
- d_gain_two: float32 [768], replicated
- d_shift_two: float32 [768], replicated
The draws below stay inside these ranges and needn't reach their ends.
Inputs may be any that keep to these rules, and one draw needn't show every extreme that they name: `lengths`: every chain fills more than half of its 160 positions.
All inputs are finite; a program needn't handle non-finite values.
Results may differ from the reference program's by a relative error of at most 0.015.
Values may be sent and summed in bfloat16 or wider, within the bound.
No kernel may reach another device: no remote copies, remote signals or barrier semaphores. Data moves between devices by JAX's collectives and lax.ppermute only.
A program may use at most 256 MiB of HBM per device.

```python
import jax
import jax.numpy as jnp
from jax import lax

D = 768
H = 12
FF = 3072
LMAX = 160
SEQ_DEV = 4
SEQS = 128


def touch_ends(drawn, stream_key, least, high):
    longest = drawn.shape.index(max(drawn.shape))
    spots = []
    for shift in (0, 1):
        where = [jax.random.randint(jax.random.fold_in(stream_key, axis), (), 0, length) for axis, length in enumerate(drawn.shape)]
        where[longest] = (where[longest] + shift) % drawn.shape[longest]
        spots.append(tuple(where))
    return drawn.at[spots[0]].set(least).at[spots[1]].set(high)


def steps_of(rng, dims, pieces, smallest, high):
    level = 1.0
    for dim, blocks in pieces:
        heights = jax.random.uniform(jax.random.fold_in(jax.random.fold_in(rng, 6), dim), (blocks,), jnp.float32, smallest / len(pieces), high / len(pieces))
        level = level * jnp.repeat(jnp.exp(heights), dims[dim] // blocks).reshape((-1,) + (1,) * (len(dims) - 1 - dim))
    return level


def centred(own_key, extent, scale, limit, cuts=(), held_as=jnp.bfloat16):
    values = jax.random.normal(own_key, extent, jnp.float32) * scale
    if len(cuts) > 0:
        values = steps_of(own_key, extent, cuts, -0.22, 0.18) * values
    return jnp.clip(values, min=-limit, max=limit).astype(held_as)


def setup_inputs(seed: int = 0) -> dict:
    splits = jax.random.split(jax.random.key(seed), 19)
    chains_in = centred(splits[0], (SEQS, LMAX, D), 1.0, 6.0, ((0, 32),))
    lengths = touch_ends(jax.random.randint(splits[1], (SEQS,), 95, LMAX + 1), jax.random.fold_in(splits[1], 1), 95, LMAX).astype(jnp.int32)
    d_out = centred(splits[2], (SEQS, LMAX, D), 1.0, 6.0, ((0, 32),))
    w_query = centred(splits[3], (D, D), D ** -0.5, 0.21875)
    b_query = centred(splits[4], (D,), 0.5, 3.0, (), jnp.float32)
    w_key = centred(splits[5], (D, D), D ** -0.5, 0.21875)
    w_value = centred(splits[6], (D, D), D ** -0.5, 0.21875)
    b_value = centred(splits[7], (D,), 0.5, 3.0, (), jnp.float32)
    w_output = centred(splits[8], (D, D), (max(D // 128, 1)) ** -0.5, 2.5)
    b_output = centred(splits[9], (D,), 0.5, 3.0, (), jnp.float32)
    gain_one = jnp.clip(1.0 + 0.15 * jax.random.normal(splits[10], (D,), jnp.float32), 0.25, 1.75)
    shift_one = centred(splits[11], (D,), 0.3, 2.0, (), jnp.float32)
    w_inner = centred(splits[12], (D, FF), D ** -0.5, 0.21875)
    b_inner = centred(splits[13], (FF,), 0.5, 3.0, (), jnp.float32)
    w_outer = centred(splits[14], (FF, D), FF ** -0.5, 0.109375)
    b_outer = centred(splits[15], (D,), 0.5, 3.0, (), jnp.float32)
    gain_two = jnp.clip(1.0 + 0.15 * jax.random.normal(splits[16], (D,), jnp.float32), 0.25, 1.75)
    shift_two = centred(splits[17], (D,), 0.3, 2.0, (), jnp.float32)
    return {"chains_in": chains_in, "lengths": lengths, "d_out": d_out, "w_query": w_query, "b_query": b_query, "w_key": w_key, "w_value": w_value, "b_value": b_value, "w_output": w_output, "b_output": b_output, "gain_one": gain_one, "shift_one": shift_one, "w_inner": w_inner, "b_inner": b_inner, "w_outer": w_outer, "b_outer": b_outer, "gain_two": gain_two, "shift_two": shift_two}


@jax.custom_vjp
def low(v):
    return lax.optimization_barrier(v.astype(jnp.bfloat16)).astype(jnp.float32)

@jax.custom_vjp
def low_back(v):
    return v

def low_keep(v):
    return (low(v), None)

def low_pass(kept, grad):
    return (grad,)

def back_keep(v):
    return (v, None)

def back_low(kept, grad):
    return (low(grad),)
low.defvjp(low_keep, low_pass)
low_back.defvjp(back_keep, back_low)
EPS = 1e-12
HIGH = lax.Precision.HIGHEST

def normed(h, gain, shift):
    centre = h - lax.optimization_barrier(jnp.mean(h, -1, keepdims=True))
    scale = lax.rsqrt(lax.optimization_barrier(jnp.mean(centre * centre, -1, keepdims=True)) + EPS)
    return centre * scale * gain + shift

def layer(params, chains, lens):
    w_query, b_query, w_key, w_value, b_value, w_output, b_output, gain_one, shift_one, w_inner, b_inner, w_outer, b_outer, gain_two, shift_two = params
    group, length, width = chains.shape
    size = width // H
    place = jnp.arange(length, dtype=jnp.int32)
    live = place[None, :] < lens[:, None]
    flat = chains.reshape(group * length, width)
    query = low_back(low(jnp.dot(flat, w_query, precision=HIGH) + b_query)).reshape(group, length, H, size)
    keys = low_back(low(jnp.dot(flat, w_key, precision=HIGH))).reshape(group, length, H, size)
    values = low_back(low(jnp.dot(flat, w_value, precision=HIGH) + b_value)).reshape(group, length, H, size)
    scores = jnp.einsum('bqhe,bkhe->bhqk', query, keys, precision=HIGH) * 0.125
    scores = low_back(jnp.where(live[:, None, None, :], scores, -1000000000.0))
    prob = low(jax.nn.softmax(scores, axis=-1))
    mixed = jnp.einsum('bhqk,bkhe->bqhe', prob, values, precision=HIGH).reshape(group * length, width)
    mixed = low_back(low(mixed))
    attn = low_back(jnp.dot(mixed, w_output, precision=HIGH) + b_output)
    first = normed(flat + attn, gain_one, shift_one)
    fin = low_back(low(first))
    pre = low_back(jnp.dot(fin, w_inner, precision=HIGH) + b_inner)
    hidden = low(jax.nn.gelu(pre, approximate=False))
    ffn = low_back(low(jnp.dot(hidden, w_outer, precision=HIGH) + b_outer))
    out = normed(first + ffn, gain_two, shift_two) * live.reshape(-1, 1).astype(jnp.float32)
    return out.reshape(group, length, width)

def reference(chains_in, lengths, d_out, w_query, b_query, w_key, w_value, b_value, w_output, b_output, gain_one, shift_one, w_inner, b_inner, w_outer, b_outer, gain_two, shift_two):
    params = tuple((p.astype(jnp.float32) for p in (w_query, b_query, w_key, w_value, b_value, w_output, b_output, gain_one, shift_one, w_inner, b_inner, w_outer, b_outer, gain_two, shift_two)))
    groups = chains_in.shape[0] // SEQ_DEV
    chains = chains_in.astype(jnp.float32).reshape(groups, SEQ_DEV, LMAX, D)
    lens = lengths.astype(jnp.int32).reshape(groups, SEQ_DEV)
    cots = d_out.astype(jnp.float32).reshape(groups, SEQ_DEV, LMAX, D)

    def step(totals, item):
        block, block_lens, block_cot = item
        result, pull = jax.vjp(lambda pp, xx: layer(pp, xx, block_lens), params, block)
        grads, grad_in = pull(block_cot)
        return (tuple((a + g for a, g in zip(totals, grads))), (result.astype(jnp.bfloat16), grad_in))
    zeros = tuple((jnp.zeros(p.shape, jnp.float32) for p in params))
    totals, (outs, grads_in) = lax.scan(step, zeros, (chains, lens, cots))
    return (outs.reshape(chains_in.shape), grads_in.reshape(chains_in.shape), totals[0], totals[1], totals[2], totals[3], totals[4], totals[5], totals[6], totals[7], totals[8], totals[9], totals[10], totals[11], totals[12], totals[13], totals[14])
```

```python
import jax
import jax.numpy as jnp
from jax import lax
from jax.sharding import PartitionSpec as P

H = 12


EPS = 1e-12


def norm_forward(h, gain, shift):
    centre = h - jnp.mean(h, -1, keepdims=True)
    scale = lax.rsqrt(jnp.mean(centre * centre, -1, keepdims=True) + EPS)
    unit = centre * scale
    return (unit * gain + shift, unit, scale)


def norm_backward(grad, unit, scale, gain):
    d_gain = jnp.sum(grad * unit, 0)
    d_shift = jnp.sum(grad, 0)
    inner = grad * gain
    d_h = scale * (
        inner
        - jnp.mean(inner, -1, keepdims=True)
        - unit * jnp.mean(inner * unit, -1, keepdims=True)
    )
    return (d_h, d_gain, d_shift)


def over_rows(left, right):
    return lax.dot_general(
        left, right, (((0,), (0,)), ((), ())), preferred_element_type=jnp.float32
    )


def times_trans(left, weight):
    return lax.dot_general(
        left, weight, (((1,), (1,)), ((), ())), preferred_element_type=jnp.float32
    )


def attn_scores(query, keys, live_keys):
    seqs, count, width = query.shape
    total = keys.shape[1]
    size = width // H
    q_heads = query.reshape(seqs, count, H, size)
    k_heads = keys.reshape(seqs, total, H, size)
    scores = (
        jnp.einsum("bqhe,bkhe->bhqk", q_heads, k_heads, preferred_element_type=jnp.float32) * 0.125
    )
    return jnp.where(live_keys[:, None, None, :], scores, -1000000000.0)


def packed(grads, count):
    flat = jnp.concatenate([g.reshape(-1) for g in grads])
    extra = -flat.shape[0] % count
    return flat.reshape(count, -1)


def unpacked(flat, grads):
    flat = flat.reshape(-1)
    pieces = []
    start = 0
    for grad in grads:
        number = grad.size
        pieces.append(flat[start : start + number].reshape(grad.shape))
        start = start + number
    return tuple(pieces)


def body(
    chains_in,
    lengths,
    d_out,
    w_query,
    b_query,
    w_key,
    w_value,
    b_value,
    w_output,
    b_output,
    gain_one,
    shift_one,
    w_inner,
    b_inner,
    w_outer,
    b_outer,
    gain_two,
    shift_two,
):
    f32 = jnp.float32
    low_type = jnp.bfloat16
    seqs, length, width = chains_in.shape
    rows = seqs * length
    size = width // H
    parts = lax.axis_size("dp")
    count = lax.axis_size("dp") * lax.axis_size("seq")
    place = jnp.arange(length, dtype=jnp.int32)
    live_rows = place[None, :] < lengths[:, None]
    flat_x = chains_in.reshape(rows, width)
    query = (
        (jnp.dot(flat_x, w_query, preferred_element_type=f32) + b_query)
        .astype(low_type)
        .reshape(seqs, length, width)
    )
    keys = (
        jnp.dot(flat_x, w_key, preferred_element_type=f32)
        .astype(low_type)
        .reshape(seqs, length, width)
    )
    values = (
        (jnp.dot(flat_x, w_value, preferred_element_type=f32) + b_value)
        .astype(low_type)
        .reshape(seqs, length, width)
    )
    scores = attn_scores(query, keys, live_rows)
    top = jnp.max(scores, -1, keepdims=True)
    expo = jnp.exp(scores - top)
    summed = jnp.sum(expo, -1, keepdims=True)
    prob_b = (expo / summed).astype(low_type)
    lse = top + jnp.log(summed)
    v_heads = values.reshape(seqs, length, H, size)
    mixed = (
        jnp.einsum("bhqk,bkhe->bqhe", prob_b, v_heads, preferred_element_type=f32)
        .reshape(rows, width)
        .astype(low_type)
    )
    h_one = flat_x.astype(f32) + jnp.dot(mixed, w_output, preferred_element_type=f32) + b_output
    first, unit_one, scale_one = norm_forward(h_one, gain_one, shift_one)
    live_flat = live_rows.reshape(rows)
    fin = first.astype(low_type)
    pre = jnp.dot(fin, w_inner, preferred_element_type=f32) + b_inner
    hidden = jax.nn.gelu(pre, approximate=False).astype(low_type)
    ffn_home = (jnp.dot(hidden, w_outer, preferred_element_type=f32) + b_outer).astype(low_type)
    h_two = first + ffn_home.astype(f32)
    second, unit_two, scale_two = norm_forward(h_two, gain_two, shift_two)
    keep = live_flat[:, None].astype(f32)
    layer_out = (second * keep).astype(low_type).reshape(seqs, length, width)
    grad_out = d_out.reshape(rows, width).astype(f32) * keep
    d_h_two, d_gain_two, d_shift_two = norm_backward(grad_out, unit_two, scale_two, gain_two)
    d_ffn = d_h_two.astype(low_type)
    d_w_outer = over_rows(hidden, d_ffn)
    d_b_outer = jnp.sum(d_ffn.astype(f32), 0)
    d_hidden = times_trans(d_ffn, w_outer)
    gelu_pull = jax.vjp(lambda z: jax.nn.gelu(z, approximate=False), pre)[1]
    d_pre = gelu_pull(d_hidden)[0].astype(low_type)
    d_w_inner = over_rows(fin, d_pre)
    d_b_inner = jnp.sum(d_pre.astype(f32), 0)
    d_fin = times_trans(d_pre, w_inner).astype(low_type)
    d_home = d_fin
    d_first = d_h_two + d_home.astype(f32)
    ffn_grads = (d_w_inner, d_b_inner, d_w_outer, d_b_outer, d_gain_two, d_shift_two)
    d_h_one, d_gain_one, d_shift_one = norm_backward(d_first, unit_one, scale_one, gain_one)
    d_attn = d_h_one.astype(low_type)
    d_w_output = over_rows(mixed, d_attn)
    d_b_output = jnp.sum(d_attn.astype(f32), 0)
    d_mixed = times_trans(d_attn, w_output).astype(low_type).reshape(seqs, length, H, size)
    scores = attn_scores(query, keys, live_rows)
    prob = jnp.exp(scores - lse)
    prob_b = prob.astype(low_type)
    d_prob = jnp.einsum("bqhe,bkhe->bhqk", d_mixed, v_heads, preferred_element_type=f32)
    delta = jnp.sum(prob * d_prob, -1, keepdims=True)
    d_scores = (prob * (d_prob - delta)).astype(low_type)
    k_heads = keys.reshape(seqs, length, H, size)
    q_heads = query.reshape(seqs, length, H, size)
    d_query = (
        (jnp.einsum("bhqk,bkhe->bqhe", d_scores, k_heads, preferred_element_type=f32) * 0.125)
        .astype(low_type)
        .reshape(rows, width)
    )
    d_key = (
        (jnp.einsum("bhqk,bqhe->bkhe", d_scores, q_heads, preferred_element_type=f32) * 0.125)
        .astype(low_type)
        .reshape(rows, width)
    )
    d_value = (
        jnp.einsum("bhqk,bqhe->bkhe", prob_b, d_mixed, preferred_element_type=f32)
        .astype(low_type)
        .reshape(rows, width)
    )
    d_w_query = over_rows(flat_x, d_query)
    d_b_query = jnp.sum(d_query.astype(f32), 0)
    d_w_key = over_rows(flat_x, d_key)
    d_w_value = over_rows(flat_x, d_value)
    d_b_value = jnp.sum(d_value.astype(f32), 0)
    d_x = (
        d_h_one
        + times_trans(d_query, w_query)
        + times_trans(d_key, w_key)
        + times_trans(d_value, w_value)
    )
    d_x = d_x.reshape(seqs, length, width)
    attn_grads = (
        d_w_query,
        d_b_query,
        d_w_key,
        d_w_value,
        d_b_value,
        d_w_output,
        d_b_output,
        d_gain_one,
        d_shift_one,
    )
    local_grads = attn_grads + ffn_grads
    big = [g for g in local_grads if g.ndim == 2]
    small = [g for g in local_grads if g.ndim == 1]
    sums = lax.psum(jnp.concatenate(small), ("dp", "seq"))
    small_sums = unpacked(sums, small)
    big_sums = []
    for grad in big:
        part = lax.psum_scatter(
            grad.astype(low_type), ("dp", "seq"), scatter_dimension=0, tiled=True
        )
        big_sums.append(lax.all_gather(part, ("dp", "seq"), axis=0, tiled=True).astype(f32))
    every = []
    for grad in local_grads:
        every.append(big_sums.pop(0) if grad.ndim == 2 else small_sums[0])
        small_sums = small_sums if grad.ndim == 2 else small_sums[1:]
    return (
        layer_out,
        d_x,
        every[0],
        every[1],
        every[2],
        every[3],
        every[4],
        every[5],
        every[6],
        every[7],
        every[8],
        every[9],
        every[10],
        every[11],
        every[12],
        every[13],
        every[14],
    )


def solution(mesh):
    return jax.shard_map(
        body,
        mesh=mesh,
        in_specs=(
            P(("dp", "seq"), None, None),
            P(("dp", "seq")),
            P(("dp", "seq"), None, None),
            P(),
            P(),
            P(),
            P(),
            P(),
            P(),
            P(),
            P(),
            P(),
            P(),
            P(),
            P(),
            P(),
            P(),
            P(),
        ),
        out_specs=(
            P(("dp", "seq"), None, None),
            P(("dp", "seq"), None, None),
            P(),
            P(),
            P(),
            P(),
            P(),
            P(),
            P(),
            P(),
            P(),
            P(),
            P(),
            P(),
            P(),
            P(),
            P(),
        ),
        check_vma=False,
    )
```

```python
import functools
import jax
import jax.numpy as jnp
from jax import lax
from jax.experimental import pallas as pl
from jax.experimental.pallas import tpu as pltpu
from jax.sharding import PartitionSpec as P
H=12; EPS=1e-12
f32=jnp.float32; bf16=jnp.bfloat16
VM=60*1024*1024
def cp(**k): return pltpu.CompilerParams(vmem_limit_bytes=VM, **k)
def nt(a,b): return lax.dot_general(a,b,(((1,),(1,)),((),())),preferred_element_type=f32)
def tn(a,b): return lax.dot_general(a,b,(((0,),(0,)),((),())),preferred_element_type=f32)
def nn(a,b): return jnp.dot(a,b,preferred_element_type=f32)

def attn_fwd_kernel(lens, x, wq, bq, wk, wv, bv, wo, bo, q_o, k_o, v_o, mixed_o, xhat_o, rstd_o, lse_o, h_s):
    rows, width = x.shape
    seqs = lens.shape[0]
    length = rows // seqs
    size = width // H
    def proj(n, _):
        c = pl.ds(pl.multiple_of(n*256,256),256)
        q_o[:, c] = ((nn(x[...], wq[:, c]) + bq[:, c]).astype(bf16).astype(f32)*0.125).astype(bf16)
        k_o[:, c] = nn(x[...], wk[:, c]).astype(bf16)
        v_o[:, c] = (nn(x[...], wv[:, c]) + bv[:, c]).astype(bf16)
        return 0
    lax.fori_loop(0, width//256, proj, 0)
    lane = lax.broadcasted_iota(jnp.int32, (length,128), 1)
    low = lane < size
    pos = lax.broadcasted_iota(jnp.int32, (length,1), 0)
    def chain(s, _):
        r = pl.ds(pl.multiple_of(s*length, 32), length)
        live = pos < lens[s]
        for p in range(H//2):
            c = slice(128*p,128*p+128)
            qp=q_o[r,c]; kp=k_o[r,c]; vp=v_o[r,c]
            outs=[]
            for h in range(2):
                sel = low if h==0 else ~low
                kh = jnp.where(sel,kp,jnp.zeros_like(kp))
                st = nt(kh,qp)
                st = jnp.where(live, st, -1e9)
                m = jnp.max(st,0,keepdims=True)
                e = jnp.exp(st-m)
                l = jnp.sum(e,0,keepdims=True)
                pt = (e*(1.0/l)).astype(bf16)
                lse_o[s, pl.ds(2*p+h,1), :] = m+jnp.log(l)
                outs.append(tn(pt,vp))
            mixed_o[r,c] = jnp.where(low,outs[0],outs[1]).astype(bf16)
        return 0
    lax.fori_loop(0, seqs, chain, 0)
    def outp(n,_):
        c = pl.ds(pl.multiple_of(n*256,256),256)
        h_s[:, c] = nn(mixed_o[...], wo[:, c]) + bo[:, c] + x[:, c].astype(f32)
        return 0
    lax.fori_loop(0, width//256, outp, 0)
    def norm(n,_):
        r = pl.ds(pl.multiple_of(n*128,128),128)
        h = h_s[r,:]
        cen = h - jnp.mean(h,-1,keepdims=True)
        rs = lax.rsqrt(jnp.mean(cen*cen,-1,keepdims=True)+EPS)
        xhat_o[r,:] = cen*rs
        rstd_o[r,:] = rs
        return 0
    lax.fori_loop(0, rows//128, norm, 0)

def attn_fwd(lens,x,wq,bq,wk,wv,bv,wo,bo):
    rows,width=x.shape; seqs=lens.shape[0]
    sd=jax.ShapeDtypeStruct
    vm=pl.BlockSpec(memory_space=pltpu.VMEM); sm=pl.BlockSpec(memory_space=pltpu.SMEM)
    return pl.pallas_call(attn_fwd_kernel, in_specs=[sm]+[vm]*8, out_specs=[vm]*7,
        out_shape=[sd((rows,width),bf16)]*4+[sd((rows,width),f32),sd((rows,1),f32),sd((seqs,H,rows//seqs),f32)],
        scratch_shapes=[pltpu.VMEM((rows,width),f32)], compiler_params=cp(), name="attn_fwd")(lens,x,wq,bq,wk,wv,bv,wo,bo)

GP=0.21
GC=(0.08371157579811618,0.08506885551666664,0.06919218864603045,0.12487264645005582,-0.09392498947908608,0.3494006440217003,-0.3302530091485681,0.2835883509790708,-0.07165625592844904)
def gelu_parts(u):
    a = jnp.abs(u)
    t = 1.0/(1.0+GP*a)
    e = jnp.exp(-0.5*u*u)
    q = jnp.full_like(t,GC[-1])
    for c in GC[-2::-1]: q = q*t+c
    tail = q*t*e
    cdf = jnp.where(u>0, 1.0-tail, tail)
    return u*cdf, cdf + u*e*0.3989422804014327

FB=512
def ffn_fwd_kernel(lens, xhat, g1, s1, wi, bi, wo, bo, g2, s2, dout, fin_o, hid_o, gp_o, lo_o, dffn_o, dh2_o, dg2_o, ds2_o, dbo_o, acc):
    n = pl.program_id(0)
    rows,width=xhat.shape
    seqs=lens.shape[0]; length=rows//seqs
    @pl.when(n==0)
    def _():
        fin_o[...] = (xhat[...]*g1[...]+s1[...]).astype(bf16)
    RB=128
    for i in range(rows//RB):
        r=slice(i*RB,(i+1)*RB)
        u = nn(fin_o[r,:],wi[...])+bi[...]
        hid,gp=gelu_parts(u)
        hb=hid.astype(bf16)
        hid_o[r,:]=hb; gp_o[r,:]=gp.astype(bf16)
    part = nn(hid_o[...],wo[...])
    @pl.when(n==0)
    def _(): acc[...]=part
    @pl.when(n>0)
    def _(): acc[...]=acc[...]+part
    @pl.when(n==pl.num_programs(0)-1)
    def _():
        dg2_o[...]=jnp.zeros_like(dg2_o); ds2_o[...]=jnp.zeros_like(ds2_o); dbo_o[...]=jnp.zeros_like(dbo_o)
        B=32
        pos=lax.broadcasted_iota(jnp.int32,(B,1),0)
        def blk(i,_):
            r=pl.ds(pl.multiple_of(i*B,B),B)
            s=i//(length//B); off=(i%(length//B))*B
            keep=jnp.where(pos+off<lens[s],1.0,0.0).astype(f32)
            x1=xhat[r,:]*g1[...]+s1[...]
            ffn=(acc[r,:]+bo[...]).astype(bf16).astype(f32)
            h=x1+ffn
            cen=h-jnp.mean(h,-1,keepdims=True)
            rs=lax.rsqrt(jnp.mean(cen*cen,-1,keepdims=True)+EPS)
            unit=cen*rs
            lo_o[r,:]=((unit*g2[...]+s2[...])*keep).astype(bf16)
            g=dout[r,:].astype(f32)*keep
            e=g*g2[...]
            dh=rs*(e-jnp.mean(e,-1,keepdims=True)-unit*jnp.mean(e*unit,-1,keepdims=True))
            dh2_o[r,:]=dh
            db=dh.astype(bf16)
            dffn_o[r,:]=db
            dg2_o[...]+=jnp.sum(g*unit,0,keepdims=True)
            ds2_o[...]+=jnp.sum(g,0,keepdims=True)
            dbo_o[...]+=jnp.sum(db.astype(f32),0,keepdims=True)
            return 0
        lax.fori_loop(0,rows//B,blk,0)

def ffn_fwd(lens,xhat,g1,s1,wi,bi,wo,bo,g2,s2,dout):
    rows,width=xhat.shape; ff=wi.shape[1]
    sd=jax.ShapeDtypeStruct
    full=lambda a: pl.BlockSpec(a.shape, lambda n,*_: (0,)*len(a.shape))
    col=lambda r: pl.BlockSpec((r,FB),lambda n,*_:(0,n))
    outs=[sd((rows,width),bf16),sd((rows,ff),bf16),sd((rows,ff),bf16),sd((rows,width),bf16),sd((rows,width),bf16),sd((rows,width),f32)]+[sd((1,width),f32)]*3
    return pl.pallas_call(ffn_fwd_kernel, grid_spec=pltpu.PrefetchScalarGridSpec(num_scalar_prefetch=1,grid=(ff//FB,),
        in_specs=[full(xhat),full(g1),full(s1),col(width),col(1),pl.BlockSpec((FB,width),lambda n,*_:(n,0)),full(bo),full(g2),full(s2),full(dout)],
        out_specs=[full(outs[0]),col(rows),col(rows)]+[full(o) for o in outs[3:]],
        scratch_shapes=[pltpu.VMEM((rows,width),f32)]),
        out_shape=outs, compiler_params=cp(), name="ffn_fwd")(lens,xhat,g1,s1,wi,bi,wo,bo,g2,s2,dout)

def ffn_bwd_kernel(dffn, wo, gp, wi, dh2, xhat, rstd, g1, wout, dpre_o, dbi_o, dh1_o, dob_o, dmix_o, dg1_o, ds1_o, dbo_o, acc):
    n=pl.program_id(0)
    rows,width=dffn.shape
    RB=128
    for i in range(rows//RB):
        r=slice(i*RB,(i+1)*RB)
        d=nt(dffn[r,:],wo[...])*gp[r,:].astype(f32)
        db=d.astype(bf16)
        dpre_o[r,:]=db
    dbi_o[...]=jnp.sum(dpre_o[...].astype(f32),0,keepdims=True)
    part=nt(dpre_o[...],wi[...])
    @pl.when(n==0)
    def _(): acc[...]=part
    @pl.when(n>0)
    def _(): acc[...]=acc[...]+part
    @pl.when(n==pl.num_programs(0)-1)
    def _():
        dg1_o[...]=jnp.zeros_like(dg1_o); ds1_o[...]=jnp.zeros_like(ds1_o); dbo_o[...]=jnp.zeros_like(dbo_o)
        B=32
        def blk(i,_):
            r=pl.ds(pl.multiple_of(i*B,B),B)
            g=dh2[r,:]+acc[r,:].astype(bf16).astype(f32)
            unit=xhat[r,:]
            e=g*g1[...]
            dh=rstd[r,:]*(e-jnp.mean(e,-1,keepdims=True)-unit*jnp.mean(e*unit,-1,keepdims=True))
            dh1_o[r,:]=dh
            db=dh.astype(bf16)
            dob_o[r,:]=db
            dg1_o[...]+=jnp.sum(g*unit,0,keepdims=True)
            ds1_o[...]+=jnp.sum(g,0,keepdims=True)
            dbo_o[...]+=jnp.sum(db.astype(f32),0,keepdims=True)
            return 0
        lax.fori_loop(0,rows//B,blk,0)
        def mx(k,_):
            c=pl.ds(pl.multiple_of(k*256,256),256)
            dmix_o[:,c]=nt(dob_o[...],wout[c,:]).astype(bf16)
            return 0
        lax.fori_loop(0,width//256,mx,0)

def ffn_bwd(dffn,wo,gp,wi,dh2,xhat,rstd,g1,wout):
    rows,width=dffn.shape; ff=wi.shape[1]
    sd=jax.ShapeDtypeStruct
    full=lambda a: pl.BlockSpec(a.shape, lambda n: (0,)*len(a.shape))
    col=lambda r: pl.BlockSpec((r,FB),lambda n:(0,n))
    outs=[sd((rows,ff),bf16),sd((1,ff),f32),sd((rows,width),f32),sd((rows,width),bf16),sd((rows,width),bf16)]+[sd((1,width),f32)]*3
    return pl.pallas_call(ffn_bwd_kernel, grid=(ff//FB,),
        in_specs=[full(dffn),pl.BlockSpec((FB,width),lambda n:(n,0)),col(rows),col(width),full(dh2),full(xhat),full(rstd),full(g1),full(wout)],
        out_specs=[col(rows),col(1)]+[full(o) for o in outs[2:]],
        scratch_shapes=[pltpu.VMEM((rows,width),f32)],
        out_shape=outs, compiler_params=cp(), name="ffn_bwd")(dffn,wo,gp,wi,dh2,xhat,rstd,g1,wout)

def attn_bwd_kernel(lens, q, k, v, dm, lse, dob, d_o, dbq_o, dbv_o):
    rows,width=q.shape; seqs=lens.shape[0]; length=rows//seqs; size=width//H
    lane=lax.broadcasted_iota(jnp.int32,(length,128),1); low=lane<size
    pos=lax.broadcasted_iota(jnp.int32,(length,1),0)
    dbq_o[...]=jnp.zeros_like(dbq_o); dbv_o[...]=jnp.zeros_like(dbv_o)
    d_o[:,3*width:]=dob[...]
    def chain(s,_):
        r=pl.ds(pl.multiple_of(s*length,32),length)
        live=pos<lens[s]
        for p in range(H//2):
            c=slice(128*p,128*p+128)
            qp=q[r,c]; kp=k[r,c]; vp=v[r,c]; dp=dm[r,c]
            dq=[];dk=[];dv=[]
            for h in range(2):
                sel=low if h==0 else ~low
                kh=jnp.where(sel,kp,jnp.zeros_like(kp)); vh=jnp.where(sel,vp,jnp.zeros_like(vp))
                st=nt(kh,qp)
                st=jnp.where(live,st,-1e9)
                pt=jnp.exp(st-lse[s,pl.ds(2*p+h,1),:])
                dpt=nt(vh,dp)
                delta=jnp.sum(pt*dpt,0,keepdims=True)
                ds=(pt*(dpt-delta)).astype(bf16)
                dv.append(nn(pt.astype(bf16),dp))
                dk.append(nn(ds,qp))
                dq.append(tn(ds,kp))
            dqb=(jnp.where(low,dq[0],dq[1])*0.125).astype(bf16)
            dvb=jnp.where(low,dv[0],dv[1]).astype(bf16)
            d_o[r,128*p:128*p+128]=dqb
            d_o[r,width+128*p:width+128*p+128]=jnp.where(low,dk[0],dk[1]).astype(bf16)
            d_o[r,2*width+128*p:2*width+128*p+128]=dvb
            dbq_o[:,c]+=jnp.sum(dqb.astype(f32),0,keepdims=True)
            dbv_o[:,c]+=jnp.sum(dvb.astype(f32),0,keepdims=True)
        return 0
    lax.fori_loop(0,seqs,chain,0)

def attn_bwd(lens,q,k,v,dm,lse,dob):
    rows,width=q.shape
    sd=jax.ShapeDtypeStruct
    vm=pl.BlockSpec(memory_space=pltpu.VMEM); sm=pl.BlockSpec(memory_space=pltpu.SMEM)
    return pl.pallas_call(attn_bwd_kernel,in_specs=[sm]+[vm]*6,out_specs=[vm]*3,
        out_shape=[sd((rows,4*width),bf16),sd((1,width),f32),sd((1,width),f32)],compiler_params=cp(),name="attn_bwd")(lens,q,k,v,dm,lse,dob)

def dx_kernel(dh1,d,wq,wk,wv,o):
    width=dh1.shape[1]
    def blk(n,_):
        c=pl.ds(pl.multiple_of(n*256,256),256)
        o[:,c]=dh1[:,c]+nt(d[:,0:width],wq[c,:])+nt(d[:,width:2*width],wk[c,:])+nt(d[:,2*width:3*width],wv[c,:])
        return 0
    lax.fori_loop(0,width//256,blk,0)
def dx_call(dh1,d,wq,wk,wv):
    vm=pl.BlockSpec(memory_space=pltpu.VMEM)
    return pl.pallas_call(dx_kernel,in_specs=[vm]*5,out_specs=vm,out_shape=jax.ShapeDtypeStruct(dh1.shape,f32),compiler_params=cp(),name="dx")(dh1,d,wq,wk,wv)

CHUNK = 384
COLORS = 3


def bit(value, name):
    return (value >> "xya".index(name)) & 1


def lhs_of(kind, me, step, refs):
    if kind == "attn":
        return jnp.where((step ^ me[1]) >= 6, refs[1][...], refs[0][...])
    return refs[0][...]


def send_kernel(kind, me, *refs):
    step = pl.program_id(0)
    rhs, out = refs[-2:]
    grad = tn(lhs_of(kind, me, step, refs), rhs[...]).astype(bf16)
    part = grad.shape[0] // 2
    for t in range(2):
        out[0, t ^ me[2]] = grad[t * part : (t + 1) * part]


def keep_kernel(kind, orders, me, *refs):
    step = pl.program_id(0)
    n_in = 4 if kind == "attn" else 3
    rhs, got = refs[n_in - 2 : n_in]
    outs = refs[n_in:]
    grad = tn(lhs_of(kind, me, step, refs), rhs[...])
    part = grad.shape[0] // 2
    piece = part // len(orders)
    for t in range(2):
        rel = t ^ me[2]
        total = (grad[t * part : (t + 1) * part] + got[0, rel].astype(f32)).astype(bf16)
        for n, order in enumerate(orders):
            where = bit(step, order[1]) * 4 + bit(step, order[2]) * 2 + rel
            first = bit(step, order[0])
            value = total[n * piece : (n + 1) * piece]

            @pl.when(first == 0)
            def _():
                outs[2 * n][where] = value

            @pl.when(first == 1)
            def _():
                outs[2 * n + 1][where] = value


def grad_specs(kind, rows, flip):
    chunk = lambda s, me: (0, s ^ me[1])
    half = lambda s, me: (0, me[0] ^ flip)
    block = (rows, CHUNK)
    if kind == "outer":
        return [pl.BlockSpec(block, chunk), pl.BlockSpec(block, half)]
    if kind == "inner":
        return [pl.BlockSpec(block, half), pl.BlockSpec(block, chunk)]
    return [pl.BlockSpec(block, half), pl.BlockSpec(block, half), pl.BlockSpec(block, chunk)]


def grad_send(kind, me, args):
    rows = args[0].shape[0]
    part = CHUNK // 2
    return pl.pallas_call(
        functools.partial(send_kernel, kind),
        grid_spec=pltpu.PrefetchScalarGridSpec(
            num_scalar_prefetch=1,
            grid=(8,),
            in_specs=grad_specs(kind, rows, 1),
            out_specs=pl.BlockSpec((1, 2, part, CHUNK), lambda s, me: (s, 0, 0, 0)),
        ),
        out_shape=jax.ShapeDtypeStruct((8, 2, part, CHUNK), bf16),
        compiler_params=cp(),
        name="send_" + kind,
    )(me, *args)


def grad_keep(kind, me, args, got, orders):
    rows = args[0].shape[0]
    part = CHUNK // 2
    shape = (8, part // len(orders), CHUNK)
    return pl.pallas_call(
        functools.partial(keep_kernel, kind, orders),
        grid_spec=pltpu.PrefetchScalarGridSpec(
            num_scalar_prefetch=1,
            grid=(8,),
            in_specs=grad_specs(kind, rows, 0)
            + [pl.BlockSpec((1, 2, part, CHUNK), lambda s, me: (s, 0, 0, 0))],
            out_specs=[pl.BlockSpec(shape, lambda s, me: (0, 0, 0))] * (2 * len(orders)),
        ),
        out_shape=[jax.ShapeDtypeStruct(shape, bf16)] * (2 * len(orders)),
        compiler_params=cp(),
        name="keep_" + kind,
    )(me, *args, got)


def unpack_kernel(kind, orders, me, *refs):
    chunk = pl.program_id(0)
    step = chunk ^ me[1]
    ins = refs[: 4 * len(orders)]
    outs = refs[4 * len(orders) :]
    part = CHUNK // 2
    piece = part // len(orders)

    def fill(out):
        for n, order in enumerate(orders):
            own0, got0, own1, got1 = ins[4 * n : 4 * n + 4]
            first = bit(step, order[0]) == 1
            for t in range(2):
                where = bit(step, order[1]) * 4 + bit(step, order[2]) * 2 + (t ^ me[2])
                near = jnp.where(first, got0[where], own0[where])
                far = jnp.where(first, got1[where], own1[where])
                for half in range(2):
                    value = jnp.where(half == me[0], near, far).astype(f32)
                    row = t * part + n * piece
                    if kind == "outer":
                        out[row : row + piece, half * CHUNK : (half + 1) * CHUNK] = value
                    else:
                        row = row + half * CHUNK
                        out[row : row + piece, :] = value

    if kind == "attn":
        for mat in range(4):

            @pl.when(chunk // 2 == mat)
            def _():
                fill(outs[mat])
    else:
        fill(outs[0])


def unpack(kind, me, pieces, orders):
    width = 2 * CHUNK
    shape = (8, CHUNK // 2 // len(orders), CHUNK)
    if kind == "outer":
        out_specs = [pl.BlockSpec((CHUNK, width), lambda c, me: (c, 0))]
        out_shape = [jax.ShapeDtypeStruct((8 * CHUNK, width), f32)]
    elif kind == "inner":
        out_specs = [pl.BlockSpec((width, CHUNK), lambda c, me: (0, c))]
        out_shape = [jax.ShapeDtypeStruct((width, 8 * CHUNK), f32)]
    else:
        out_specs = [
            pl.BlockSpec((width, CHUNK), lambda c, me, m=m: (0, jnp.clip(c - 2 * m, 0, 1)))
            for m in range(4)
        ]
        out_shape = [jax.ShapeDtypeStruct((width, width), f32)] * 4
    return pl.pallas_call(
        functools.partial(unpack_kernel, kind, orders),
        grid_spec=pltpu.PrefetchScalarGridSpec(
            num_scalar_prefetch=1,
            grid=(8,),
            in_specs=[pl.BlockSpec(shape, lambda c, me: (0, 0, 0))] * (4 * len(orders)),
            out_specs=out_specs,
        ),
        out_shape=out_shape,
        compiler_params=cp(),
        name="unpack_" + kind,
    )(me, *pieces)


AXES = ("dp", "seq")
DP_BIT = {"x": 0, "y": 1, "a": 2, "b": 3}


def swap(value, name):
    dp = lax.axis_size("dp")
    seq = lax.axis_size("seq")
    flip = 1 if name == "c" else seq << (name if isinstance(name, int) else DP_BIT[name])
    return lax.ppermute(value, AXES, [(i, i ^ flip) for i in range(dp * seq)])


def scatter_sum(keep, send, order):
    for n, name in enumerate(order):
        got = swap(send, name)
        if n + 1 < len(order):
            half = keep.shape[0] // 2
            keep, send = keep[:half] + got[:half], keep[half:] + got[half:]
        else:
            keep = keep + got
    own = keep
    for extra in range(4, lax.axis_size("dp").bit_length() - 1):
        own = own + swap(own, extra)
    return own


def gather(own, order):
    for n, name in enumerate(reversed(order)):
        got = swap(own, name)
        if n + 1 < len(order):
            own = jnp.concatenate([own, got])
    return own, got


ORDERS = {
    "outer": ("xyab", "yxab", "axyb"),
    "inner": ("xyab", "yxab", "ayxb"),
    "attn": ("xyab", "yxab", "axyb"),
}


def reduce_group(kind, me, args):
    orders = ORDERS[kind]
    got = swap(grad_send(kind, me, args), "c")
    blocks = grad_keep(kind, me, args, got, orders)
    pieces = []
    for n, order in enumerate(orders):
        own = scatter_sum(blocks[2 * n], blocks[2 * n + 1], order)
        own0, got0 = gather(own, order)
        pieces += [own0, got0, swap(own0, "c"), swap(got0, "c")]
    return unpack(kind, me, pieces, orders)


def body(chains_in, lengths, d_out, w_query, b_query, w_key, w_value, b_value, w_output, b_output, gain_one, shift_one,
         w_inner, b_inner, w_outer, b_outer, gain_two, shift_two):
    seqs, length, width = chains_in.shape
    rows = seqs * length
    place = lax.axis_index("dp") * 2 + lax.axis_index("seq")
    me = (place >> jnp.array([0, 1, 4], jnp.int32)) & jnp.array([1, 7, 1], jnp.int32)
    x = chains_in.reshape(rows, width)
    row = lambda v: v.reshape(1, -1)
    q, k, v, mixed, xhat, rstd, lse = attn_fwd(
        lengths, x, w_query, row(b_query), w_key, w_value, row(b_value), w_output, row(b_output)
    )
    fin, hid, slope, out, dffn, dh2, dg2, ds2, dbo2 = ffn_fwd(
        lengths, xhat, row(gain_one), row(shift_one), w_inner, row(b_inner), w_outer, row(b_outer),
        row(gain_two), row(shift_two), d_out.reshape(rows, width),
    )
    (d_w_outer,) = reduce_group("outer", me, (hid, dffn))
    dpre, dbi, dh1, dob, dmix, dg1, ds1, dbo1 = ffn_bwd(
        dffn, w_outer, slope, w_inner, dh2, xhat, rstd, row(gain_one), w_output
    )
    (d_w_inner,) = reduce_group("inner", me, (fin, dpre))
    d, dbq, dbv = attn_bwd(lengths, q, k, v, dmix, lse, dob)
    d_w_query, d_w_key, d_w_value, d_w_output = reduce_group("attn", me, (x, mixed, d))
    small = [dbq[0], dbv[0], dbo1[0], dg1[0], ds1[0], dbi[0], dbo2[0], dg2[0], ds2[0]]
    sums = lax.psum(jnp.concatenate(small), AXES)
    cuts = []
    start = 0
    for value in small:
        cuts.append(sums[start : start + value.size])
        start += value.size
    d_x = dx_call(dh1, d, w_query, w_key, w_value)
    return (
        out.reshape(seqs, length, width), d_x.reshape(seqs, length, width),
        d_w_query, cuts[0], d_w_key, d_w_value, cuts[1], d_w_output, cuts[2], cuts[3], cuts[4],
        d_w_inner, cuts[5], d_w_outer, cuts[6], cuts[7], cuts[8],
    )


def solution(mesh):
    rows = P(AXES, None, None)
    return jax.shard_map(
        body, mesh=mesh, in_specs=(rows, P(AXES), rows) + (P(),) * 15, out_specs=(rows, rows) + (P(),) * 15, check_vma=False
    )
```

```python
import functools
import jax
import jax.numpy as jnp
from jax import lax
from jax.experimental import pallas as pl
from jax.experimental.pallas import tpu as pltpu
from jax.sharding import PartitionSpec as P

H = 12
EPS = 1e-12
f32 = jnp.float32
bf16 = jnp.bfloat16
sd = jax.ShapeDtypeStruct
HBM = pl.BlockSpec(memory_space=pl.ANY)
VMEM = pl.BlockSpec(memory_space=pltpu.VMEM)
SMEM = pl.BlockSpec(memory_space=pltpu.SMEM)
LIMIT = 60 * 1024 * 1024
CHUNK = 384
HALF = CHUNK // 2


def params():
    return pltpu.CompilerParams(vmem_limit_bytes=LIMIT)


def cost(flops, nbytes=1 << 20):
    return pl.CostEstimate(flops=int(flops), transcendentals=0, bytes_accessed=int(nbytes))


def nn(a, b):
    return lax.dot_general(a, b, (((1,), (0,)), ((), ())), preferred_element_type=f32)


def nt(a, b):
    return lax.dot_general(a, b, (((1,), (1,)), ((), ())), preferred_element_type=f32)


def tn(a, b):
    return lax.dot_general(a, b, (((0,), (0,)), ((), ())), preferred_element_type=f32)


def row_mean(v):
    return jnp.mean(v, -1, keepdims=True)


def ds(start, size, align=None):
    return pl.ds(pl.multiple_of(start, align or size), size)


FWD_IN = ("x", "wq", "wk", "wv", "wo", "wi", "w2", "dout")
FWD_OUT = ("q", "k", "v", "mixed", "xhat", "rstd", "fin", "out", "dffn")


def row(ref):
    return ref[...].reshape(1, ref.shape[0])


def both(low, v):
    zero = jnp.zeros_like(v)
    return jnp.concatenate([jnp.where(low, v, zero), jnp.where(low, zero, v)], 0)


def pairs_of(width, size):
    return [slice(2 * size * p, 2 * size * (p + 1)) for p in range(width // (2 * size))]


def attention(lens, q, k, v, mixed, lse):
    rows, width = q.shape
    seqs = lens.shape[0]
    length = rows // seqs
    size = width // H
    low = lax.broadcasted_iota(jnp.int32, (length, 2 * size), 1) < size
    pos = lax.broadcasted_iota(jnp.int32, (2, length, 1), 1)

    def chain(s, _):
        r = ds(s * length, length, 32)
        live = pos < lens[s]
        cols = pairs_of(width, size)
        scores = [nt(both(low, k[r, c]), q[r, c]) for c in cols]
        for p, c in enumerate(cols):
            st = jnp.where(live, scores[p].reshape(2, length, length), -1e9)
            top = jnp.max(st, 1, keepdims=True)
            e = jnp.exp(st - top)
            total = jnp.sum(e, 1, keepdims=True)
            lse[s, pl.ds(2 * p, 2), :] = (top + jnp.log(total)).reshape(2, length)
            prob = (e * (1.0 / total)).astype(bf16).reshape(2 * length, length)
            mixed[r, c] = tn(prob, both(low, v[r, c])).astype(bf16)
        return 0

    lax.fori_loop(0, seqs, chain, 0)


def put_send(out, grad, base, chunk0, me, rows_are_chunks):
    size = grad.shape[0 if rows_are_chunks else 1]
    for i in range(size // CHUNK):
        for t in range(2):
            if rows_are_chunks:
                value = grad[i * CHUNK + t * HALF : i * CHUNK + (t + 1) * HALF, :]
            else:
                value = grad[t * HALF : (t + 1) * HALF, i * CHUNK : (i + 1) * CHUNK]
            out[((chunk0 + i) ^ me[1]) * 2 + (t ^ me[2]) - base] = value.astype(bf16)


def fwd_kernel(*refs):
    lens, me = refs[:2]
    bq, bv, bo, g1, s1, bi, b2, g2, s2 = refs[2:11]
    src = dict(zip(FWD_IN, refs[11:19]))
    lse, small = refs[19:21]
    dst = dict(zip(FWD_OUT, refs[21:30]))
    hid_h, slope_h, send_h = refs[30:33]
    rest = refs[33:]
    vin = dict(zip(FWD_IN, rest[:8]))
    vout = dict(zip(FWD_OUT, rest[8:17]))
    hid, slope, send, acc, sem_in, sem_out, sem_ff, sem_send = rest[17:]
    rows, width = vin["x"].shape
    ff = vin["wi"].shape[1]
    seqs = lens.shape[0]
    length = rows // seqs

    def load(name):
        return pltpu.make_async_copy(src[name], vin[name], sem_in.at[FWD_IN.index(name)])

    def store(name):
        return pltpu.make_async_copy(vout[name], dst[name], sem_out.at[FWD_OUT.index(name)])

    x, q, k, v, mixed = vin["x"], vout["q"], vout["k"], vout["v"], vout["mixed"]
    for name in ("x", "wq", "wk"):
        load(name).start()
    load("x").wait()
    load("wq").wait()
    load("wv").start()
    load("wo").start()
    q[...] = ((nn(x[...], vin["wq"][...]) + row(bq)).astype(bf16).astype(f32) * 0.125).astype(bf16)
    store("q").start()
    load("wk").wait()
    load("wi").start()
    k[...] = nn(x[...], vin["wk"][...]).astype(bf16)
    store("k").start()
    load("wv").wait()
    load("w2").start()
    load("dout").start()
    v[...] = (nn(x[...], vin["wv"][...]) + row(bv)).astype(bf16)
    store("v").start()
    attention(lens, q, k, v, mixed, lse)
    store("mixed").start()
    load("wo").wait()
    xhat, rstd, fin = vout["xhat"], vout["rstd"], vout["fin"]
    acc[...] = nn(mixed[...], vin["wo"][...])
    R = length
    gain1, shift1, bias_o = row(g1), row(s1), row(bo)

    def norm_one(n, _):
        r = ds(n * R, R, 32)
        h = acc[r, :] + bias_o + x[r, :].astype(f32)
        centre = h - row_mean(h)
        scale = lax.rsqrt(row_mean(centre * centre) + EPS)
        unit = centre * scale
        xhat[r, :] = unit
        rstd[r, :] = scale
        fin[r, :] = (unit * gain1 + shift1).astype(bf16)
        return 0

    lax.fori_loop(0, rows // R, norm_one, 0)
    store("rstd").start()
    store("fin").start()
    store("xhat").start()
    wi, w2 = vin["wi"], vin["w2"]
    load("wi").wait()
    load("w2").wait()
    RB = 320
    part_ff = ff // width

    def ff_copies(n):
        c = ds(n * width, width)
        return (
            pltpu.make_async_copy(hid.at[:, c], hid_h.at[:, c], sem_ff.at[0, n]),
            pltpu.make_async_copy(slope.at[:, c], slope_h.at[:, c], sem_ff.at[1, n]),
        )

    def feed(n, _):
        c = ds(n * width, width)
        bias_i = bi[ds(n * width, width)].reshape(1, width)
        for i in range(rows // RB):
            r = slice(i * RB, (i + 1) * RB)
            u = nn(fin[r, :], wi[:, c]) + bias_i
            cdf = 0.5 * lax.erf(u * 0.7071067811865476) + 0.5
            hid[r, c] = (u * cdf).astype(bf16)
            slope[r, c] = (cdf + u * jnp.exp(-0.5 * (u * u)) * 0.3989422804014327).astype(bf16)
            part = nn(hid[r, c], w2[c, :])
            acc[r, :] = jnp.where(n == 0, part, acc[r, :] + part)
        for one in ff_copies(n):
            one.start()
        return 0

    lax.fori_loop(0, part_ff, feed, 0)
    load("dout").wait()
    dout, out, dffn = vin["dout"], vout["out"], vout["dffn"]
    small[...] = jnp.zeros_like(small)
    gain2, shift2, bias_2 = row(g2), row(s2), row(b2)
    pos = lax.broadcasted_iota(jnp.int32, (R, 1), 0)

    def norm_two(n, _):
        r = ds(n * R, R, 32)
        keep = jnp.where(pos < lens[n], 1.0, 0.0).astype(f32)
        h = xhat[r, :] * gain1 + shift1 + (acc[r, :] + bias_2).astype(bf16).astype(f32)
        centre = h - row_mean(h)
        scale = lax.rsqrt(row_mean(centre * centre) + EPS)
        unit = centre * scale
        out[r, :] = ((unit * gain2 + shift2) * keep).astype(bf16)
        g = dout[r, :].astype(f32) * keep
        e = g * gain2
        low = (scale * (e - row_mean(e) - unit * row_mean(e * unit))).astype(bf16)
        dffn[r, :] = low
        small[0:1, :] += jnp.sum(g * unit, 0, keepdims=True)
        small[1:2, :] += jnp.sum(g, 0, keepdims=True)
        small[2:3, :] += jnp.sum(low.astype(f32), 0, keepdims=True)
        return 0

    lax.fori_loop(0, seqs, norm_two, 0)
    store("dffn").start()
    store("out").start()
    far = ds((1 - me[0]) * CHUNK, CHUNK)

    def send_copy(n):
        part = pl.ds(4 * (n ^ (me[1] >> 1)), 4)
        return pltpu.make_async_copy(send.at[part], send_h.at[part], sem_send.at[n])

    def grads(n, _):
        put_send(send, tn(hid[:, ds(n * width, width)], dffn[:, far]), 0, 2 * n, me, True)
        send_copy(n).start()
        return 0

    lax.fori_loop(0, part_ff, grads, 0)
    for name in FWD_OUT:
        store(name).wait()
    for n in range(part_ff):
        for one in ff_copies(n):
            one.wait()
        send_copy(n).wait()


def forward(lens, me, vectors, arrays):
    rows, width = arrays[0].shape
    ff = arrays[5].shape[1]
    seqs = lens.shape[0]
    like = lambda shape, dtype=bf16: sd(shape, dtype)
    thin = like((rows, width))
    outs = [thin, thin, thin, thin, like((rows, width), f32), like((rows, 1), f32), thin, thin, thin]
    wide = [like((rows, ff)), like((rows, ff)), like((16, HALF, CHUNK))]
    dma = pltpu.SemaphoreType.DMA
    return pl.pallas_call(
        fwd_kernel,
        in_specs=[SMEM, SMEM] + [VMEM] * 9 + [HBM] * 8,
        out_specs=[VMEM, VMEM] + [HBM] * 12,
        out_shape=[like((seqs, H, rows // seqs), f32), like((8, width), f32)] + outs + wide,
        scratch_shapes=[pltpu.VMEM(a.shape, a.dtype) for a in arrays]
        + [pltpu.VMEM(o.shape, o.dtype) for o in outs + wide]
        + [pltpu.VMEM((rows, width), f32), dma((8,)), dma((9,)), dma((2, ff // width)), dma((ff // width,))],
        compiler_params=params(),
        cost_estimate=cost(28e9),
        name="forward",
    )(lens, me, *vectors, *arrays)


def pre_kernel(me, dffn, w2, slope, fin, small2, dpre_o, send_o, small):
    p = pl.program_id(0)
    n = p ^ (me[1] >> 1)

    @pl.when(p == 0)
    def _():
        small[0:8, :] = small2[...]
        small[8:16, :] = jnp.zeros((8, small.shape[1]), f32)

    d = (nt(dffn[...], w2[...]) * slope[...].astype(f32)).astype(bf16)
    dpre_o[...] = d
    small[pl.ds(8 + n, 1), :] = jnp.sum(d.astype(f32), 0, keepdims=True)
    put_send(send_o, tn(fin[...], dpre_o[...]), 4 * p, 2 * n, me, False)


def pre_call(me, dffn, w2, slope, fin, small2):
    rows, width = dffn.shape
    ff = w2.shape[0]
    at = lambda p, me: p ^ (me[1] >> 1)
    return pl.pallas_call(
        pre_kernel,
        grid_spec=pltpu.PrefetchScalarGridSpec(
            num_scalar_prefetch=1,
            grid=(ff // width,),
            in_specs=[
                pl.BlockSpec((rows, width), lambda p, me: (0, 0)),
                pl.BlockSpec((width, width), lambda p, me: (at(p, me), 0)),
                pl.BlockSpec((rows, width), lambda p, me: (0, at(p, me))),
                pl.BlockSpec((rows, CHUNK), lambda p, me: (0, 1 - me[0])),
                pl.BlockSpec((8, width), lambda p, me: (0, 0)),
            ],
            out_specs=[
                pl.BlockSpec((rows, width), lambda p, me: (0, at(p, me))),
                pl.BlockSpec((4, HALF, CHUNK), lambda p, me: (p, 0, 0)),
                pl.BlockSpec((16, width), lambda p, me: (0, 0)),
            ],
        ),
        out_shape=[sd((rows, ff), bf16), sd((16, HALF, CHUNK), bf16), sd((16, width), f32)],
        compiler_params=params(),
        cost_estimate=cost(8e9),
        name="pre_bwd",
    )(me, dffn, w2, slope, fin, small2)


BWD_IN = ("dffn", "xhat", "rstd", "wo", "q", "k", "v", "lse", "x", "mixed")


def attention_bwd(lens, q, k, v, dm, lse, d, small):
    rows, width = q.shape
    seqs = lens.shape[0]
    length = rows // seqs
    size = width // H
    low = lax.broadcasted_iota(jnp.int32, (length, 2 * size), 1) < size
    pos = lax.broadcasted_iota(jnp.int32, (2, length, 1), 1)

    def chain(s, _):
        r = ds(s * length, length, 32)
        live = pos < lens[s]
        cols = pairs_of(width, size)
        first = []
        for c in cols:
            k2 = both(low, k[r, c])
            first.append((k2, nt(k2, q[r, c]), nt(both(low, v[r, c]), dm[r, c])))
        for p, c in enumerate(cols):
            k2, st, dprob = first[p]
            st = jnp.where(live, st.reshape(2, length, length), -1e9)
            dprob = dprob.reshape(2, length, length)
            prob = jnp.exp(st - lse[s, pl.ds(2 * p, 2), :].reshape(2, 1, length))
            delta = jnp.sum(prob * dprob, 1, keepdims=True)
            dst = (prob * (dprob - delta)).astype(bf16).reshape(2 * length, length)
            dv = nn(prob.astype(bf16).reshape(2 * length, length), dm[r, c])
            dk = nn(dst, q[r, c])
            dq = (tn(dst, k2) * 0.125).astype(bf16)
            dv = jnp.where(low, dv[:length], dv[length:]).astype(bf16)
            d[r, c] = dq
            d[r, slice(width + c.start, width + c.stop)] = jnp.where(low, dk[:length], dk[length:]).astype(bf16)
            d[r, slice(2 * width + c.start, 2 * width + c.stop)] = dv
            small[6:7, c] += jnp.sum(dq.astype(f32), 0, keepdims=True)
            small[7:8, c] += jnp.sum(dv.astype(f32), 0, keepdims=True)
        return 0

    lax.fori_loop(0, seqs, chain, 0)


def bwd_kernel(*refs):
    lens, me, g1, small1, dpre_h, wi_h = refs[:6]
    src = dict(zip(BWD_IN, refs[6:16]))
    small, dh1_h, d_h, send_h = refs[16:20]
    dpre, wi = refs[20:22]
    vin = dict(zip(BWD_IN, refs[22:32]))
    dh1, d, send, acc, dm, sem_ff, sem_in, sem_out, sem_send = refs[32:]
    rows, width = acc.shape
    part_ff = dpre.shape[1] // width
    seqs = lens.shape[0]
    R = rows // seqs

    def load(name):
        return pltpu.make_async_copy(src[name], vin[name], sem_in.at[BWD_IN.index(name)])

    def ff_copies(n):
        c = slice(n * width, (n + 1) * width)
        return (
            pltpu.make_async_copy(dpre_h.at[:, c], dpre.at[:, c], sem_ff.at[0, n]),
            pltpu.make_async_copy(wi_h.at[:, c], wi.at[:, c], sem_ff.at[1, n]),
        )

    for n in range(part_ff):
        for one in ff_copies(n):
            one.start()
    for name in BWD_IN:
        load(name).start()
    for n in range(part_ff):
        c = slice(n * width, (n + 1) * width)
        for one in ff_copies(n):
            one.wait()
        part = nt(dpre[:, c], wi[:, c])
        acc[...] = part if n == 0 else acc[...] + part
    small[...] = small1[...]
    gain1 = row(g1)
    dffn, xhat, rstd = vin["dffn"], vin["xhat"], vin["rstd"]
    for name in ("dffn", "xhat", "rstd"):
        load(name).wait()
    dob = slice(3 * width, 4 * width)

    def norm_one(i, _):
        r = ds(i * R, R, 32)
        g = dffn[r, :].astype(f32) + acc[r, :].astype(bf16).astype(f32)
        unit = xhat[r, :]
        e = g * gain1
        v = rstd[r, :] * (e - row_mean(e) - unit * row_mean(e * unit))
        dh1[r, :] = v
        low = v.astype(bf16)
        d[r, dob] = low
        small[3:4, :] += jnp.sum(g * unit, 0, keepdims=True)
        small[4:5, :] += jnp.sum(g, 0, keepdims=True)
        small[5:6, :] += jnp.sum(low.astype(f32), 0, keepdims=True)
        return 0

    lax.fori_loop(0, seqs, norm_one, 0)
    dh1_copy = pltpu.make_async_copy(dh1, dh1_h, sem_out.at[0])
    dh1_copy.start()
    load("wo").wait()
    dm[...] = nt(d[:, dob], vin["wo"][...]).astype(bf16)
    for name in ("q", "k", "v", "lse"):
        load(name).wait()
    attention_bwd(lens, vin["q"], vin["k"], vin["v"], dm, vin["lse"], d, small)
    d_copy = pltpu.make_async_copy(d, d_h, sem_out.at[1])
    d_copy.start()
    load("x").wait()
    load("mixed").wait()
    far = ds((1 - me[0]) * CHUNK, CHUNK)

    def send_copy(n):
        part = pl.ds(4 * (n ^ (me[1] >> 1)), 4)
        return pltpu.make_async_copy(send.at[part], send_h.at[part], sem_send.at[n])

    for n in range(4):
        left = vin["mixed" if n == 3 else "x"]
        put_send(send, tn(left[:, far], d[:, n * width : (n + 1) * width]), 0, 2 * n, me, False)
        send_copy(n).start()
    dh1_copy.wait()
    d_copy.wait()
    for n in range(4):
        send_copy(n).wait()


def bwd_call(lens, me, g1, small1, dpre, wi, arrays):
    rows, width = arrays[0].shape
    ff = wi.shape[1]
    dma = pltpu.SemaphoreType.DMA
    vm = lambda a: pltpu.VMEM(a.shape, a.dtype)
    outs = [sd((rows, width), f32), sd((rows, 4 * width), bf16), sd((16, HALF, CHUNK), bf16)]
    return pl.pallas_call(
        bwd_kernel,
        in_specs=[SMEM, SMEM, VMEM, VMEM] + [HBM] * 12,
        out_specs=[VMEM] + [HBM] * 3,
        out_shape=[sd((16, width), f32)] + outs,
        scratch_shapes=[vm(dpre), vm(wi)] + [vm(a) for a in arrays] + [vm(o) for o in outs]
        + [pltpu.VMEM((rows, width), f32), pltpu.VMEM((rows, width), bf16)]
        + [dma((2, ff // width)), dma((10,)), dma((2,)), dma((4,))],
        compiler_params=params(),
        cost_estimate=cost(22e9),
        name="backward",
    )(lens, me, g1, small1, dpre, wi, *arrays)


def dx_kernel(dh1_h, d_h, wq_h, wk_h, wv_h, o_h, dh1, d, wq, wk, wv, o, sem, sem_out):
    width = dh1.shape[1]
    loads = []
    for n, (w_h, w) in enumerate(((wq_h, wq), (wk_h, wk), (wv_h, wv))):
        c = slice(n * width, (n + 1) * width)
        loads.append(pltpu.make_async_copy(d_h.at[:, c], d.at[:, c], sem.at[2 * n]))
        loads.append(pltpu.make_async_copy(w_h, w, sem.at[2 * n + 1]))
    loads.insert(2, pltpu.make_async_copy(dh1_h, dh1, sem.at[6]))
    for one in loads:
        one.start()
    loads[0].wait()
    loads[1].wait()
    part = nt(d[:, :width], wq[...])
    loads[2].wait()
    o[...] = dh1[...] + part
    loads[3].wait()
    loads[4].wait()
    o[...] = o[...] + nt(d[:, width : 2 * width], wk[...])
    loads[5].wait()
    loads[6].wait()
    half = dh1.shape[0] // 2
    stores = []
    for i in range(2):
        r = slice(i * half, (i + 1) * half)
        o[r, :] = o[r, :] + nt(d[r, 2 * width : 3 * width], wv[...])
        stores.append(pltpu.make_async_copy(o.at[r, :], o_h.at[r, :], sem_out.at[i]))
        stores[i].start()
    for one in stores:
        one.wait()


def dx_call(dh1, d, wq, wk, wv):
    rows, width = dh1.shape
    dma = pltpu.SemaphoreType.DMA
    return pl.pallas_call(
        dx_kernel,
        in_specs=[HBM] * 5,
        out_specs=HBM,
        out_shape=sd((rows, width), f32),
        scratch_shapes=[
            pltpu.VMEM((rows, width), f32), pltpu.VMEM((rows, 3 * width), bf16), pltpu.VMEM(wq.shape, bf16),
            pltpu.VMEM(wq.shape, bf16), pltpu.VMEM(wq.shape, bf16), pltpu.VMEM((rows, width), f32), dma((7,)), dma((2,)),
        ],
        compiler_params=params(),
        cost_estimate=cost(5e9),
        name="dx",
    )(dh1, d, wq, wk, wv)


def bit(value, name):
    return (value >> "xya".index(name)) & 1


def pair_grad(kind, pair, refs):
    if kind == "attn":
        x, mixed, d = refs
        return tn(jnp.where(pair == 3, mixed[...], x[...]), d[...])
    return tn(refs[0][...], refs[1][...])


def keep_kernel(kind, orders, me, *refs):
    p = pl.program_id(0)
    n_in = 3 if kind == "attn" else 2
    got = refs[n_in]
    outs = refs[n_in + 1 : -1]
    g = refs[-1]
    g[...] = pair_grad(kind, p ^ (me[1] >> 1), refs[:n_in])
    size = HALF // len(orders)
    for i in range(2):
        step = 2 * p + i
        far = ds((i ^ (me[1] & 1)) * CHUNK, CHUNK)
        for t in range(2):
            part = (t ^ me[2]) * HALF
            if kind == "outer":
                grad = g[ds((i ^ (me[1] & 1)) * CHUNK + part, HALF), :]
            else:
                grad = g[ds(part, HALF), far]
            total = (grad + got[2 * i + t].astype(f32)).astype(bf16)
            for n, order in enumerate(orders):
                where = bit(step, order[1]) * 4 + bit(step, order[2]) * 2 + t
                first = bit(step, order[0])
                value = total[n * size : (n + 1) * size]
                if order[0] == "x":
                    outs[2 * n + i][where] = value
                    continue

                @pl.when(first == 0)
                def _():
                    outs[2 * n][where] = value

                @pl.when(first == 1)
                def _():
                    outs[2 * n + 1][where] = value


def grad_specs(kind, rows, flip, pair_of):
    pair = lambda p, me: (0, pair_of(p, me))
    half = lambda p, me: (0, me[0] ^ flip)
    wide = (rows, 2 * CHUNK)
    thin = (rows, CHUNK)
    if kind == "outer":
        return [pl.BlockSpec(wide, pair), pl.BlockSpec(thin, half)]
    if kind == "inner":
        return [pl.BlockSpec(thin, half), pl.BlockSpec(wide, pair)]
    return [pl.BlockSpec(thin, half), pl.BlockSpec(thin, half), pl.BlockSpec(wide, pair)]


def grad_keep(kind, me, args, got, orders):
    rows = args[0].shape[0]
    shape = (8, HALF // len(orders), CHUNK)
    g_shape = (2 * CHUNK, CHUNK) if kind == "outer" else (CHUNK, 2 * CHUNK)
    return pl.pallas_call(
        functools.partial(keep_kernel, kind, orders),
        grid_spec=pltpu.PrefetchScalarGridSpec(
            num_scalar_prefetch=1,
            grid=(4,),
            in_specs=grad_specs(kind, rows, 0, lambda p, me: p ^ (me[1] >> 1))
            + [pl.BlockSpec((4, HALF, CHUNK), lambda p, me: (p, 0, 0))],
            out_specs=[pl.BlockSpec(shape, lambda p, me: (0, 0, 0))] * (2 * len(orders)),
            scratch_shapes=[pltpu.VMEM(g_shape, f32)],
        ),
        out_shape=[sd(shape, bf16)] * (2 * len(orders)),
        compiler_params=params(),
        cost_estimate=cost(3e9),
        name="keep_" + kind,
    )(me, *args, got)


def unpack_kernel(kind, colors, me, *refs):
    ins = refs[: 4 * colors]
    n_out = 4 if kind == "attn" else 1
    outs = refs[4 * colors : 4 * colors + n_out]
    buf, sem = refs[4 * colors + n_out :]
    size = HALF // colors

    def copy(step, slot):
        chunk = step ^ me[1]
        if kind == "outer":
            return [(None, pltpu.make_async_copy(buf.at[slot], outs[0].at[ds(chunk * CHUNK, CHUNK), :], sem.at[slot]))]
        if kind == "inner":
            return [(None, pltpu.make_async_copy(buf.at[slot], outs[0].at[:, ds(chunk * CHUNK, CHUNK)], sem.at[slot]))]
        return [
            (chunk // 2 == m, pltpu.make_async_copy(buf.at[slot], outs[m].at[:, ds((chunk % 2) * CHUNK, CHUNK)], sem.at[slot]))
            for m in range(4)
        ]

    def each(step, slot, act):
        for cond, one in copy(step, slot):
            if cond is None:
                act(one)
            else:
                pl.when(cond)(functools.partial(act, one))

    for step in range(8):
        slot = step % 2
        if step >= 2:
            each(step - 2, slot, lambda one: one.wait())
        for half in range(2):
            place = (half ^ me[0]) * CHUNK
            for n in range(colors):
                own, got = ins[4 * n + 2 * half : 4 * n + 2 * half + 2]
                order = ORDER_OF[n]
                src = got if bit(step, order[0]) else own
                for t in range(2):
                    where = bit(step, order[1]) * 4 + bit(step, order[2]) * 2 + t
                    row = (t ^ me[2]) * HALF + n * size
                    value = src[where].astype(f32)
                    if kind == "outer":
                        buf[slot, ds(row, size, 32), ds(place, CHUNK)] = value
                    else:
                        buf[slot, ds(place + row, size, 32), :] = value
        each(step, slot, lambda one: one.start())
    for step in (6, 7):
        each(step, step % 2, lambda one: one.wait())


ORDER_OF = ("xyab", "yxab", "axyb")


def unpack(kind, me, pieces):
    colors = len(pieces) // 4
    width = 2 * CHUNK
    if kind == "outer":
        out_shape = [sd((8 * CHUNK, width), f32)]
    elif kind == "inner":
        out_shape = [sd((width, 8 * CHUNK), f32)]
    else:
        out_shape = [sd((width, width), f32)] * 4
    buf = (2, CHUNK, width) if kind == "outer" else (2, width, CHUNK)
    return pl.pallas_call(
        functools.partial(unpack_kernel, kind, colors),
        in_specs=[SMEM] + [VMEM] * (4 * colors),
        out_specs=[HBM] * len(out_shape),
        out_shape=out_shape,
        scratch_shapes=[pltpu.VMEM(buf, f32), pltpu.SemaphoreType.DMA((2,))],
        compiler_params=params(),
        cost_estimate=cost(4e9),
        name="unpack_" + kind,
    )(me, *pieces)


SMALL_ROWS = (6, 7, 5, 3, 4, 8, 2, 0, 1)


def small_kernel(parts, *outs):
    width = parts.shape[1]
    total = jnp.sum(parts[...].reshape(parts.shape[0] // 16, 16, width), 0)
    for at, out in zip(SMALL_ROWS, outs):
        for n in range(out.shape[0] // width):
            out[pl.ds(n * width, width)] = total[at + n : at + n + 1, :].reshape(width)


def small_call(parts, ff):
    width = parts.shape[1]
    sizes = [ff if at == 8 else width for at in SMALL_ROWS]
    return pl.pallas_call(
        small_kernel,
        in_specs=[VMEM],
        out_specs=[VMEM] * 9,
        out_shape=[sd((n,), f32) for n in sizes],
        compiler_params=params(),
        cost_estimate=cost(2e9),
        name="vectors",
    )(parts)


AXES = ("dp", "seq")
DP_BIT = {"x": 0, "y": 1, "a": 2, "b": 3}


def swap(value, name):
    dp = lax.axis_size("dp")
    seq = lax.axis_size("seq")
    flip = 1 if name == "c" else seq << (name if isinstance(name, int) else DP_BIT[name])
    return lax.ppermute(value, AXES, [(i, i ^ flip) for i in range(dp * seq)])


def after(value, *earlier):
    return lax.optimization_barrier((value,) + earlier)[0]


def add_halves(keep, got):
    half = keep.shape[0] // 2
    return keep[:half] + got[:half], keep[half:] + got[half:]


def gather(own, order):
    for n, name in enumerate(reversed(order)):
        got = swap(own, name)
        if n + 1 < len(order):
            own = jnp.concatenate([own, got])
    return own, got


def finish(own):
    for extra in range(4, lax.axis_size("dp").bit_length() - 1):
        own = own + swap(own, extra)
    return own


RS_ORDERS = {"outer": ("xyab",), "inner": ("axyb",), "attn": ORDER_OF}


class Line:
    def __init__(self):
        self.last = ()

    def __call__(self, value):
        return lax.optimization_barrier((value,) + self.last)[0]

    def done(self, *values):
        self.last = values


def rows_of(value, start, stop):
    return value[:, start:stop]


class One:
    def __init__(self, line, blocks, order):
        self.line, self.order, self.level = line, order, 0
        self.keep = blocks[0]
        self.got = swap(blocks[1], order[0])

    def step(self):
        got = self.line(self.got)
        self.level += 1
        if self.level == 4:
            self.keep = self.keep + got
            self.line.done(self.keep)
            return finish(self.keep[0])
        self.keep, send = add_halves(self.keep, got)
        self.line.done(self.keep, send)
        self.got = swap(send, self.order[self.level])


class Three:
    def __init__(self, line, blocks):
        self.line = line
        self.keep = dict(zip("ABC", blocks[0::2]))
        self.got = {n: swap(blocks[2 * i + 1], ORDER_OF[i][0]) for i, n in enumerate("ABC")}

    def first(self, n):
        got = self.line(self.got[n])
        self.keep[n], send = add_halves(self.keep[n], got)
        self.line.done(self.keep[n], send)
        self.got[n] = swap(send, ORDER_OF["ABC".index(n)][1])

    def join(self):
        gots = [self.line(self.got[n]) for n in "AB"]
        pairs = [add_halves(self.keep[n], got) for n, got in zip("AB", gots)]
        self.keep["AB"], send = [jnp.concatenate(v, 1) for v in zip(*pairs)]
        self.line.done(self.keep["AB"], send)
        self.got["AB"] = swap(send, "a")

    def second(self):
        got = self.line(self.got["C"])
        self.keep["C"], send = add_halves(self.keep["C"], got)
        self.line.done(self.keep["C"], send)
        self.got["C"] = swap(send, ORDER_OF[2][2])

    def last(self):
        gots = [self.line(self.got[n]) for n in ("AB", "C")]
        pairs = [add_halves(self.keep[n], got) for n, got in zip(("AB", "C"), gots)]
        self.keep, send = [jnp.concatenate(v, 1) for v in zip(*pairs)]
        self.line.done(self.keep, send)
        self.got = swap(send, "b")

    def end(self):
        own = self.keep + self.line(self.got)
        self.line.done(own)
        return finish(own[0])


class Gather:
    def __init__(self, line, own):
        self.line = line
        self.own = own[None]
        self.got = swap(self.own, "b")
        self.pieces = {}

    def first(self):
        both_parts = jnp.concatenate([self.own, self.line(self.got)])
        size = both_parts.shape[1] // 3
        self.own = {"AB": both_parts[:, : 2 * size], "C": both_parts[:, 2 * size :]}
        self.line.done(*self.own.values())
        self.got = {"AB": swap(self.own["AB"], "a"), "C": swap(self.own["C"], ORDER_OF[2][2])}

    def second(self):
        four = jnp.concatenate([self.own["AB"], self.line(self.got["AB"])])
        size = four.shape[1] // 2
        self.own["A"], self.own["B"] = four[:, :size], four[:, size:]
        self.line.done(self.own["A"], self.own["B"])
        for n in "AB":
            self.got[n] = swap(self.own[n], ORDER_OF["ABC".index(n)][1])

    def third(self):
        self.own["C"] = jnp.concatenate([self.own["C"], self.line(self.got["C"])])
        self.line.done(self.own["C"])
        self.got["C"] = swap(self.own["C"], ORDER_OF[2][1])

    def fourth(self, n):
        own = jnp.concatenate([self.own[n], self.line(self.got[n])])
        self.line.done(own)
        self.got[n] = swap(own, ORDER_OF["ABC".index(n)][0])
        self.pieces[n] = [own, None, swap(own, "c"), None]

    def last(self, n):
        got = self.got[n]
        self.pieces[n][1] = got
        self.pieces[n][3] = swap(got, "c")

    def all(self):
        return [v for n in "ABC" for v in self.pieces[n]]


def body(chains_in, lengths, d_out, w_query, b_query, w_key, w_value, b_value, w_output, b_output, gain_one, shift_one,
         w_inner, b_inner, w_outer, b_outer, gain_two, shift_two):
    seqs, length, width = chains_in.shape
    rows = seqs * length
    place = lax.axis_index("dp") * 2 + lax.axis_index("seq")
    me = (place >> jnp.array([0, 1, 4], jnp.int32)) & jnp.array([1, 7, 1], jnp.int32)
    x = chains_in.reshape(rows, width)
    line = Line()
    lse, small2, q, k, v, mixed, xhat, rstd, fin, out, dffn, hid, slope, send = forward(
        lengths, me, (b_query, b_value, b_output, gain_one, shift_one, b_inner, b_outer, gain_two, shift_two),
        (x, w_query, w_key, w_value, w_output, w_inner, w_outer, d_out.reshape(rows, width)),
    )
    got1 = swap(send, "c")
    dpre, send, small1 = pre_call(me, dffn, w_outer, slope, fin, small2)
    got2 = swap(send, "c")
    line.done(dpre)
    blocks = grad_keep("outer", me, (hid, dffn), line(got1), RS_ORDERS["outer"])
    line.done(*blocks)
    r1 = One(line, blocks, "xyab")
    blocks = grad_keep("inner", me, (fin, dpre), line(got2), RS_ORDERS["inner"])
    line.done(*blocks)
    r2 = One(line, blocks, "axyb")
    small, dh1, d, send = bwd_call(
        lengths, me, gain_one, small1, line(dpre), w_inner, (dffn, xhat, rstd, w_output, q, k, v, lse, x, mixed)
    )
    line.done(dh1, d, send)
    r1.step()
    r2.step()
    got3 = swap(line(send), "c")
    d_x = dx_call(line(dh1), d, w_query, w_key, w_value)
    line.done(d_x)
    blocks = grad_keep("attn", me, (x, mixed, d), line(got3), RS_ORDERS["attn"])
    line.done(*blocks)
    r3 = Three(line, blocks)
    r1.step()
    r2.step()
    for n in "ABC":
        r3.first(n)
    r1.step()
    r2.step()
    r3.join()
    r3.second()
    g1 = Gather(line, r1.step())
    g2 = Gather(line, r2.step())
    r3.last()
    g1.first()
    g2.first()
    g3 = Gather(line, r3.end())
    for g in (g1, g2):
        g.second()
        g.third()
    g3.first()
    for n in "ABC":
        g1.fourth(n)
    for n in "ABC":
        g2.fourth(n)
    g3.second()
    g3.third()
    for n in "ABC":
        g1.last(n)
    for n in "ABC":
        g3.fourth(n)
    for n in "ABC":
        g2.last(n)
    for n in "ABC":
        g3.last(n)
    (d_w_outer,) = unpack("outer", me, g1.all())
    (d_w_inner,) = unpack("inner", me, g2.all())
    d_w_query, d_w_key, d_w_value, d_w_output = unpack("attn", me, g3.all())
    vec = small_call(lax.all_gather(small, AXES, axis=0, tiled=True), w_inner.shape[1])
    return (
        out.reshape(seqs, length, width), d_x.reshape(seqs, length, width),
        d_w_query, vec[0], d_w_key, d_w_value, vec[1], d_w_output, vec[2], vec[3], vec[4],
        d_w_inner, vec[5], d_w_outer, vec[6], vec[7], vec[8],
    )


def solution(mesh):
    rows = P(AXES, None, None)
    return jax.shard_map(
        body, mesh=mesh, in_specs=(rows, P(AXES), rows) + (P(),) * 15, out_specs=(rows, rows) + (P(),) * 15, check_vma=False
    )
```

```python
import functools
import math
import jax
import jax.numpy as jnp
from jax import lax
from jax.experimental import pallas as pl
from jax.experimental.pallas import tpu as pltpu
from jax.sharding import PartitionSpec as P

H = 12
EPS = 1e-12
f32 = jnp.float32
bf16 = jnp.bfloat16
sd = jax.ShapeDtypeStruct
HBM = pl.BlockSpec(memory_space=pl.ANY)
VMEM = pl.BlockSpec(memory_space=pltpu.VMEM)
SMEM = pl.BlockSpec(memory_space=pltpu.SMEM)
LIMIT = 60 * 1024 * 1024
CHUNK = 384
HALF = CHUNK // 2


def params():
    return pltpu.CompilerParams(vmem_limit_bytes=LIMIT)


def cost(flops, nbytes=1 << 20):
    return pl.CostEstimate(flops=int(flops), transcendentals=0, bytes_accessed=int(nbytes))


def nn(a, b):
    return lax.dot_general(a, b, (((1,), (0,)), ((), ())), preferred_element_type=f32)


def nt(a, b):
    return lax.dot_general(a, b, (((1,), (1,)), ((), ())), preferred_element_type=f32)


def tn(a, b):
    return lax.dot_general(a, b, (((0,), (0,)), ((), ())), preferred_element_type=f32)


def row_mean(v):
    return jnp.mean(v, -1, keepdims=True)


def ds(start, size, align=None):
    return pl.ds(pl.multiple_of(start, align or size), size)


FWD_IN = ("x", "wq", "wk", "wv", "wo", "wi", "w2", "dout")
FWD_OUT = ("q", "k", "v", "mixed", "xhat", "rstd", "fin", "out", "dffn")


def row(ref):
    return ref[...].reshape(1, ref.shape[0])


def both(low, v):
    zero = jnp.zeros_like(v)
    return jnp.concatenate([jnp.where(low, v, zero), jnp.where(low, zero, v)], 0)


def pairs_of(width, size):
    return [slice(2 * size * p, 2 * size * (p + 1)) for p in range(width // (2 * size))]


def attention(lens, q, k, v, mixed, lse):
    rows, width = q.shape
    seqs = lens.shape[0]
    length = rows // seqs
    size = width // H
    low = lax.broadcasted_iota(jnp.int32, (length, 2 * size), 1) < size
    pos = lax.broadcasted_iota(jnp.int32, (2, length, 1), 1)

    def chain(s, _):
        r = ds(s * length, length, 32)
        live = pos < lens[s]
        cols = pairs_of(width, size)
        scores = [nt(both(low, k[r, c]), q[r, c]) for c in cols]
        for p, c in enumerate(cols):
            st = jnp.where(live, scores[p].reshape(2, length, length), -1e9)
            top = jnp.max(st, 1, keepdims=True)
            e = jnp.exp(st - top)
            total = jnp.sum(e, 1, keepdims=True)
            lse[s, pl.ds(2 * p, 2), :] = (top + jnp.log(total)).reshape(2, length)
            prob = (e * (1.0 / total)).astype(bf16).reshape(2 * length, length)
            mixed[r, c] = tn(prob, both(low, v[r, c])).astype(bf16)
        return 0

    lax.fori_loop(0, seqs, chain, 0)


SPLIT = 1
PIECE = HALF // SPLIT


def put_send(outs, grad, base, chunk0, me, rows_are_chunks):
    size = grad.shape[0 if rows_are_chunks else 1]
    for i in range(size // CHUNK):
        for t in range(2):
            if rows_are_chunks:
                value = grad[i * CHUNK + t * HALF : i * CHUNK + (t + 1) * HALF, :]
            else:
                value = grad[t * HALF : (t + 1) * HALF, i * CHUNK : (i + 1) * CHUNK]
            value = value.astype(bf16)
            for n, out in enumerate(outs):
                out[((chunk0 + i) ^ me[1]) * 2 + (t ^ me[2]) - base] = value[n * PIECE : (n + 1) * PIECE]


def fwd_kernel(*refs):
    lens, me = refs[:2]
    bq, bv, bo, g1, s1, bi, b2, g2, s2 = refs[2:11]
    src = dict(zip(FWD_IN, refs[11:19]))
    lse, small = refs[19:21]
    dst = dict(zip(FWD_OUT, refs[21:30]))
    hid_h, slope_h = refs[30:32]
    send_h = refs[32 : 32 + SPLIT]
    rest = refs[32 + SPLIT :]
    vin = dict(zip(FWD_IN, rest[:8]))
    vout = dict(zip(FWD_OUT, rest[8:17]))
    hid, slope = rest[17:19]
    send = rest[19 : 19 + SPLIT]
    acc, sem_in, sem_out, sem_ff, sem_send = rest[19 + SPLIT :]
    rows, width = vin["x"].shape
    ff = vin["wi"].shape[1]
    seqs = lens.shape[0]
    length = rows // seqs

    def load(name):
        return pltpu.make_async_copy(src[name], vin[name], sem_in.at[FWD_IN.index(name)])

    def store(name):
        return pltpu.make_async_copy(vout[name], dst[name], sem_out.at[FWD_OUT.index(name)])

    x, q, k, v, mixed = vin["x"], vout["q"], vout["k"], vout["v"], vout["mixed"]
    for name in ("x", "wq", "wk"):
        load(name).start()
    load("x").wait()
    load("wq").wait()
    load("wv").start()
    load("wo").start()
    q[...] = ((nn(x[...], vin["wq"][...]) + row(bq)).astype(bf16).astype(f32) * 0.125).astype(bf16)
    store("q").start()
    load("wk").wait()
    load("wi").start()
    k[...] = nn(x[...], vin["wk"][...]).astype(bf16)
    store("k").start()
    load("wv").wait()
    load("w2").start()
    load("dout").start()
    v[...] = (nn(x[...], vin["wv"][...]) + row(bv)).astype(bf16)
    store("v").start()
    attention(lens, q, k, v, mixed, lse)
    store("mixed").start()
    load("wo").wait()
    xhat, rstd, fin = vout["xhat"], vout["rstd"], vout["fin"]
    acc[...] = nn(mixed[...], vin["wo"][...])
    R = length
    gain1, shift1, bias_o = row(g1), row(s1), row(bo)

    def norm_one(n, _):
        r = ds(n * R, R, 32)
        h = acc[r, :] + bias_o + x[r, :].astype(f32)
        centre = h - row_mean(h)
        scale = lax.rsqrt(row_mean(centre * centre) + EPS)
        unit = centre * scale
        xhat[r, :] = unit
        rstd[r, :] = scale
        fin[r, :] = (unit * gain1 + shift1).astype(bf16)
        return 0

    lax.fori_loop(0, rows // R, norm_one, 0)
    store("rstd").start()
    store("fin").start()
    store("xhat").start()
    wi, w2 = vin["wi"], vin["w2"]
    load("wi").wait()
    load("w2").wait()
    RB = 320
    part_ff = ff // width

    def ff_copies(n):
        c = ds(n * width, width)
        return (
            pltpu.make_async_copy(hid.at[:, c], hid_h.at[:, c], sem_ff.at[0, n]),
            pltpu.make_async_copy(slope.at[:, c], slope_h.at[:, c], sem_ff.at[1, n]),
        )

    def feed(n, _):
        c = ds(n * width, width)
        bias_i = bi[ds(n * width, width)].reshape(1, width)
        for i in range(rows // RB):
            r = slice(i * RB, (i + 1) * RB)
            u = nn(fin[r, :], wi[:, c]) + bias_i
            cdf = 0.5 * lax.erf(u * 0.7071067811865476) + 0.5
            hid[r, c] = (u * cdf).astype(bf16)
            slope[r, c] = (cdf + u * jnp.exp(-0.5 * (u * u)) * 0.3989422804014327).astype(bf16)
            part = nn(hid[r, c], w2[c, :])
            acc[r, :] = jnp.where(n == 0, part, acc[r, :] + part)
        for one in ff_copies(n):
            one.start()
        return 0

    lax.fori_loop(0, part_ff, feed, 0)
    load("dout").wait()
    dout, out, dffn = vin["dout"], vout["out"], vout["dffn"]
    small[...] = jnp.zeros_like(small)
    gain2, shift2, bias_2 = row(g2), row(s2), row(b2)
    pos = lax.broadcasted_iota(jnp.int32, (R, 1), 0)

    def norm_two(n, _):
        r = ds(n * R, R, 32)
        keep = jnp.where(pos < lens[n], 1.0, 0.0).astype(f32)
        h = xhat[r, :] * gain1 + shift1 + (acc[r, :] + bias_2).astype(bf16).astype(f32)
        centre = h - row_mean(h)
        scale = lax.rsqrt(row_mean(centre * centre) + EPS)
        unit = centre * scale
        out[r, :] = ((unit * gain2 + shift2) * keep).astype(bf16)
        g = dout[r, :].astype(f32) * keep
        e = g * gain2
        low = (scale * (e - row_mean(e) - unit * row_mean(e * unit))).astype(bf16)
        dffn[r, :] = low
        small[0:1, :] += jnp.sum(g * unit, 0, keepdims=True)
        small[1:2, :] += jnp.sum(g, 0, keepdims=True)
        small[2:3, :] += jnp.sum(low.astype(f32), 0, keepdims=True)
        return 0

    lax.fori_loop(0, seqs, norm_two, 0)
    store("dffn").start()
    store("out").start()
    far = ds((1 - me[0]) * CHUNK, CHUNK)

    def send_copies(n):
        part = pl.ds(4 * (n ^ (me[1] >> 1)), 4)
        return [
            pltpu.make_async_copy(a.at[part], b.at[part], sem_send.at[i, n]) for i, (a, b) in enumerate(zip(send, send_h))
        ]

    def grads(n, _):
        put_send(send, tn(hid[:, ds(n * width, width)], dffn[:, far]), 0, 2 * n, me, True)
        for one in send_copies(n):
            one.start()
        return 0

    lax.fori_loop(0, part_ff, grads, 0)
    for name in FWD_OUT:
        store(name).wait()
    for n in range(part_ff):
        for one in ff_copies(n) + tuple(send_copies(n)):
            one.wait()


def forward(lens, me, vectors, arrays):
    rows, width = arrays[0].shape
    ff = arrays[5].shape[1]
    seqs = lens.shape[0]
    like = lambda shape, dtype=bf16: sd(shape, dtype)
    thin = like((rows, width))
    outs = [thin, thin, thin, thin, like((rows, width), f32), like((rows, 1), f32), thin, thin, thin]
    wide = [like((rows, ff)), like((rows, ff))] + [like((16, PIECE, CHUNK))] * SPLIT
    dma = pltpu.SemaphoreType.DMA
    return pl.pallas_call(
        fwd_kernel,
        in_specs=[SMEM, SMEM] + [VMEM] * 9 + [HBM] * 8,
        out_specs=[VMEM, VMEM] + [HBM] * (11 + SPLIT),
        out_shape=[like((seqs, H, rows // seqs), f32), like((8, width), f32)] + outs + wide,
        scratch_shapes=[pltpu.VMEM(a.shape, a.dtype) for a in arrays]
        + [pltpu.VMEM(o.shape, o.dtype) for o in outs + wide]
        + [pltpu.VMEM((rows, width), f32), dma((8,)), dma((9,)), dma((2, ff // width)), dma((SPLIT, ff // width))],
        compiler_params=params(),
        cost_estimate=cost(28e9),
        name="forward",
    )(lens, me, *vectors, *arrays)


def pre_kernel(me, dffn, w2, slope, fin, small2, dpre_o, small, *send_o):
    p = pl.program_id(0)
    n = p ^ (me[1] >> 1)

    @pl.when(p == 0)
    def _():
        small[0:8, :] = small2[...]
        small[8:16, :] = jnp.zeros((8, small.shape[1]), f32)

    d = (nt(dffn[...], w2[...]) * slope[...].astype(f32)).astype(bf16)
    dpre_o[...] = d
    small[pl.ds(8 + n, 1), :] = jnp.sum(d.astype(f32), 0, keepdims=True)
    put_send(send_o, tn(fin[...], dpre_o[...]), 4 * p, 2 * n, me, False)


def pre_call(me, dffn, w2, slope, fin, small2):
    rows, width = dffn.shape
    ff = w2.shape[0]
    at = lambda p, me: p ^ (me[1] >> 1)
    return pl.pallas_call(
        pre_kernel,
        grid_spec=pltpu.PrefetchScalarGridSpec(
            num_scalar_prefetch=1,
            grid=(ff // width,),
            in_specs=[
                pl.BlockSpec((rows, width), lambda p, me: (0, 0)),
                pl.BlockSpec((width, width), lambda p, me: (at(p, me), 0)),
                pl.BlockSpec((rows, width), lambda p, me: (0, at(p, me))),
                pl.BlockSpec((rows, CHUNK), lambda p, me: (0, 1 - me[0])),
                pl.BlockSpec((8, width), lambda p, me: (0, 0)),
            ],
            out_specs=[
                pl.BlockSpec((rows, width), lambda p, me: (0, at(p, me))),
                pl.BlockSpec((16, width), lambda p, me: (0, 0)),
            ]
            + [pl.BlockSpec((4, PIECE, CHUNK), lambda p, me: (p, 0, 0))] * SPLIT,
        ),
        out_shape=[sd((rows, ff), bf16), sd((16, width), f32)] + [sd((16, PIECE, CHUNK), bf16)] * SPLIT,
        compiler_params=params(),
        cost_estimate=cost(8e9),
        name="pre_bwd",
    )(me, dffn, w2, slope, fin, small2)


def attention_bwd(lens, q, k, v, dm, lse, d, small):
    rows, width = q.shape
    seqs = lens.shape[0]
    length = rows // seqs
    size = width // H
    low = lax.broadcasted_iota(jnp.int32, (length, 2 * size), 1) < size
    pos = lax.broadcasted_iota(jnp.int32, (2, length, 1), 1)

    def chain(s, _):
        r = ds(s * length, length, 32)
        live = pos < lens[s]
        cols = pairs_of(width, size)
        first = []
        for c in cols:
            k2 = both(low, k[r, c])
            first.append((k2, nt(k2, q[r, c]), nt(both(low, v[r, c]), dm[r, c])))
        for p, c in enumerate(cols):
            k2, st, dprob = first[p]
            st = jnp.where(live, st.reshape(2, length, length), -1e9)
            dprob = dprob.reshape(2, length, length)
            prob = jnp.exp(st - lse[s, pl.ds(2 * p, 2), :].reshape(2, 1, length))
            delta = jnp.sum(prob * dprob, 1, keepdims=True)
            dst = (prob * (dprob - delta)).astype(bf16).reshape(2 * length, length)
            dv = nn(prob.astype(bf16).reshape(2 * length, length), dm[r, c])
            dk = nn(dst, q[r, c])
            dq = (tn(dst, k2) * 0.125).astype(bf16)
            dv = jnp.where(low, dv[:length], dv[length:]).astype(bf16)
            d[r, c] = dq
            d[r, slice(width + c.start, width + c.stop)] = jnp.where(low, dk[:length], dk[length:]).astype(bf16)
            d[r, slice(2 * width + c.start, 2 * width + c.stop)] = dv
            small[6:7, c] += jnp.sum(dq.astype(f32), 0, keepdims=True)
            small[7:8, c] += jnp.sum(dv.astype(f32), 0, keepdims=True)
        return 0

    lax.fori_loop(0, seqs, chain, 0)


MID_IN = ("dffn", "xhat", "rstd", "wo")


def mid_kernel(*refs):
    g1, small1, dpre_h, wi_h = refs[:4]
    src = dict(zip(MID_IN, refs[4:8]))
    small, dh1_h, dob_h, dm_h = refs[8:12]
    dpre, wi = refs[12:14]
    vin = dict(zip(MID_IN, refs[14:18]))
    dh1, dob, dm, acc, sem_ff, sem_in, sem_out = refs[18:]
    rows, width = acc.shape
    part_ff = dpre.shape[1] // width
    R = 160

    def load(name):
        return pltpu.make_async_copy(src[name], vin[name], sem_in.at[MID_IN.index(name)])

    def ff_copies(n):
        c = slice(n * width, (n + 1) * width)
        return (
            pltpu.make_async_copy(dpre_h.at[:, c], dpre.at[:, c], sem_ff.at[0, n]),
            pltpu.make_async_copy(wi_h.at[:, c], wi.at[:, c], sem_ff.at[1, n]),
        )

    for n in range(part_ff):
        for one in ff_copies(n):
            one.start()
    for name in MID_IN:
        load(name).start()
    for n in range(part_ff):
        c = slice(n * width, (n + 1) * width)
        for one in ff_copies(n):
            one.wait()
        part = nt(dpre[:, c], wi[:, c])
        acc[...] = part if n == 0 else acc[...] + part
    small[...] = small1[...]
    gain1 = row(g1)
    dffn, xhat, rstd = vin["dffn"], vin["xhat"], vin["rstd"]
    for name in ("dffn", "xhat", "rstd"):
        load(name).wait()

    def norm_one(i, _):
        r = ds(i * R, R, 32)
        g = dffn[r, :].astype(f32) + acc[r, :].astype(bf16).astype(f32)
        unit = xhat[r, :]
        e = g * gain1
        v = rstd[r, :] * (e - row_mean(e) - unit * row_mean(e * unit))
        dh1[r, :] = v
        low = v.astype(bf16)
        dob[r, :] = low
        small[3:4, :] += jnp.sum(g * unit, 0, keepdims=True)
        small[4:5, :] += jnp.sum(g, 0, keepdims=True)
        small[5:6, :] += jnp.sum(low.astype(f32), 0, keepdims=True)
        return 0

    lax.fori_loop(0, rows // R, norm_one, 0)
    stores = [pltpu.make_async_copy(a, b, sem_out.at[n]) for n, (a, b) in enumerate(((dh1, dh1_h), (dob, dob_h), (dm, dm_h)))]
    stores[0].start()
    stores[1].start()
    load("wo").wait()
    dm[...] = nt(dob[...], vin["wo"][...]).astype(bf16)
    stores[2].start()
    for one in stores:
        one.wait()


def mid_call(g1, small1, dpre, wi, arrays):
    rows, width = arrays[0].shape
    ff = wi.shape[1]
    dma = pltpu.SemaphoreType.DMA
    vm = lambda a: pltpu.VMEM(a.shape, a.dtype)
    outs = [sd((rows, width), f32), sd((rows, width), bf16), sd((rows, width), bf16)]
    return pl.pallas_call(
        mid_kernel,
        in_specs=[VMEM, VMEM] + [HBM] * 6,
        out_specs=[VMEM] + [HBM] * 3,
        out_shape=[sd((16, width), f32)] + outs,
        scratch_shapes=[vm(dpre), vm(wi)] + [vm(a) for a in arrays] + [vm(o) for o in outs]
        + [pltpu.VMEM((rows, width), f32), dma((2, ff // width)), dma((4,)), dma((3,))],
        compiler_params=params(),
        cost_estimate=cost(10e9),
        name="mid_bwd",
    )(g1, small1, dpre, wi, *arrays)


ATT_IN = ("q", "k", "v", "dm", "lse", "x", "mixed", "dob")


def att_kernel(*refs):
    lens, me, small1 = refs[:3]
    src = dict(zip(ATT_IN, refs[3:11]))
    small, d_h = refs[11:13]
    send_h = refs[13 : 13 + SPLIT]
    rest = refs[13 + SPLIT :]
    vin = dict(zip(ATT_IN, rest[:8]))
    d = rest[8]
    send = rest[9 : 9 + SPLIT]
    sem_in, sem_out, sem_send = rest[9 + SPLIT :]
    width = d.shape[1] // 4

    def load(name):
        if name == "dob":
            return pltpu.make_async_copy(src[name], d.at[:, 3 * width : 4 * width], sem_in.at[7])
        return pltpu.make_async_copy(src[name], vin[name], sem_in.at[ATT_IN.index(name)])

    for name in ATT_IN:
        load(name).start()
    small[...] = small1[...]
    for name in ("q", "k", "v", "dm", "lse"):
        load(name).wait()
    attention_bwd(lens, vin["q"], vin["k"], vin["v"], vin["dm"], vin["lse"], d, small)
    load("dob").wait()
    d_copy = pltpu.make_async_copy(d, d_h, sem_out.at[0])
    d_copy.start()
    load("x").wait()
    load("mixed").wait()
    far = ds((1 - me[0]) * CHUNK, CHUNK)

    def send_copies(n):
        part = pl.ds(4 * (n ^ (me[1] >> 1)), 4)
        return [
            pltpu.make_async_copy(a.at[part], b.at[part], sem_send.at[i, n]) for i, (a, b) in enumerate(zip(send, send_h))
        ]

    for n in range(4):
        left = vin["mixed" if n == 3 else "x"]
        put_send(send, tn(left[:, far], d[:, n * width : (n + 1) * width]), 0, 2 * n, me, False)
        for one in send_copies(n):
            one.start()
    d_copy.wait()
    for n in range(4):
        for one in send_copies(n):
            one.wait()


def att_call(lens, me, small1, arrays):
    rows, width = arrays[0].shape
    dma = pltpu.SemaphoreType.DMA
    vm = lambda a: pltpu.VMEM(a.shape, a.dtype)
    outs = [sd((rows, 4 * width), bf16)] + [sd((16, PIECE, CHUNK), bf16)] * SPLIT
    return pl.pallas_call(
        att_kernel,
        in_specs=[SMEM, SMEM, VMEM] + [HBM] * 8,
        out_specs=[VMEM] + [HBM] * (1 + SPLIT),
        out_shape=[sd((16, width), f32)] + outs,
        scratch_shapes=[vm(a) for a in arrays[:7]] + [pltpu.VMEM((8, 128), bf16)] + [vm(o) for o in outs]
        + [dma((8,)), dma((1,)), dma((SPLIT, 4))],
        compiler_params=params(),
        cost_estimate=cost(12e9),
        name="att_bwd",
    )(lens, me, small1, *arrays)


def dx_kernel(dh1_h, d_h, wq_h, wk_h, wv_h, o_h, dh1, d, wq, wk, wv, o, sem, sem_out):
    width = dh1.shape[1]
    loads = []
    for n, (w_h, w) in enumerate(((wq_h, wq), (wk_h, wk), (wv_h, wv))):
        c = slice(n * width, (n + 1) * width)
        loads.append(pltpu.make_async_copy(d_h.at[:, c], d.at[:, c], sem.at[2 * n]))
        loads.append(pltpu.make_async_copy(w_h, w, sem.at[2 * n + 1]))
    loads.insert(2, pltpu.make_async_copy(dh1_h, dh1, sem.at[6]))
    for one in loads:
        one.start()
    loads[0].wait()
    loads[1].wait()
    part = nt(d[:, :width], wq[...])
    loads[2].wait()
    o[...] = dh1[...] + part
    loads[3].wait()
    loads[4].wait()
    o[...] = o[...] + nt(d[:, width : 2 * width], wk[...])
    loads[5].wait()
    loads[6].wait()
    half = dh1.shape[0] // 2
    stores = []
    for i in range(2):
        r = slice(i * half, (i + 1) * half)
        o[r, :] = o[r, :] + nt(d[r, 2 * width : 3 * width], wv[...])
        stores.append(pltpu.make_async_copy(o.at[r, :], o_h.at[r, :], sem_out.at[i]))
        stores[i].start()
    for one in stores:
        one.wait()


def dx_call(dh1, d, wq, wk, wv):
    rows, width = dh1.shape
    dma = pltpu.SemaphoreType.DMA
    return pl.pallas_call(
        dx_kernel,
        in_specs=[HBM] * 5,
        out_specs=HBM,
        out_shape=sd((rows, width), f32),
        scratch_shapes=[
            pltpu.VMEM((rows, width), f32), pltpu.VMEM((rows, 3 * width), bf16), pltpu.VMEM(wq.shape, bf16),
            pltpu.VMEM(wq.shape, bf16), pltpu.VMEM(wq.shape, bf16), pltpu.VMEM((rows, width), f32), dma((7,)), dma((2,)),
        ],
        compiler_params=params(),
        cost_estimate=cost(5e9),
        name="dx",
    )(dh1, d, wq, wk, wv)


def bit(value, name):
    return (value >> "xya".index(name)) & 1


def pair_grad(kind, pair, refs):
    if kind == "attn":
        x, mixed, d = refs
        return tn(jnp.where(pair == 3, mixed[...], x[...]), d[...])
    return tn(refs[0][...], refs[1][...])


def keep_kernel(kind, orders, me, *refs):
    p = pl.program_id(0)
    n_in = 3 if kind == "attn" else 2
    gots = refs[n_in : n_in + SPLIT]
    outs = refs[n_in + SPLIT : -1]
    g = refs[-1]
    g[...] = pair_grad(kind, p ^ (me[1] >> 1), refs[:n_in])
    size = HALF // len(orders)
    for i in range(2):
        step = 2 * p + i
        far = ds((i ^ (me[1] & 1)) * CHUNK, CHUNK)
        for t in range(2):
            part = (t ^ me[2]) * HALF
            if kind == "outer":
                grad = g[ds((i ^ (me[1] & 1)) * CHUNK + part, HALF), :]
            else:
                grad = g[ds(part, HALF), far]
            got = jnp.concatenate([v[2 * i + t] for v in gots])
            total = (grad + got.astype(f32)).astype(bf16)
            for n, order in enumerate(orders):
                where = bit(step, order[1]) * 4 + bit(step, order[2]) * 2 + t
                first = bit(step, order[0])
                value = total[n * size : (n + 1) * size]
                if order[0] == "x":
                    outs[2 * n + i][where] = value
                    continue

                @pl.when(first == 0)
                def _():
                    outs[2 * n][where] = value

                @pl.when(first == 1)
                def _():
                    outs[2 * n + 1][where] = value


def grad_specs(kind, rows, flip, pair_of):
    pair = lambda p, me: (0, pair_of(p, me))
    half = lambda p, me: (0, me[0] ^ flip)
    wide = (rows, 2 * CHUNK)
    thin = (rows, CHUNK)
    if kind == "outer":
        return [pl.BlockSpec(wide, pair), pl.BlockSpec(thin, half)]
    if kind == "inner":
        return [pl.BlockSpec(thin, half), pl.BlockSpec(wide, pair)]
    return [pl.BlockSpec(thin, half), pl.BlockSpec(thin, half), pl.BlockSpec(wide, pair)]


def grad_keep(kind, me, args, got, orders):
    rows = args[0].shape[0]
    shape = (8, HALF // len(orders), CHUNK)
    g_shape = (2 * CHUNK, CHUNK) if kind == "outer" else (CHUNK, 2 * CHUNK)
    return pl.pallas_call(
        functools.partial(keep_kernel, kind, orders),
        grid_spec=pltpu.PrefetchScalarGridSpec(
            num_scalar_prefetch=1,
            grid=(4,),
            in_specs=grad_specs(kind, rows, 0, lambda p, me: p ^ (me[1] >> 1))
            + [pl.BlockSpec((4, PIECE, CHUNK), lambda p, me: (p, 0, 0))] * SPLIT,
            out_specs=[pl.BlockSpec(shape, lambda p, me: (0, 0, 0))] * (2 * len(orders)),
            scratch_shapes=[pltpu.VMEM(g_shape, f32)],
        ),
        out_shape=[sd(shape, bf16)] * (2 * len(orders)),
        compiler_params=params(),
        cost_estimate=cost(3e9),
        name="keep_" + kind,
    )(me, *args, *got)


ORDER_OF = ("xyab", "yxab", "axyb")


def unpack_kernel(kind, orders, me, *refs):
    colors = len(orders)
    n_in = 4 * colors
    src = refs[:n_in]
    n_out = 4 if kind == "attn" else 1
    outs = refs[n_in : n_in + n_out]
    ins = refs[n_in + n_out : 2 * n_in + n_out]
    buf, sem_in, sem = refs[2 * n_in + n_out :]
    size = HALF // colors
    slots = buf.shape[0]

    order_in = [n for first in range(2) for n in range(n_in) if n % 2 == first]
    loads = [pltpu.make_async_copy(src[n], ins[n], sem_in.at[n]) for n in range(n_in)]
    for n in order_in:
        loads[n].start()
    waited = set()

    def copies(step):
        chunk = step ^ me[1]
        slot = step % slots
        if kind == "outer":
            return [(None, pltpu.make_async_copy(buf.at[slot], outs[0].at[ds(chunk * CHUNK, CHUNK), :], sem.at[slot]))]
        if kind == "inner":
            return [(None, pltpu.make_async_copy(buf.at[slot], outs[0].at[:, ds(chunk * CHUNK, CHUNK)], sem.at[slot]))]
        return [
            (chunk // 2 == m, pltpu.make_async_copy(buf.at[slot], outs[m].at[:, ds((chunk % 2) * CHUNK, CHUNK)], sem.at[slot]))
            for m in range(4)
        ]

    def each(step, act):
        for cond, one in copies(step):
            if cond is None:
                act(one)
            else:
                pl.when(cond)(functools.partial(act, one))

    for step in range(8):
        slot = step % slots
        if step >= slots:
            each(step - slots, lambda one: one.wait())
        for half in range(2):
            place = (half ^ me[0]) * CHUNK
            for n in range(colors):
                order = orders[n]
                at = 4 * n + 2 * half + bit(step, order[0])
                if at not in waited:
                    waited.add(at)
                    loads[at].wait()
                for t in range(2):
                    where = bit(step, order[1]) * 4 + bit(step, order[2]) * 2 + t
                    start = (t ^ me[2]) * HALF + n * size
                    value = ins[at][where].astype(f32)
                    if kind == "outer":
                        buf[slot, ds(start, size, 32), ds(place, CHUNK)] = value
                    else:
                        buf[slot, ds(place + start, size, 32), :] = value
        each(step, lambda one: one.start())
    for step in range(8 - slots, 8):
        each(step, lambda one: one.wait())


def unpack(kind, me, pieces, orders):
    colors = len(orders)
    width = 2 * CHUNK
    if kind == "outer":
        out_shape = [sd((8 * CHUNK, width), f32)]
    elif kind == "inner":
        out_shape = [sd((width, 8 * CHUNK), f32)]
    else:
        out_shape = [sd((width, width), f32)] * 4
    buf = (4, CHUNK, width) if kind == "outer" else (4, width, CHUNK)
    dma = pltpu.SemaphoreType.DMA
    return pl.pallas_call(
        functools.partial(unpack_kernel, kind, orders),
        in_specs=[SMEM] + [HBM] * (4 * colors),
        out_specs=[HBM] * len(out_shape),
        out_shape=out_shape,
        scratch_shapes=[pltpu.VMEM(v.shape, v.dtype) for v in pieces]
        + [pltpu.VMEM(buf, f32), dma((4 * colors,)), dma((4,))],
        compiler_params=params(),
        cost_estimate=cost(4e9),
        name="unpack_" + kind,
    )(me, *pieces)


SMALL_ROWS = (6, 7, 5, 3, 4, 8, 2, 0, 1)


def small_kernel(total, *outs):
    half = total.shape[1]
    for at, out in zip(SMALL_ROWS, outs):
        for n in range(out.shape[0] // half):
            line = at + n // 2 + (n % 2) * (total.shape[0] // 2)
            out[pl.ds(n * half, half)] = total[line : line + 1, :].reshape(half)


def small_call(total, ff):
    width = 2 * total.shape[1]
    sizes = [ff if at == 8 else width for at in SMALL_ROWS]
    return pl.pallas_call(
        small_kernel,
        in_specs=[VMEM],
        out_specs=[VMEM] * 9,
        out_shape=[sd((n,), f32) for n in sizes],
        compiler_params=params(),
        cost_estimate=cost(1e9),
        name="vectors",
    )(total)


AXES = ("dp", "seq")
DP_BIT = {"x": 0, "y": 1, "a": 2, "b": 3}


def swap(value, name):
    dp = lax.axis_size("dp")
    seq = lax.axis_size("seq")
    flip = 1 if name == "c" else seq << (name if isinstance(name, int) else DP_BIT[name])
    return lax.ppermute(value, AXES, [(i, i ^ flip) for i in range(dp * seq)])


ORDERS = ("xya", "yax", "axy")


def both_halves(keep, got):
    return keep[0] + got[0], keep[1] + got[1]


def reduction(blocks):
    keeps = [v.reshape((2, 2, 2) + v.shape[1:]) for v in blocks[0::2]]
    sends = [v.reshape((2, 2, 2) + v.shape[1:]) for v in blocks[1::2]]
    for level in range(3):
        gots = yield [(o[level], v) for o, v in zip(ORDERS, sends)]
        if level < 2:
            keeps, sends = zip(*[both_halves(k, g) for k, g in zip(keeps, gots)])
    own = jnp.concatenate([k + g for k, g in zip(keeps, gots)], -2)
    (got,) = yield [("b", own)]
    own = own + jnp.concatenate([got[1:], got[:1]])
    for extra in range(4, lax.axis_size("dp").bit_length() - 1):
        own = own + swap(own, extra)
    size = own.shape[1] // 3
    owns = [own[:, n * size : (n + 1) * size] for n in range(3)]
    for level in (2, 1):
        gots = yield [(o[level], v) for o, v in zip(ORDERS, owns)]
        owns = [jnp.concatenate(v) for v in zip(owns, gots)]
    gots = yield [(o[0], v) for o, v in zip(ORDERS, owns)] + [("c", v) for v in owns]
    near, far = gots[:3], gots[3:]
    others = yield [("c", v) for v in near]
    return [v for four in zip(owns, near, far, others) for v in four]


def vector_sum(small):
    half = small.shape[1] // 2
    value = jnp.concatenate([small[:, :half], small[:, half:]])
    links = ["c"] + list("axyb") + list(range(4, lax.axis_size("dp").bit_length() - 1))
    for link in links:
        sent = value.astype(bf16)
        if isinstance(link, int):
            got = swap(sent, link)
        else:
            (got,) = yield [(link, sent)]
        value = sent.astype(f32) + got.astype(f32)
    return value


def unroll(v):
    return v.reshape((-1, v.shape[-1]))


class Rounds:
    def __init__(self):
        self.flows = {}
        self.results = {}
        self.wanted = {}
        self.mark = ()

    def add(self, name, flow):
        self.flows[name] = flow
        self.wanted[name] = next(flow)

    def hold(self, value):
        return lax.optimization_barrier((value,) + self.mark)[0]

    def begin(self, extra=()):
        self.order = [(name, n) for name in self.wanted for n in range(len(self.wanted[name]))]
        links = {}
        alone = {}
        for name, n in self.order:
            link, value = self.wanted[name][n]
            if link == "c":
                alone[name, n] = value
            else:
                links.setdefault(link, []).append((name, n))
        merged = {}
        for link, keys in links.items():
            values = [self.wanted[k][n][1] for k, n in keys]
            merged[link] = values[0] if len(values) == 1 else jnp.concatenate([unroll(v) for v in values])
        merged, alone, extra = lax.optimization_barrier((merged, alone, tuple(extra)))
        self.mark = tuple(merged.values())
        self.got = {}
        for link in "baxy":
            if link not in links:
                continue
            keys = links[link]
            got = swap(merged[link], link)
            if len(keys) == 1:
                self.got[keys[0]] = got
                continue
            row = 0
            for k, n in keys:
                shape = self.wanted[k][n][1].shape
                count = math.prod(shape[:-1])
                self.got[k, n] = got[row : row + count].reshape(shape)
                row += count
        for key, value in alone.items():
            self.got[key] = swap(value, "c")
        return [swap(v, "c") for v in extra]

    def end(self, *beside):
        got, _ = lax.optimization_barrier((self.got, tuple(beside)))
        for name in list(self.flows):
            if name not in self.wanted or (name, 0) not in got:
                continue
            values = [got[name, n] for n in range(len(self.wanted[name]))]
            try:
                self.wanted[name] = self.flows[name].send(values)
            except StopIteration as stop:
                self.results[name] = stop.value
                del self.flows[name], self.wanted[name]


def body(chains_in, lengths, d_out, w_query, b_query, w_key, w_value, b_value, w_output, b_output, gain_one, shift_one,
         w_inner, b_inner, w_outer, b_outer, gain_two, shift_two):
    seqs, length, width = chains_in.shape
    rows = seqs * length
    place = lax.axis_index("dp") * 2 + lax.axis_index("seq")
    me = (place >> jnp.array([0, 1, 4], jnp.int32)) & jnp.array([1, 7, 1], jnp.int32)
    x = chains_in.reshape(rows, width)
    lse, small2, q, k, v, mixed, xhat, rstd, fin, out, dffn, hid, slope, send = forward(
        lengths, me, (b_query, b_value, b_output, gain_one, shift_one, b_inner, b_outer, gain_two, shift_two),
        (x, w_query, w_key, w_value, w_output, w_inner, w_outer, d_out.reshape(rows, width)),
    )
    rounds = Rounds()
    (got,) = rounds.begin([send])
    dpre, small1, send = pre_call(me, dffn, w_outer, slope, fin, small2)
    got, send = lax.optimization_barrier((got, send))
    (got_i,) = rounds.begin([send])
    blocks = grad_keep("outer", me, (hid, dffn), (got,), ORDERS)
    rounds.add("outer", reduction(blocks))
    rounds.begin()
    blocks = grad_keep("inner", me, (fin, dpre), (rounds.hold(got_i),), ORDERS)
    rounds.end(*blocks)
    rounds.add("inner", reduction(blocks))
    rounds.begin()
    small, dh1, dob, dm = mid_call(gain_one, small1, rounds.hold(dpre), w_inner, (dffn, xhat, rstd, w_output))
    rounds.end(dh1, dob, dm)
    rounds.begin()
    small, d, send = att_call(lengths, me, small, (q, k, v, rounds.hold(dm), lse, x, mixed, dob))
    rounds.end(d, send)
    rounds.add("vectors", vector_sum(small))
    (got,) = rounds.begin([send])
    blocks = grad_keep("attn", me, (x, mixed, d), (got,), ORDERS)
    rounds.end(*blocks)
    rounds.add("attn", reduction(blocks))
    rounds.begin()
    d_x = dx_call(rounds.hold(dh1), d, w_query, w_key, w_value)
    rounds.end(d_x)
    for _ in range(3):
        rounds.begin()
        rounds.end()
    rounds.begin()
    vec = small_call(rounds.hold(rounds.results["vectors"]), w_inner.shape[1])
    rounds.end(vec[0])
    rounds.begin()
    (d_w_outer,) = unpack("outer", me, rounds.hold(rounds.results["outer"]), ORDERS)
    rounds.end(d_w_outer)
    rounds.begin()
    (d_w_inner,) = unpack("inner", me, rounds.hold(rounds.results["inner"]), ORDERS)
    rounds.end(d_w_inner)
    rounds.begin()
    rounds.end()
    d_w_query, d_w_key, d_w_value, d_w_output = unpack("attn", me, rounds.results["attn"], ORDERS)
    return (
        out.reshape(seqs, length, width), d_x.reshape(seqs, length, width),
        d_w_query, vec[0], d_w_key, d_w_value, vec[1], d_w_output, vec[2], vec[3], vec[4],
        d_w_inner, vec[5], d_w_outer, vec[6], vec[7], vec[8],
    )


def solution(mesh):
    rows = P(AXES, None, None)
    return jax.shard_map(
        body, mesh=mesh, in_specs=(rows, P(AXES), rows) + (P(),) * 15, out_specs=(rows, rows) + (P(),) * 15, check_vma=False
    )
```

```python
import functools
import math
import jax
import jax.numpy as jnp
from jax import lax
from jax.experimental import pallas as pl
from jax.experimental.pallas import tpu as pltpu
from jax.sharding import PartitionSpec as P

H = 12
EPS = 1e-12
f32 = jnp.float32
bf16 = jnp.bfloat16
sd = jax.ShapeDtypeStruct
ANY = pl.BlockSpec(memory_space=pl.ANY)
HBM = pl.BlockSpec(memory_space=pltpu.HBM)
VMEM = pl.BlockSpec(memory_space=pltpu.VMEM)
SMEM = pl.BlockSpec(memory_space=pltpu.SMEM)
CHUNK = 384
HALF = CHUNK // 2


def params(mib=60):
    return pltpu.CompilerParams(vmem_limit_bytes=mib * 1024 * 1024)


def cost(flops, nbytes=1 << 20):
    return pl.CostEstimate(flops=int(flops), transcendentals=0, bytes_accessed=int(nbytes))


def nn(a, b):
    return lax.dot_general(a, b, (((1,), (0,)), ((), ())), preferred_element_type=f32)


def nt(a, b):
    return lax.dot_general(a, b, (((1,), (1,)), ((), ())), preferred_element_type=f32)


def tn(a, b):
    return lax.dot_general(a, b, (((0,), (0,)), ((), ())), preferred_element_type=f32)


def row_mean(v):
    return jnp.mean(v, -1, keepdims=True)


def ds(start, size, align=None):
    return pl.ds(pl.multiple_of(start, align or size), size)


FWD_IN = ("x", "wq", "wk", "wv", "wo", "wi", "w2", "dout")
FWD_OUT = ("q", "k", "v", "mixed", "xhat", "rstd", "fin", "out", "dffn")


def row(ref):
    return ref[...].reshape(1, ref.shape[0])


def both(low, v):
    zero = jnp.zeros_like(v)
    return jnp.concatenate([jnp.where(low, v, zero), jnp.where(low, zero, v)], 0)


def pairs_of(width, size):
    return [slice(2 * size * p, 2 * size * (p + 1)) for p in range(width // (2 * size))]


def attention(lens, q, k, v, mixed, lse):
    rows, width = q.shape
    seqs = lens.shape[0]
    length = rows // seqs
    size = width // H
    low = lax.broadcasted_iota(jnp.int32, (length, 2 * size), 1) < size
    pos = lax.broadcasted_iota(jnp.int32, (2, length, 1), 1)

    def chain(s, _):
        r = ds(s * length, length, 32)
        live = pos < lens[s]
        cols = pairs_of(width, size)
        scores = [nt(both(low, k[r, c]), q[r, c]) for c in cols]
        for p, c in enumerate(cols):
            st = jnp.where(live, scores[p].reshape(2, length, length), -1e9)
            top = jnp.max(st, 1, keepdims=True)
            e = jnp.exp(st - top)
            total = jnp.sum(e, 1, keepdims=True)
            lse[s, pl.ds(2 * p, 2), :] = (top + jnp.log(total)).reshape(2, length)
            prob = (e * (1.0 / total)).astype(bf16).reshape(2 * length, length)
            mixed[r, c] = tn(prob, both(low, v[r, c])).astype(bf16)
        return 0

    lax.fori_loop(0, seqs, chain, 0)


def put_blocks(out, grad, chunk0, me, rows_are_chunks):
    size = grad.shape[0 if rows_are_chunks else 1]
    for i in range(size // CHUNK):
        for t in range(2):
            if rows_are_chunks:
                value = grad[i * CHUNK + t * HALF : i * CHUNK + (t + 1) * HALF, :]
            else:
                value = grad[t * HALF : (t + 1) * HALF, i * CHUNK : (i + 1) * CHUNK]
            out[((chunk0 + i) ^ me[1]) * 2 + (t ^ me[2])] = value.astype(bf16)


def pair_part(n, me):
    return pl.ds(4 * (n ^ (me[1] >> 1)), 4)


def fwd_kernel(*refs):
    lens, me = refs[:2]
    bq, bv, bo, g1, s1, bi, b2, g2, s2 = refs[2:11]
    src = dict(zip(FWD_IN, refs[11:19]))
    lse, small = refs[19:21]
    dst = dict(zip(FWD_OUT, refs[21:30]))
    dpre_h = refs[30]
    block_h = refs[31:35]
    rest = refs[35:]
    vin = dict(zip(FWD_IN, rest[:8]))
    vout = dict(zip(FWD_OUT, rest[8:17]))
    dpre = rest[17]
    block = rest[18:22]
    hid, slope, acc, sem_in, sem_out, sem_ff, sem_block = rest[22:]
    rows, width = vin["x"].shape
    ff = vin["wi"].shape[1]
    seqs = lens.shape[0]
    length = rows // seqs

    def load(name):
        return pltpu.make_async_copy(src[name], vin[name], sem_in.at[FWD_IN.index(name)])

    def store(name):
        return pltpu.make_async_copy(vout[name], dst[name], sem_out.at[FWD_OUT.index(name)])

    x, q, k, v, mixed = vin["x"], vout["q"], vout["k"], vout["v"], vout["mixed"]
    for name in ("x", "wq", "wk"):
        load(name).start()
    load("x").wait()
    load("wq").wait()
    load("wv").start()
    load("wo").start()
    q[...] = ((nn(x[...], vin["wq"][...]) + row(bq)).astype(bf16).astype(f32) * 0.125).astype(bf16)
    store("q").start()
    load("wk").wait()
    load("wi").start()
    k[...] = nn(x[...], vin["wk"][...]).astype(bf16)
    store("k").start()
    load("wv").wait()
    load("w2").start()
    load("dout").start()
    v[...] = (nn(x[...], vin["wv"][...]) + row(bv)).astype(bf16)
    store("v").start()
    attention(lens, q, k, v, mixed, lse)
    store("mixed").start()
    load("wo").wait()
    xhat, rstd, fin = vout["xhat"], vout["rstd"], vout["fin"]
    acc[...] = nn(mixed[...], vin["wo"][...])
    R = length
    gain1, shift1, bias_o = row(g1), row(s1), row(bo)

    def norm_one(n, _):
        r = ds(n * R, R, 32)
        h = acc[r, :] + bias_o + x[r, :].astype(f32)
        centre = h - row_mean(h)
        scale = lax.rsqrt(row_mean(centre * centre) + EPS)
        unit = centre * scale
        xhat[r, :] = unit
        rstd[r, :] = scale
        fin[r, :] = (unit * gain1 + shift1).astype(bf16)
        return 0

    lax.fori_loop(0, rows // R, norm_one, 0)
    store("rstd").start()
    store("fin").start()
    store("xhat").start()
    wi, w2 = vin["wi"], vin["w2"]
    load("wi").wait()
    load("w2").wait()
    RB = 320
    part_ff = ff // width

    def feed(n, _):
        c = ds(n * width, width)
        bias_i = bi[ds(n * width, width)].reshape(1, width)
        for i in range(rows // RB):
            r = slice(i * RB, (i + 1) * RB)
            u = nn(fin[r, :], wi[:, c]) + bias_i
            cdf = 0.5 * lax.erf(u * 0.7071067811865476) + 0.5
            hid[r, c] = (u * cdf).astype(bf16)
            slope[r, c] = (cdf + u * jnp.exp(-0.5 * (u * u)) * 0.3989422804014327).astype(bf16)
            part = nn(hid[r, c], w2[c, :])
            acc[r, :] = jnp.where(n == 0, part, acc[r, :] + part)
        return 0

    lax.fori_loop(0, part_ff, feed, 0)
    load("dout").wait()
    dout, out, dffn = vin["dout"], vout["out"], vout["dffn"]
    small[...] = jnp.zeros_like(small)
    gain2, shift2, bias_2 = row(g2), row(s2), row(b2)
    pos = lax.broadcasted_iota(jnp.int32, (R, 1), 0)

    def norm_two(n, _):
        r = ds(n * R, R, 32)
        keep = jnp.where(pos < lens[n], 1.0, 0.0).astype(f32)
        h = xhat[r, :] * gain1 + shift1 + (acc[r, :] + bias_2).astype(bf16).astype(f32)
        centre = h - row_mean(h)
        scale = lax.rsqrt(row_mean(centre * centre) + EPS)
        unit = centre * scale
        out[r, :] = ((unit * gain2 + shift2) * keep).astype(bf16)
        g = dout[r, :].astype(f32) * keep
        e = g * gain2
        low = (scale * (e - row_mean(e) - unit * row_mean(e * unit))).astype(bf16)
        dffn[r, :] = low
        small[0:1, :] += jnp.sum(g * unit, 0, keepdims=True)
        small[1:2, :] += jnp.sum(g, 0, keepdims=True)
        small[2:3, :] += jnp.sum(low.astype(f32), 0, keepdims=True)
        return 0

    lax.fori_loop(0, seqs, norm_two, 0)
    store("dffn").start()
    store("out").start()
    far = ds((1 - me[0]) * CHUNK, CHUNK)
    near = ds(me[0] * CHUNK, CHUNK)

    def block_copy(i, n):
        part = pair_part(n, me)
        return pltpu.make_async_copy(block[i].at[part], block_h[i].at[part], sem_block.at[i, n])

    def dpre_copy(n):
        c = ds(n * width, width)
        return pltpu.make_async_copy(dpre.at[:, c], dpre_h.at[:, c], sem_ff.at[n])

    def grads(n, _):
        c = ds(n * width, width)
        put_blocks(block[0], tn(hid[:, c], dffn[:, far]), 2 * n, me, True)
        block_copy(0, n).start()
        put_blocks(block[1], tn(hid[:, c], dffn[:, near]), 2 * n, me, True)
        block_copy(1, n).start()
        d = (nt(dffn[...], w2[c, :]) * slope[:, c].astype(f32)).astype(bf16)
        dpre[:, c] = d
        dpre_copy(n).start()
        small[pl.ds(8 + n, 1), :] = jnp.sum(d.astype(f32), 0, keepdims=True)
        put_blocks(block[2], tn(fin[:, far], dpre[:, c]), 2 * n, me, False)
        block_copy(2, n).start()
        put_blocks(block[3], tn(fin[:, near], dpre[:, c]), 2 * n, me, False)
        block_copy(3, n).start()
        return 0

    lax.fori_loop(0, part_ff, grads, 0)
    for name in FWD_OUT:
        store(name).wait()
    for n in range(part_ff):
        dpre_copy(n).wait()
        for i in range(4):
            block_copy(i, n).wait()


def forward(lens, me, vectors, arrays):
    rows, width = arrays[0].shape
    ff = arrays[5].shape[1]
    seqs = lens.shape[0]
    like = lambda shape, dtype=bf16: sd(shape, dtype)
    thin = like((rows, width))
    outs = [thin, thin, thin, thin, like((rows, width), f32), like((rows, 1), f32), thin, thin, thin]
    wide = [like((rows, ff))] + [like((16, HALF, CHUNK))] * 4
    dma = pltpu.SemaphoreType.DMA
    return pl.pallas_call(
        fwd_kernel,
        in_specs=[SMEM, SMEM] + [VMEM] * 9 + [HBM] * 8,
        out_specs=[VMEM, VMEM] + [HBM] * 14,
        out_shape=[like((seqs, H, rows // seqs), f32), like((16, width), f32)] + outs + wide,
        scratch_shapes=[pltpu.VMEM(a.shape, a.dtype) for a in arrays]
        + [pltpu.VMEM(o.shape, o.dtype) for o in outs + wide]
        + [pltpu.VMEM((rows, ff), bf16), pltpu.VMEM((rows, ff), bf16), pltpu.VMEM((rows, width), f32)]
        + [dma((8,)), dma((9,)), dma((ff // width,)), dma((4, ff // width))],
        compiler_params=params(),
        cost_estimate=cost(28e9),
        name="forward",
    )(lens, me, *vectors, *arrays)


def attention_bwd(lens, q, k, v, dm, lse, d, small):
    rows, width = q.shape
    seqs = lens.shape[0]
    length = rows // seqs
    size = width // H
    low = lax.broadcasted_iota(jnp.int32, (length, 2 * size), 1) < size
    pos = lax.broadcasted_iota(jnp.int32, (2, length, 1), 1)

    def chain(s, _):
        r = ds(s * length, length, 32)
        live = pos < lens[s]
        cols = pairs_of(width, size)
        first = []
        for c in cols:
            k2 = both(low, k[r, c])
            first.append((k2, nt(k2, q[r, c]), nt(both(low, v[r, c]), dm[r, c])))
        for p, c in enumerate(cols):
            k2, st, dprob = first[p]
            st = jnp.where(live, st.reshape(2, length, length), -1e9)
            dprob = dprob.reshape(2, length, length)
            prob = jnp.exp(st - lse[s, pl.ds(2 * p, 2), :].reshape(2, 1, length))
            delta = jnp.sum(prob * dprob, 1, keepdims=True)
            dst = (prob * (dprob - delta)).astype(bf16).reshape(2 * length, length)
            dv = nn(prob.astype(bf16).reshape(2 * length, length), dm[r, c])
            dk = nn(dst, q[r, c])
            dq = (tn(dst, k2) * 0.125).astype(bf16)
            dv = jnp.where(low, dv[:length], dv[length:]).astype(bf16)
            d[r, c] = dq
            d[r, slice(width + c.start, width + c.stop)] = jnp.where(low, dk[:length], dk[length:]).astype(bf16)
            d[r, slice(2 * width + c.start, 2 * width + c.stop)] = dv
            small[6:7, c] += jnp.sum(dq.astype(f32), 0, keepdims=True)
            small[7:8, c] += jnp.sum(dv.astype(f32), 0, keepdims=True)
        return 0

    lax.fori_loop(0, seqs, chain, 0)


MID_IN = ("dffn", "xhat", "rstd", "wo")


def mid_kernel(*refs):
    g1, small1, dpre_h, wi_h = refs[:4]
    src = dict(zip(MID_IN, refs[4:8]))
    small, dh1_h, dob_h, dm_h = refs[8:12]
    dpre, wi = refs[12:14]
    vin = dict(zip(MID_IN, refs[14:18]))
    dh1, dob, dm, acc, sem_ff, sem_in, sem_out = refs[18:]
    rows, width = acc.shape
    part_ff = dpre.shape[1] // width
    R = 160

    def load(name):
        return pltpu.make_async_copy(src[name], vin[name], sem_in.at[MID_IN.index(name)])

    def ff_copies(n):
        c = slice(n * width, (n + 1) * width)
        return (
            pltpu.make_async_copy(dpre_h.at[:, c], dpre.at[:, c], sem_ff.at[0, n]),
            pltpu.make_async_copy(wi_h.at[:, c], wi.at[:, c], sem_ff.at[1, n]),
        )

    for n in range(part_ff):
        for one in ff_copies(n):
            one.start()
    for name in MID_IN:
        load(name).start()
    for n in range(part_ff):
        c = slice(n * width, (n + 1) * width)
        for one in ff_copies(n):
            one.wait()
        part = nt(dpre[:, c], wi[:, c])
        acc[...] = part if n == 0 else acc[...] + part
    small[...] = small1[...]
    gain1 = row(g1)
    dffn, xhat, rstd = vin["dffn"], vin["xhat"], vin["rstd"]
    for name in ("dffn", "xhat", "rstd"):
        load(name).wait()

    def norm_one(i, _):
        r = ds(i * R, R, 32)
        g = dffn[r, :].astype(f32) + acc[r, :].astype(bf16).astype(f32)
        unit = xhat[r, :]
        e = g * gain1
        v = rstd[r, :] * (e - row_mean(e) - unit * row_mean(e * unit))
        dh1[r, :] = v
        low = v.astype(bf16)
        dob[r, :] = low
        small[3:4, :] += jnp.sum(g * unit, 0, keepdims=True)
        small[4:5, :] += jnp.sum(g, 0, keepdims=True)
        small[5:6, :] += jnp.sum(low.astype(f32), 0, keepdims=True)
        return 0

    lax.fori_loop(0, rows // R, norm_one, 0)
    stores = [pltpu.make_async_copy(a, b, sem_out.at[n]) for n, (a, b) in enumerate(((dh1, dh1_h), (dob, dob_h), (dm, dm_h)))]
    stores[0].start()
    stores[1].start()
    load("wo").wait()
    dm[...] = nt(dob[...], vin["wo"][...]).astype(bf16)
    stores[2].start()
    for one in stores:
        one.wait()


def mid_call(g1, small1, dpre, wi, arrays):
    rows, width = arrays[0].shape
    ff = wi.shape[1]
    dma = pltpu.SemaphoreType.DMA
    vm = lambda a: pltpu.VMEM(a.shape, a.dtype)
    outs = [sd((rows, width), f32), sd((rows, width), bf16), sd((rows, width), bf16)]
    return pl.pallas_call(
        mid_kernel,
        in_specs=[VMEM, VMEM] + [HBM] * 6,
        out_specs=[VMEM] + [HBM] * 3,
        out_shape=[sd((16, width), f32)] + outs,
        scratch_shapes=[vm(dpre), vm(wi)] + [vm(a) for a in arrays] + [vm(o) for o in outs]
        + [pltpu.VMEM((rows, width), f32), dma((2, ff // width)), dma((4,)), dma((3,))],
        compiler_params=params(44),
        cost_estimate=cost(10e9),
        name="mid_bwd",
    )(g1, small1, dpre, wi, *arrays)


ATT_IN = ("q", "k", "v", "dm", "lse", "x", "mixed", "dob")


def att_kernel(*refs):
    lens, me, small1 = refs[:3]
    src = dict(zip(ATT_IN, refs[3:11]))
    small, d_h = refs[11:13]
    block_h = refs[13:15]
    rest = refs[15:]
    vin = dict(zip(ATT_IN, rest[:8]))
    d = rest[8]
    block = rest[9:11]
    sem_in, sem_out, sem_block = rest[11:]
    width = d.shape[1] // 4

    def load(name):
        if name == "dob":
            return pltpu.make_async_copy(src[name], d.at[:, 3 * width : 4 * width], sem_in.at[7])
        return pltpu.make_async_copy(src[name], vin[name], sem_in.at[ATT_IN.index(name)])

    for name in ATT_IN:
        load(name).start()
    small[...] = small1[...]
    for name in ("q", "k", "v", "dm", "lse"):
        load(name).wait()
    attention_bwd(lens, vin["q"], vin["k"], vin["v"], vin["dm"], vin["lse"], d, small)
    load("dob").wait()
    d_copy = pltpu.make_async_copy(d, d_h, sem_out.at[0])
    d_copy.start()
    load("x").wait()
    load("mixed").wait()
    sides = (ds((1 - me[0]) * CHUNK, CHUNK), ds(me[0] * CHUNK, CHUNK))

    def block_copy(i, n):
        part = pair_part(n, me)
        return pltpu.make_async_copy(block[i].at[part], block_h[i].at[part], sem_block.at[i, n])

    for n in range(4):
        left = vin["mixed" if n == 3 else "x"]
        for i, side in enumerate(sides):
            put_blocks(block[i], tn(left[:, side], d[:, n * width : (n + 1) * width]), 2 * n, me, False)
            block_copy(i, n).start()
    d_copy.wait()
    for n in range(4):
        for i in range(2):
            block_copy(i, n).wait()


def att_call(lens, me, small1, arrays):
    rows, width = arrays[0].shape
    dma = pltpu.SemaphoreType.DMA
    vm = lambda a: pltpu.VMEM(a.shape, a.dtype)
    outs = [sd((rows, 4 * width), bf16)] + [sd((16, HALF, CHUNK), bf16)] * 2
    return pl.pallas_call(
        att_kernel,
        in_specs=[SMEM, SMEM, VMEM] + [HBM] * 8,
        out_specs=[VMEM] + [HBM] * 3,
        out_shape=[sd((16, width), f32)] + outs,
        scratch_shapes=[vm(a) for a in arrays[:7]] + [pltpu.VMEM((8, 128), bf16)] + [vm(o) for o in outs]
        + [dma((8,)), dma((1,)), dma((2, 4))],
        compiler_params=params(44),
        cost_estimate=cost(12e9),
        name="att_bwd",
    )(lens, me, small1, *arrays)


def dx_kernel(dh1_h, d_h, wq_h, wk_h, wv_h, o_h, dh1, d, wq, wk, wv, o, sem, sem_out):
    width = dh1.shape[1]
    loads = []
    for n, (w_h, w) in enumerate(((wq_h, wq), (wk_h, wk), (wv_h, wv))):
        c = slice(n * width, (n + 1) * width)
        loads.append(pltpu.make_async_copy(d_h.at[:, c], d.at[:, c], sem.at[2 * n]))
        loads.append(pltpu.make_async_copy(w_h, w, sem.at[2 * n + 1]))
    loads.insert(2, pltpu.make_async_copy(dh1_h, dh1, sem.at[6]))
    for one in loads:
        one.start()
    loads[0].wait()
    loads[1].wait()
    part = nt(d[:, :width], wq[...])
    loads[2].wait()
    o[...] = dh1[...] + part
    loads[3].wait()
    loads[4].wait()
    o[...] = o[...] + nt(d[:, width : 2 * width], wk[...])
    loads[5].wait()
    loads[6].wait()
    half = dh1.shape[0] // 2
    stores = []
    for i in range(2):
        r = slice(i * half, (i + 1) * half)
        o[r, :] = o[r, :] + nt(d[r, 2 * width : 3 * width], wv[...])
        stores.append(pltpu.make_async_copy(o.at[r, :], o_h.at[r, :], sem_out.at[i]))
        stores[i].start()
    for one in stores:
        one.wait()


def dx_call(dh1, d, wq, wk, wv):
    rows, width = dh1.shape
    dma = pltpu.SemaphoreType.DMA
    return pl.pallas_call(
        dx_kernel,
        in_specs=[HBM] * 5,
        out_specs=HBM,
        out_shape=sd((rows, width), f32),
        scratch_shapes=[
            pltpu.VMEM((rows, width), f32), pltpu.VMEM((rows, 3 * width), bf16), pltpu.VMEM(wq.shape, bf16),
            pltpu.VMEM(wq.shape, bf16), pltpu.VMEM(wq.shape, bf16), pltpu.VMEM((rows, width), f32), dma((7,)), dma((2,)),
        ],
        compiler_params=params(30),
        cost_estimate=cost(5e9),
        name="dx",
    )(dh1, d, wq, wk, wv)


def bit(value, name):
    return (value >> "xya".index(name)) & 1


def unpack_kernel(kind, orders, me, *refs):
    colors = len(orders)
    n_in = 4 * colors
    src = refs[:n_in]
    n_out = 4 if kind == "attn" else 1
    outs = refs[n_in : n_in + n_out]
    ins = refs[n_in + n_out : 2 * n_in + n_out]
    buf, sem_in, sem = refs[2 * n_in + n_out :]
    size = HALF // colors
    slots = buf.shape[0]

    order_in = [n for first in range(2) for n in range(n_in) if n % 2 == first]
    loads = [pltpu.make_async_copy(src[n], ins[n], sem_in.at[n]) for n in range(n_in)]
    for n in order_in:
        loads[n].start()
    waited = set()

    def copies(step):
        chunk = step ^ me[1]
        slot = step % slots
        if kind == "outer":
            return [(None, pltpu.make_async_copy(buf.at[slot], outs[0].at[ds(chunk * CHUNK, CHUNK), :], sem.at[slot]))]
        if kind == "inner":
            return [(None, pltpu.make_async_copy(buf.at[slot], outs[0].at[:, ds(chunk * CHUNK, CHUNK)], sem.at[slot]))]
        return [
            (chunk // 2 == m, pltpu.make_async_copy(buf.at[slot], outs[m].at[:, ds((chunk % 2) * CHUNK, CHUNK)], sem.at[slot]))
            for m in range(4)
        ]

    def each(step, act):
        for cond, one in copies(step):
            if cond is None:
                act(one)
            else:
                pl.when(cond)(functools.partial(act, one))

    for step in range(8):
        slot = step % slots
        if step >= slots:
            each(step - slots, lambda one: one.wait())
        for half in range(2):
            place = (half ^ me[0]) * CHUNK
            for n in range(colors):
                order = orders[n]
                at = 4 * n + 2 * half + bit(step, order[0])
                if at not in waited:
                    waited.add(at)
                    loads[at].wait()
                for t in range(2):
                    bits = [t if c == "b" else bit(step, c) for c in order]
                    where = bits[1] * 4 + bits[2] * 2 + bits[3]
                    start = (t ^ me[2]) * HALF + n * size
                    value = ins[at][where].astype(f32)
                    if kind == "outer":
                        buf[slot, ds(start, size, 32), ds(place, CHUNK)] = value
                    else:
                        buf[slot, ds(place + start, size, 32), :] = value
        each(step, lambda one: one.start())
    for step in range(8 - slots, 8):
        each(step, lambda one: one.wait())


def unpack(kind, me, pieces, orders):
    colors = len(orders)
    width = 2 * CHUNK
    if kind == "outer":
        out_shape = [sd((8 * CHUNK, width), f32)]
    elif kind == "inner":
        out_shape = [sd((width, 8 * CHUNK), f32)]
    else:
        out_shape = [sd((width, width), f32)] * 4
    buf = (4, CHUNK, width) if kind == "outer" else (4, width, CHUNK)
    dma = pltpu.SemaphoreType.DMA
    return pl.pallas_call(
        functools.partial(unpack_kernel, kind, orders),
        in_specs=[SMEM] + [ANY] * (4 * colors),
        out_specs=[HBM] * len(out_shape),
        out_shape=out_shape,
        scratch_shapes=[pltpu.VMEM(v.shape, v.dtype) for v in pieces]
        + [pltpu.VMEM(buf, f32), dma((4 * colors,)), dma((4,))],
        compiler_params=params(24),
        cost_estimate=cost(4e9),
        name="unpack_" + kind,
    )(me, *pieces)


SMALL_ROWS = (6, 7, 5, 3, 4, 8, 2, 0, 1)


def small_kernel(total, *outs):
    half = total.shape[1]
    for at, out in zip(SMALL_ROWS, outs):
        for n in range(out.shape[0] // half):
            line = at + n // 2 + (n % 2) * (total.shape[0] // 2)
            out[pl.ds(n * half, half)] = total[line : line + 1, :].reshape(half)


def small_call(total, ff):
    width = 2 * total.shape[1]
    sizes = [ff if at == 8 else width for at in SMALL_ROWS]
    return pl.pallas_call(
        small_kernel,
        in_specs=[VMEM],
        out_specs=[VMEM] * 9,
        out_shape=[sd((n,), f32) for n in sizes],
        compiler_params=params(4),
        cost_estimate=cost(1e9),
        name="vectors",
    )(total)


AXES = ("dp", "seq")
DP_BIT = {"x": 0, "y": 1, "a": 2, "b": 3}


def swap(value, name):
    dp = lax.axis_size("dp")
    seq = lax.axis_size("seq")
    flip = 1 if name == "c" else seq << (name if isinstance(name, int) else DP_BIT[name])
    return lax.ppermute(value, AXES, [(i, i ^ flip) for i in range(dp * seq)])


ORDERS = ("xyab", "yaxb", "axyb")


def pick(value, at, n):
    return lax.index_in_dim(value, n, at, keepdims=False)


def reduction(keep, got):
    size = HALF // 3
    shape = (2, 2, 2, 2, HALF, CHUNK)
    keeps = [keep.reshape(shape)[..., n * size : (n + 1) * size, :] for n in range(3)]
    gots = [got.reshape(shape)[..., n * size : (n + 1) * size, :] for n in range(3)]
    dims = ["ayxb"] * 3
    for level in range(3):
        places = [d.index(o[level]) for d, o in zip(dims, ORDERS)]
        sends = [pick(k, at, 1) + pick(g, at, 1) for k, g, at in zip(keeps, gots, places)]
        keeps = [pick(k, at, 0) + pick(g, at, 0) for k, g, at in zip(keeps, gots, places)]
        dims = [d.replace(o[level], "") for d, o in zip(dims, ORDERS)]
        gots = yield [(o[level], v) for o, v in zip(ORDERS, sends)]
    owns = [k + g for k, g in zip(keeps, gots)]
    gots = yield [(o[3], v) for o, v in zip(ORDERS, owns)]
    owns = [v + jnp.concatenate([g[1:], g[:1]]) for v, g in zip(owns, gots)]
    for extra in range(4, lax.axis_size("dp").bit_length() - 1):
        owns = [v + swap(v, extra) for v in owns]
    for level in (2, 1):
        gots = yield [(o[level], v) for o, v in zip(ORDERS, owns)]
        owns = [jnp.stack(v) for v in zip(owns, gots)]
    owns = [v.reshape((8, size, CHUNK)) for v in owns]
    gots = yield [(o[0], v) for o, v in zip(ORDERS, owns)] + [("c", v) for v in owns]
    near, far = gots[:3], gots[3:]
    others = yield [("c", v) for v in near]
    return [v for four in zip(owns, near, far, others) for v in four]


def vector_sum(small):
    half = small.shape[1] // 2
    value = jnp.concatenate([small[:, :half], small[:, half:]])
    links = ["c"] + list("axyb") + list(range(4, lax.axis_size("dp").bit_length() - 1))
    for link in links:
        sent = value.astype(bf16)
        if isinstance(link, int):
            got = swap(sent, link)
        else:
            (got,) = yield [(link, sent)]
        value = sent.astype(f32) + got.astype(f32)
    return value


def unroll(v):
    return v.reshape((-1, v.shape[-1]))


class Rounds:
    def __init__(self):
        self.flows = {}
        self.results = {}
        self.wanted = {}
        self.mark = ()

    def add(self, name, flow):
        self.flows[name] = flow
        self.wanted[name] = next(flow)

    def hold(self, value):
        return lax.optimization_barrier((value,) + self.mark)[0]

    def begin(self, extra=(), skip=()):
        self.order = [(name, n) for name in self.wanted if name not in skip for n in range(len(self.wanted[name]))]
        links = {}
        alone = {}
        for name, n in self.order:
            link, value = self.wanted[name][n]
            if link == "c":
                alone[name, n] = value
            else:
                links.setdefault(link, []).append((name, n))
        merged = {}
        for link, keys in links.items():
            values = [self.wanted[k][n][1] for k, n in keys]
            merged[link] = values[0] if len(values) == 1 else jnp.concatenate([unroll(v) for v in values])
        merged, alone, extra = lax.optimization_barrier((merged, alone, tuple(extra)))
        self.mark = tuple(merged.values())
        self.got = {}
        for link in "baxy":
            if link not in links:
                continue
            keys = links[link]
            got = swap(merged[link], link)
            if len(keys) == 1:
                self.got[keys[0]] = got
                continue
            row = 0
            for k, n in keys:
                shape = self.wanted[k][n][1].shape
                count = math.prod(shape[:-1])
                self.got[k, n] = got[row : row + count].reshape(shape)
                row += count
        for key, value in alone.items():
            self.got[key] = swap(value, "c")
        return [swap(v, "c") for v in extra]

    def end(self, *beside):
        got, _ = lax.optimization_barrier((self.got, tuple(beside)))
        for name in list(self.flows):
            if name not in self.wanted or (name, 0) not in got:
                continue
            values = [got[name, n] for n in range(len(self.wanted[name]))]
            try:
                self.wanted[name] = self.flows[name].send(values)
            except StopIteration as stop:
                self.results[name] = stop.value
                del self.flows[name], self.wanted[name]


def body(chains_in, lengths, d_out, w_query, b_query, w_key, w_value, b_value, w_output, b_output, gain_one, shift_one,
         w_inner, b_inner, w_outer, b_outer, gain_two, shift_two):
    seqs, length, width = chains_in.shape
    rows = seqs * length
    place = lax.axis_index("dp") * 2 + lax.axis_index("seq")
    me = (place >> jnp.array([0, 1, 4], jnp.int32)) & jnp.array([1, 7, 1], jnp.int32)
    x = chains_in.reshape(rows, width)
    lse, small, q, k, v, mixed, xhat, rstd, fin, out, dffn, dpre, send_o, keep_o, send_i, keep_i = forward(
        lengths, me, (b_query, b_value, b_output, gain_one, shift_one, b_inner, b_outer, gain_two, shift_two),
        (x, w_query, w_key, w_value, w_output, w_inner, w_outer, d_out.reshape(rows, width)),
    )
    rounds = Rounds()
    got_o, got_i = rounds.begin([send_o, send_i])
    rounds.add("outer", reduction(keep_o, got_o))
    rounds.begin()
    small, dh1, dob, dm = mid_call(gain_one, small, rounds.hold(dpre), w_inner, (dffn, xhat, rstd, w_output))
    got_i, dm = lax.optimization_barrier((got_i, dm))
    rounds.end(dh1, dob, dm)
    rounds.add("inner", reduction(keep_i, got_i))
    rounds.begin()
    small, d, send, keep = att_call(lengths, me, small, (q, k, v, rounds.hold(dm), lse, x, mixed, dob))
    rounds.end(d, send)
    rounds.add("vectors", vector_sum(small))
    (got,) = rounds.begin([send])
    d_x = dx_call(rounds.hold(dh1), d, w_query, w_key, w_value)
    got, d_x = lax.optimization_barrier((got, d_x))
    rounds.end(got)
    rounds.add("attn", reduction(keep, got))
    for _ in range(4):
        rounds.begin()
        rounds.end()
    rounds.begin()
    vec = small_call(rounds.hold(rounds.results["vectors"]), w_inner.shape[1])
    rounds.end(vec[0])
    rounds.begin()
    (d_w_outer,) = unpack("outer", me, rounds.hold(rounds.results["outer"]), ORDERS)
    rounds.end(d_w_outer)
    rounds.begin()
    (d_w_inner,) = unpack("inner", me, rounds.hold(rounds.results["inner"]), ORDERS)
    rounds.end(d_w_inner)
    rounds.begin()
    rounds.end()
    d_w_query, d_w_key, d_w_value, d_w_output = unpack("attn", me, rounds.results["attn"], ORDERS)
    return (
        out.reshape(seqs, length, width), d_x.reshape(seqs, length, width),
        d_w_query, vec[0], d_w_key, d_w_value, vec[1], d_w_output, vec[2], vec[3], vec[4],
        d_w_inner, vec[5], d_w_outer, vec[6], vec[7], vec[8],
    )


def solution(mesh):
    rows = P(AXES, None, None)
    return jax.shard_map(
        body, mesh=mesh, in_specs=(rows, P(AXES), rows) + (P(),) * 15, out_specs=(rows, rows) + (P(),) * 15, check_vma=False
    )
```

```python
import functools
import math
import jax
import jax.numpy as jnp
from jax import lax
from jax.experimental import pallas as pl
from jax.experimental.pallas import tpu as pltpu
from jax.sharding import PartitionSpec as P

H = 12
EPS = 1e-12
f32 = jnp.float32
bf16 = jnp.bfloat16
sd = jax.ShapeDtypeStruct
ANY = pl.BlockSpec(memory_space=pl.ANY)
HBM = pl.BlockSpec(memory_space=pltpu.HBM)
VMEM = pl.BlockSpec(memory_space=pltpu.VMEM)
SMEM = pl.BlockSpec(memory_space=pltpu.SMEM)
CHUNK = 384
HALF = CHUNK // 2


def params(mib=60):
    return pltpu.CompilerParams(vmem_limit_bytes=mib * 1024 * 1024)


def cost(flops, nbytes=1 << 20):
    return pl.CostEstimate(flops=int(flops), transcendentals=0, bytes_accessed=int(nbytes))


def nn(a, b):
    return lax.dot_general(a, b, (((1,), (0,)), ((), ())), preferred_element_type=f32)


def nt(a, b):
    return lax.dot_general(a, b, (((1,), (1,)), ((), ())), preferred_element_type=f32)


def tn(a, b):
    return lax.dot_general(a, b, (((0,), (0,)), ((), ())), preferred_element_type=f32)


def own_place():
    dp = lax.axis_index("dp")
    return lax.axis_index("seq"), dp & 7, (dp >> 3) & 1


def row_mean(v):
    return jnp.mean(v, -1, keepdims=True)


def ds(start, size, align=None):
    return pl.ds(pl.multiple_of(start, align or size), size)


FWD_IN = ("x", "wq", "wk", "wv", "wo", "wi", "w2", "dout")
FWD_OUT = ("q", "k", "v", "mixed", "xhat", "rstd", "fin", "out", "dffn")


def row(ref):
    return ref[...].reshape(1, ref.shape[0])


def both(low, v):
    zero = jnp.zeros_like(v)
    return jnp.concatenate([jnp.where(low, v, zero), jnp.where(low, zero, v)], 0)


def pairs_of(width, size):
    return [slice(2 * size * p, 2 * size * (p + 1)) for p in range(width // (2 * size))]


def attention(lens, q, k, v, mixed, lse):
    rows, width = q.shape
    seqs = lens.shape[0]
    length = rows // seqs
    size = width // H
    low = lax.broadcasted_iota(jnp.int32, (length, 2 * size), 1) < size
    pos = lax.broadcasted_iota(jnp.int32, (2, length, 1), 1)

    def chain(s, _):
        r = ds(s * length, length, 32)
        live = pos < lens[s]
        cols = pairs_of(width, size)
        scores = [nt(both(low, k[r, c]), q[r, c]) for c in cols]
        for p, c in enumerate(cols):
            st = jnp.where(live, scores[p].reshape(2, length, length), -1e9)
            top = jnp.max(st, 1, keepdims=True)
            e = jnp.exp(st - top)
            total = jnp.sum(e, 1, keepdims=True)
            lse[s, pl.ds(2 * p, 2), :] = (top + jnp.log(total)).reshape(2, length)
            prob = (e * (1.0 / total)).astype(bf16).reshape(2 * length, length)
            mixed[r, c] = tn(prob, both(low, v[r, c])).astype(bf16)
        return 0

    lax.fori_loop(0, seqs, chain, 0)


def put_blocks(outs, grad, chunk0, me, rows_are_chunks):
    for i in range(2):
        for n, out in enumerate(outs):
            half = (me[0] ^ (1 - n)) * CHUNK
            for t in range(2):
                if rows_are_chunks:
                    value = grad[i * CHUNK + t * HALF : i * CHUNK + (t + 1) * HALF, ds(half, CHUNK)]
                else:
                    value = grad[ds(half + t * HALF, HALF), i * CHUNK : (i + 1) * CHUNK]
                out[((chunk0 + i) ^ me[1]) * 2 + (t ^ me[2])] = value.astype(bf16)


def put_side(out, grad, chunk0, me):
    for i in range(2):
        for t in range(2):
            value = grad[t * HALF : (t + 1) * HALF, i * CHUNK : (i + 1) * CHUNK]
            out[((chunk0 + i) ^ me[1]) * 2 + (t ^ me[2])] = value.astype(bf16)


def pair_part(n, me):
    return pl.ds(4 * (n ^ (me[1] >> 1)), 4)


def fwd_kernel(*refs):
    lens, me = refs[:2]
    bq, bv, bo, g1, s1, bi, b2, g2, s2 = refs[2:11]
    src = dict(zip(FWD_IN, refs[11:19]))
    lse, small = refs[19:21]
    dst = dict(zip(FWD_OUT, refs[21:30]))
    dpre_h = refs[30]
    block_h = refs[31:35]
    rest = refs[35:]
    vin = dict(zip(FWD_IN, rest[:8]))
    vout = dict(zip(FWD_OUT, rest[8:17]))
    dpre = rest[17]
    block = rest[18:22]
    hid, slope, acc, both_grad, sem_in, sem_out, sem_ff, sem_block = rest[22:]
    rows, width = vin["x"].shape
    ff = vin["wi"].shape[1]
    seqs = lens.shape[0]
    length = rows // seqs

    def load(name):
        return pltpu.make_async_copy(src[name], vin[name], sem_in.at[FWD_IN.index(name)])

    def store(name):
        return pltpu.make_async_copy(vout[name], dst[name], sem_out.at[FWD_OUT.index(name)])

    x, q, k, v, mixed = vin["x"], vout["q"], vout["k"], vout["v"], vout["mixed"]
    for name in ("x", "wq", "wk"):
        load(name).start()
    load("x").wait()
    load("wq").wait()
    load("wv").start()
    load("wo").start()
    q[...] = ((nn(x[...], vin["wq"][...]) + row(bq)).astype(bf16).astype(f32) * 0.125).astype(bf16)
    store("q").start()
    load("wk").wait()
    load("wi").start()
    k[...] = nn(x[...], vin["wk"][...]).astype(bf16)
    store("k").start()
    load("wv").wait()
    load("w2").start()
    load("dout").start()
    v[...] = (nn(x[...], vin["wv"][...]) + row(bv)).astype(bf16)
    store("v").start()
    attention(lens, q, k, v, mixed, lse)
    store("mixed").start()
    load("wo").wait()
    xhat, rstd, fin = vout["xhat"], vout["rstd"], vout["fin"]
    acc[...] = nn(mixed[...], vin["wo"][...])
    R = length
    gain1, shift1, bias_o = row(g1), row(s1), row(bo)

    def norm_one(n, _):
        r = ds(n * R, R, 32)
        h = acc[r, :] + bias_o + x[r, :].astype(f32)
        centre = h - row_mean(h)
        scale = lax.rsqrt(row_mean(centre * centre) + EPS)
        unit = centre * scale
        xhat[r, :] = unit
        rstd[r, :] = scale
        fin[r, :] = (unit * gain1 + shift1).astype(bf16)
        return 0

    lax.fori_loop(0, rows // R, norm_one, 0)
    store("rstd").start()
    store("fin").start()
    store("xhat").start()
    wi, w2 = vin["wi"], vin["w2"]
    load("wi").wait()
    load("w2").wait()
    RB = 320
    part_ff = ff // width

    def feed(n, _):
        c = ds(n * width, width)
        bias_i = bi[ds(n * width, width)].reshape(1, width)
        for i in range(rows // RB):
            r = slice(i * RB, (i + 1) * RB)
            u = nn(fin[r, :], wi[:, c]) + bias_i
            cdf = 0.5 * lax.erf(u * 0.7071067811865476) + 0.5
            hid[r, c] = (u * cdf).astype(bf16)
            slope[r, c] = (cdf + u * jnp.exp(-0.5 * (u * u)) * 0.3989422804014327).astype(bf16)
            part = nn(hid[r, c], w2[c, :])
            acc[r, :] = jnp.where(n == 0, part, acc[r, :] + part)
        return 0

    lax.fori_loop(0, part_ff, feed, 0)
    load("dout").wait()
    dout, out, dffn = vin["dout"], vout["out"], vout["dffn"]
    small[...] = jnp.zeros_like(small)
    gain2, shift2, bias_2 = row(g2), row(s2), row(b2)
    pos = lax.broadcasted_iota(jnp.int32, (R, 1), 0)

    def norm_two(n, _):
        r = ds(n * R, R, 32)
        keep = jnp.where(pos < lens[n], 1.0, 0.0).astype(f32)
        h = xhat[r, :] * gain1 + shift1 + (acc[r, :] + bias_2).astype(bf16).astype(f32)
        centre = h - row_mean(h)
        scale = lax.rsqrt(row_mean(centre * centre) + EPS)
        unit = centre * scale
        out[r, :] = ((unit * gain2 + shift2) * keep).astype(bf16)
        g = dout[r, :].astype(f32) * keep
        e = g * gain2
        low = (scale * (e - row_mean(e) - unit * row_mean(e * unit))).astype(bf16)
        dffn[r, :] = low
        small[0:1, :] += jnp.sum(g * unit, 0, keepdims=True)
        small[1:2, :] += jnp.sum(g, 0, keepdims=True)
        small[2:3, :] += jnp.sum(low.astype(f32), 0, keepdims=True)
        return 0

    lax.fori_loop(0, seqs, norm_two, 0)
    store("dffn").start()
    store("out").start()
    def block_copy(i, n):
        part = pair_part(n, me)
        return pltpu.make_async_copy(block[i].at[part], block_h[i].at[part], sem_block.at[i, n])

    def dpre_copy(n):
        c = ds(n * width, width)
        return pltpu.make_async_copy(dpre.at[:, c], dpre_h.at[:, c], sem_ff.at[n])

    def grads(n, _):
        c = ds(n * width, width)
        both_grad[...] = tn(hid[:, c], dffn[...])
        put_blocks(block[0:2], both_grad, 2 * n, me, True)
        block_copy(0, n).start()
        block_copy(1, n).start()
        d = (nt(dffn[...], w2[c, :]) * slope[:, c].astype(f32)).astype(bf16)
        dpre[:, c] = d
        dpre_copy(n).start()
        small[pl.ds(8 + n, 1), :] = jnp.sum(d.astype(f32), 0, keepdims=True)
        both_grad[...] = tn(fin[...], dpre[:, c])
        put_blocks(block[2:4], both_grad, 2 * n, me, False)
        block_copy(2, n).start()
        block_copy(3, n).start()
        return 0

    lax.fori_loop(0, part_ff, grads, 0)
    for name in FWD_OUT:
        store(name).wait()
    for n in range(part_ff):
        dpre_copy(n).wait()
        for i in range(4):
            block_copy(i, n).wait()


def forward(lens, me, vectors, arrays):
    rows, width = arrays[0].shape
    ff = arrays[5].shape[1]
    seqs = lens.shape[0]
    like = lambda shape, dtype=bf16: sd(shape, dtype)
    thin = like((rows, width))
    outs = [thin, thin, thin, thin, like((rows, width), f32), like((rows, 1), f32), thin, thin, thin]
    wide = [like((rows, ff))] + [like((16, HALF, CHUNK))] * 4
    dma = pltpu.SemaphoreType.DMA
    return pl.pallas_call(
        fwd_kernel,
        in_specs=[SMEM, SMEM] + [VMEM] * 9 + [HBM] * 8,
        out_specs=[VMEM, VMEM] + [HBM] * 14,
        out_shape=[like((seqs, H, rows // seqs), f32), like((16, width), f32)] + outs + wide,
        scratch_shapes=[pltpu.VMEM(a.shape, a.dtype) for a in arrays]
        + [pltpu.VMEM(o.shape, o.dtype) for o in outs + wide]
        + [pltpu.VMEM((rows, ff), bf16), pltpu.VMEM((rows, ff), bf16), pltpu.VMEM((rows, width), f32)]
        + [pltpu.VMEM((width, width), f32), dma((8,)), dma((9,)), dma((ff // width,)), dma((4, ff // width))],
        compiler_params=params(),
        cost_estimate=cost(28e9),
        name="forward",
    )(lens, me, *vectors, *arrays)


def attention_bwd(lens, q, k, v, dm, lse, d, small):
    rows, width = q.shape
    seqs = lens.shape[0]
    length = rows // seqs
    size = width // H
    low = lax.broadcasted_iota(jnp.int32, (length, 2 * size), 1) < size
    pos = lax.broadcasted_iota(jnp.int32, (2, length, 1), 1)

    def chain(s, _):
        r = ds(s * length, length, 32)
        live = pos < lens[s]
        cols = pairs_of(width, size)
        first = []
        for c in cols:
            k2 = both(low, k[r, c])
            first.append((k2, nt(k2, q[r, c]), nt(both(low, v[r, c]), dm[r, c])))
        for p, c in enumerate(cols):
            k2, st, dprob = first[p]
            st = jnp.where(live, st.reshape(2, length, length), -1e9)
            dprob = dprob.reshape(2, length, length)
            prob = jnp.exp(st - lse[s, pl.ds(2 * p, 2), :].reshape(2, 1, length))
            delta = jnp.sum(prob * dprob, 1, keepdims=True)
            dst = (prob * (dprob - delta)).astype(bf16).reshape(2 * length, length)
            dv = nn(prob.astype(bf16).reshape(2 * length, length), dm[r, c])
            dk = nn(dst, q[r, c])
            dq = (tn(dst, k2) * 0.125).astype(bf16)
            dv = jnp.where(low, dv[:length], dv[length:]).astype(bf16)
            d[r, c] = dq
            d[r, slice(width + c.start, width + c.stop)] = jnp.where(low, dk[:length], dk[length:]).astype(bf16)
            d[r, slice(2 * width + c.start, 2 * width + c.stop)] = dv
            small[6:7, c] += jnp.sum(dq.astype(f32), 0, keepdims=True)
            small[7:8, c] += jnp.sum(dv.astype(f32), 0, keepdims=True)
        return 0

    lax.fori_loop(0, seqs, chain, 0)


MID_IN = ("dffn", "xhat", "rstd", "wo")


def mid_kernel(*refs):
    g1, small1, dpre_h, wi_h = refs[:4]
    src = dict(zip(MID_IN, refs[4:8]))
    small, dh1_h, dob_h, dm_h = refs[8:12]
    dpre, wi = refs[12:14]
    vin = dict(zip(MID_IN, refs[14:18]))
    dh1, dob, dm, acc, sem_ff, sem_in, sem_out = refs[18:]
    rows, width = acc.shape
    part_ff = dpre.shape[1] // width
    R = 160

    def load(name):
        return pltpu.make_async_copy(src[name], vin[name], sem_in.at[MID_IN.index(name)])

    def ff_copies(n):
        c = ds(n * width, width)
        return (
            pltpu.make_async_copy(dpre_h.at[:, c], dpre.at[:, c], sem_ff.at[0, n]),
            pltpu.make_async_copy(wi_h.at[:, c], wi.at[:, c], sem_ff.at[1, n]),
        )

    for n in range(part_ff):
        for one in ff_copies(n):
            one.start()
    for name in MID_IN:
        load(name).start()
    def products(n, _):
        c = ds(n * width, width)
        for one in ff_copies(n):
            one.wait()
        part = nt(dpre[:, c], wi[:, c])
        acc[...] = jnp.where(n == 0, part, acc[...] + part)
        return 0

    lax.fori_loop(0, part_ff, products, 0)
    small[...] = small1[...]
    gain1 = row(g1)
    dffn, xhat, rstd = vin["dffn"], vin["xhat"], vin["rstd"]
    for name in ("dffn", "xhat", "rstd"):
        load(name).wait()

    def norm_one(i, _):
        r = ds(i * R, R, 32)
        g = dffn[r, :].astype(f32) + acc[r, :].astype(bf16).astype(f32)
        unit = xhat[r, :]
        e = g * gain1
        v = rstd[r, :] * (e - row_mean(e) - unit * row_mean(e * unit))
        dh1[r, :] = v
        low = v.astype(bf16)
        dob[r, :] = low
        small[3:4, :] += jnp.sum(g * unit, 0, keepdims=True)
        small[4:5, :] += jnp.sum(g, 0, keepdims=True)
        small[5:6, :] += jnp.sum(low.astype(f32), 0, keepdims=True)
        return 0

    lax.fori_loop(0, rows // R, norm_one, 0)
    stores = [pltpu.make_async_copy(a, b, sem_out.at[n]) for n, (a, b) in enumerate(((dh1, dh1_h), (dob, dob_h), (dm, dm_h)))]
    stores[0].start()
    stores[1].start()
    load("wo").wait()
    dm[...] = nt(dob[...], vin["wo"][...]).astype(bf16)
    stores[2].start()
    for one in stores:
        one.wait()


def mid_call(g1, small1, dpre, wi, arrays):
    rows, width = arrays[0].shape
    ff = wi.shape[1]
    dma = pltpu.SemaphoreType.DMA
    vm = lambda a: pltpu.VMEM(a.shape, a.dtype)
    outs = [sd((rows, width), f32), sd((rows, width), bf16), sd((rows, width), bf16)]
    return pl.pallas_call(
        mid_kernel,
        in_specs=[VMEM, VMEM] + [HBM] * 6,
        out_specs=[VMEM] + [HBM] * 3,
        out_shape=[sd((16, width), f32)] + outs,
        scratch_shapes=[vm(dpre), vm(wi)] + [vm(a) for a in arrays] + [vm(o) for o in outs]
        + [pltpu.VMEM((rows, width), f32), dma((2, ff // width)), dma((4,)), dma((3,))],
        compiler_params=params(44),
        cost_estimate=cost(10e9),
        name="mid_bwd",
    )(g1, small1, dpre, wi, *arrays)


ATT_IN = ("q", "k", "v", "dm", "lse", "x", "mixed", "dob")


def att_kernel(*refs):
    lens, me, small1 = refs[:3]
    src = dict(zip(ATT_IN, refs[3:11]))
    small, d_h = refs[11:13]
    block_h = refs[13:15]
    rest = refs[15:]
    vin = dict(zip(ATT_IN, rest[:8]))
    d = rest[8]
    block = rest[9:11]
    sem_in, sem_out, sem_block = rest[11:]
    width = d.shape[1] // 4

    def load(name):
        if name == "dob":
            return pltpu.make_async_copy(src[name], d.at[:, 3 * width : 4 * width], sem_in.at[7])
        return pltpu.make_async_copy(src[name], vin[name], sem_in.at[ATT_IN.index(name)])

    for name in ATT_IN:
        load(name).start()
    small[...] = small1[...]
    for name in ("q", "k", "v", "dm", "lse"):
        load(name).wait()
    attention_bwd(lens, vin["q"], vin["k"], vin["v"], vin["dm"], vin["lse"], d, small)
    load("dob").wait()
    d_copy = pltpu.make_async_copy(d, d_h, sem_out.at[0])
    d_copy.start()
    load("x").wait()
    load("mixed").wait()
    def block_copy(i, n):
        part = pair_part(n, me)
        return pltpu.make_async_copy(block[i].at[part], block_h[i].at[part], sem_block.at[i, n])

    sides = (ds((1 - me[0]) * CHUNK, CHUNK), ds(me[0] * CHUNK, CHUNK))

    for n in range(4):
        left = vin["mixed" if n == 3 else "x"]
        for i, side in enumerate(sides):
            put_side(block[i], tn(left[:, side], d[:, n * width : (n + 1) * width]), 2 * n, me)
            block_copy(i, n).start()
    d_copy.wait()
    for n in range(4):
        for i in range(2):
            block_copy(i, n).wait()


def att_call(lens, me, small1, arrays):
    rows, width = arrays[0].shape
    dma = pltpu.SemaphoreType.DMA
    vm = lambda a: pltpu.VMEM(a.shape, a.dtype)
    outs = [sd((rows, 4 * width), bf16)] + [sd((16, HALF, CHUNK), bf16)] * 2
    return pl.pallas_call(
        att_kernel,
        in_specs=[SMEM, SMEM, VMEM] + [HBM] * 8,
        out_specs=[VMEM] + [HBM] * 3,
        out_shape=[sd((16, width), f32)] + outs,
        scratch_shapes=[vm(a) for a in arrays[:7]] + [pltpu.VMEM((8, 128), bf16)] + [vm(o) for o in outs]
        + [dma((8,)), dma((1,)), dma((2, 4))],
        compiler_params=params(44),
        cost_estimate=cost(12e9),
        name="att_bwd",
    )(lens, me, small1, *arrays)


def dx_kernel(dh1_h, d_h, wq_h, wk_h, wv_h, o_h, dh1, d, wq, wk, wv, o, sem, sem_out):
    width = dh1.shape[1]
    loads = []
    for n, (w_h, w) in enumerate(((wq_h, wq), (wk_h, wk), (wv_h, wv))):
        c = slice(n * width, (n + 1) * width)
        loads.append(pltpu.make_async_copy(d_h.at[:, c], d.at[:, c], sem.at[2 * n]))
        loads.append(pltpu.make_async_copy(w_h, w, sem.at[2 * n + 1]))
    loads.insert(2, pltpu.make_async_copy(dh1_h, dh1, sem.at[6]))
    for one in loads:
        one.start()
    loads[0].wait()
    loads[1].wait()
    part = nt(d[:, :width], wq[...])
    loads[2].wait()
    o[...] = dh1[...] + part
    loads[3].wait()
    loads[4].wait()
    o[...] = o[...] + nt(d[:, width : 2 * width], wk[...])
    loads[5].wait()
    loads[6].wait()
    half = dh1.shape[0] // 2
    stores = []
    for i in range(2):
        r = slice(i * half, (i + 1) * half)
        o[r, :] = o[r, :] + nt(d[r, 2 * width : 3 * width], wv[...])
        stores.append(pltpu.make_async_copy(o.at[r, :], o_h.at[r, :], sem_out.at[i]))
        stores[i].start()
    for one in stores:
        one.wait()


def dx_call(dh1, d, wq, wk, wv):
    rows, width = dh1.shape
    dma = pltpu.SemaphoreType.DMA
    return pl.pallas_call(
        dx_kernel,
        in_specs=[HBM] * 5,
        out_specs=HBM,
        out_shape=sd((rows, width), f32),
        scratch_shapes=[
            pltpu.VMEM((rows, width), f32), pltpu.VMEM((rows, 3 * width), bf16), pltpu.VMEM(wq.shape, bf16),
            pltpu.VMEM(wq.shape, bf16), pltpu.VMEM(wq.shape, bf16), pltpu.VMEM((rows, width), f32), dma((7,)), dma((2,)),
        ],
        compiler_params=params(30),
        cost_estimate=cost(5e9),
        name="dx",
    )(dh1, d, wq, wk, wv)


def bit(value, name):
    return (value >> "xya".index(name)) & 1


def unpack_kernel(kind, orders, *refs):
    me = own_place()
    colors = len(orders)
    n_in = 4 * colors
    src = refs[:n_in]
    n_out = 4 if kind == "attn" else 1
    outs = refs[n_in : n_in + n_out]
    ins = refs[n_in + n_out : 2 * n_in + n_out]
    buf, sem_in, sem = refs[2 * n_in + n_out :]
    sizes = [src[4 * n].shape[1] for n in range(colors)]
    slots = buf.shape[0]

    order_in = [n for first in range(2) for n in range(n_in) if n % 2 == first]
    loads = [pltpu.make_async_copy(src[n], ins[n], sem_in.at[n]) for n in range(n_in)]
    for n in order_in:
        loads[n].start()
    waited = set()

    def copies(step):
        chunk = step ^ me[1]
        slot = step % slots
        if kind == "outer":
            return [(None, pltpu.make_async_copy(buf.at[slot], outs[0].at[ds(chunk * CHUNK, CHUNK), :], sem.at[slot]))]
        if kind == "inner":
            return [(None, pltpu.make_async_copy(buf.at[slot], outs[0].at[:, ds(chunk * CHUNK, CHUNK)], sem.at[slot]))]
        return [
            (chunk // 2 == m, pltpu.make_async_copy(buf.at[slot], outs[m].at[:, ds((chunk % 2) * CHUNK, CHUNK)], sem.at[slot]))
            for m in range(4)
        ]

    def each(step, act):
        for cond, one in copies(step):
            if cond is None:
                act(one)
            else:
                pl.when(cond)(functools.partial(act, one))

    for step in range(8):
        slot = step % slots
        if step >= slots:
            each(step - slots, lambda one: one.wait())
        for half in range(2):
            place = (half ^ me[0]) * CHUNK
            for n in range(colors):
                order, size, first = orders[n], sizes[n], sum(sizes[:n])
                at = 4 * n + 2 * half + bit(step, order[0])
                if at not in waited:
                    waited.add(at)
                    loads[at].wait()
                for t in range(2):
                    bits = [t if c == "b" else bit(step, c) for c in order]
                    where = bits[1] * 4 + bits[2] * 2 + bits[3]
                    start = (t ^ me[2]) * HALF + first
                    value = ins[at][where].astype(f32)
                    if kind == "outer":
                        buf[slot, ds(start, size, 16), ds(place, CHUNK)] = value
                    else:
                        buf[slot, ds(place + start, size, 16), :] = value
        each(step, lambda one: one.start())
    for step in range(8 - slots, 8):
        each(step, lambda one: one.wait())


def unpack(kind, pieces, orders):
    colors = len(orders)
    width = 2 * CHUNK
    if kind == "outer":
        out_shape = [sd((8 * CHUNK, width), f32)]
    elif kind == "inner":
        out_shape = [sd((width, 8 * CHUNK), f32)]
    else:
        out_shape = [sd((width, width), f32)] * 4
    buf = (4, CHUNK, width) if kind == "outer" else (4, width, CHUNK)
    dma = pltpu.SemaphoreType.DMA
    return pl.pallas_call(
        functools.partial(unpack_kernel, kind, orders),
        in_specs=[ANY] * (4 * colors),
        out_specs=[HBM] * len(out_shape),
        out_shape=out_shape,
        scratch_shapes=[pltpu.VMEM(v.shape, v.dtype) for v in pieces]
        + [pltpu.VMEM(buf, f32), dma((4 * colors,)), dma((4,))],
        compiler_params=params(24),
        cost_estimate=cost(4e9),
        name="unpack_" + kind,
    )(*pieces)


SMALL_ROWS = (6, 7, 5, 3, 4, 8, 2, 0, 1)


def small_kernel(total, *outs):
    half = total.shape[1]
    for at, out in zip(SMALL_ROWS, outs):
        for n in range(out.shape[0] // half):
            line = at + n // 2 + (n % 2) * (total.shape[0] // 2)
            out[pl.ds(n * half, half)] = total[line : line + 1, :].reshape(half)


def small_call(total, ff):
    width = 2 * total.shape[1]
    sizes = [ff if at == 8 else width for at in SMALL_ROWS]
    return pl.pallas_call(
        small_kernel,
        in_specs=[VMEM],
        out_specs=[VMEM] * 9,
        out_shape=[sd((n,), f32) for n in sizes],
        compiler_params=params(4),
        cost_estimate=cost(1e9),
        name="vectors",
    )(total)


AXES = ("dp", "seq")
DP_BIT = {"x": 0, "y": 1, "a": 2, "b": 3}


def swap(value, name):
    dp = lax.axis_size("dp")
    seq = lax.axis_size("seq")
    flip = 1 if name == "c" else seq << (name if isinstance(name, int) else DP_BIT[name])
    return lax.ppermute(value, AXES, [(i, i ^ flip) for i in range(dp * seq)])


ORDERS = ("xyab", "yaxb", "axyb")


def pick(value, at, n):
    return lax.index_in_dim(value, n, at, keepdims=False)


def cut(value, sizes):
    return [value[..., sum(sizes[:n]) : sum(sizes[: n + 1]), :] for n in range(len(sizes))]


EVEN = (64, 64, 64)
LEAN = (80, 64, 48)


def reduction(keep, got, down=EVEN, up=EVEN):
    shape = (2, 2, 2, 2, HALF, CHUNK)
    keeps = cut(keep.reshape(shape), down)
    gots = cut(got.reshape(shape), down)
    dims = ["ayxb"] * 3
    for level in range(3):
        places = [d.index(o[level]) for d, o in zip(dims, ORDERS)]
        sends = [pick(k, at, 1) + pick(g, at, 1) for k, g, at in zip(keeps, gots, places)]
        keeps = [pick(k, at, 0) + pick(g, at, 0) for k, g, at in zip(keeps, gots, places)]
        dims = [d.replace(o[level], "") for d, o in zip(dims, ORDERS)]
        gots = yield [(o[level], v) for o, v in zip(ORDERS, sends)]
    own = jnp.concatenate([k + g for k, g in zip(keeps, gots)], -2)
    (got,) = yield [("b", own)]
    own = own + jnp.concatenate([got[1:], got[:1]])
    for extra in range(4, lax.axis_size("dp").bit_length() - 1):
        own = own + swap(own, extra)
    owns = cut(own, up)
    for level in (2, 1):
        gots = yield [(o[level], v) for o, v in zip(ORDERS, owns)]
        owns = [jnp.stack(v) for v in zip(owns, gots)]
    owns = [v.reshape((8,) + v.shape[-2:]) for v in owns]
    gots = yield [(o[0], v) for o, v in zip(ORDERS, owns)] + [("c", v) for v in owns]
    near, far = gots[:3], gots[3:]
    others = yield [("c", v) for v in near]
    return [v for four in zip(owns, near, far, others) for v in four]


def vector_sum(small):
    half = small.shape[1] // 2
    value = jnp.concatenate([small[:, :half], small[:, half:]])
    links = ["c"] + list("axyb") + list(range(4, lax.axis_size("dp").bit_length() - 1))
    for link in links:
        sent = value.astype(bf16)
        if isinstance(link, int):
            got = swap(sent, link)
        else:
            (got,) = yield [(link, sent)]
        value = sent.astype(f32) + got.astype(f32)
    return value


def unroll(v):
    return v.reshape((-1, v.shape[-1]))


class Rounds:
    def __init__(self):
        self.flows = {}
        self.results = {}
        self.wanted = {}
        self.mark = ()

    def add(self, name, flow):
        self.flows[name] = flow
        self.wanted[name] = next(flow)

    def hold(self, value):
        return lax.optimization_barrier((value,) + self.mark)[0]

    def begin(self, extra=(), skip=()):
        self.order = [(name, n) for name in self.wanted if name not in skip for n in range(len(self.wanted[name]))]
        links = {}
        alone = {}
        for name, n in self.order:
            link, value = self.wanted[name][n]
            if link == "c":
                alone[name, n] = value
            else:
                links.setdefault(link, []).append((name, n))
        merged = {}
        for link, keys in links.items():
            values = [self.wanted[k][n][1] for k, n in keys]
            merged[link] = values[0] if len(values) == 1 else jnp.concatenate([unroll(v) for v in values])
        merged, alone, extra = lax.optimization_barrier((merged, alone, tuple(extra)))
        self.mark = tuple(merged.values())
        self.got = {}
        for link in "baxy":
            if link not in links:
                continue
            keys = links[link]
            got = swap(merged[link], link)
            if len(keys) == 1:
                self.got[keys[0]] = got
                continue
            row = 0
            for k, n in keys:
                shape = self.wanted[k][n][1].shape
                count = math.prod(shape[:-1])
                self.got[k, n] = got[row : row + count].reshape(shape)
                row += count
        for key, value in alone.items():
            self.got[key] = swap(value, "c")
        return [swap(v, "c") for v in extra]

    def end(self, *beside):
        got, _ = lax.optimization_barrier((self.got, tuple(beside)))
        for name in list(self.flows):
            if name not in self.wanted or (name, 0) not in got:
                continue
            values = [got[name, n] for n in range(len(self.wanted[name]))]
            try:
                self.wanted[name] = self.flows[name].send(values)
            except StopIteration as stop:
                self.results[name] = stop.value
                del self.flows[name], self.wanted[name]


def body(chains_in, lengths, d_out, w_query, b_query, w_key, w_value, b_value, w_output, b_output, gain_one, shift_one,
         w_inner, b_inner, w_outer, b_outer, gain_two, shift_two):
    seqs, length, width = chains_in.shape
    rows = seqs * length
    place = lax.axis_index("dp") * 2 + lax.axis_index("seq")
    me = (place >> jnp.array([0, 1, 4], jnp.int32)) & jnp.array([1, 7, 1], jnp.int32)
    x = chains_in.reshape(rows, width)
    lse, small, q, k, v, mixed, xhat, rstd, fin, out, dffn, dpre, send_o, keep_o, send_i, keep_i = forward(
        lengths, me, (b_query, b_value, b_output, gain_one, shift_one, b_inner, b_outer, gain_two, shift_two),
        (x, w_query, w_key, w_value, w_output, w_inner, w_outer, d_out.reshape(rows, width)),
    )
    rounds = Rounds()
    got_o, got_i = rounds.begin([send_o, send_i])
    rounds.add("outer", reduction(keep_o, got_o))
    rounds.begin()
    small, dh1, dob, dm = mid_call(gain_one, small, rounds.hold(dpre), w_inner, (dffn, xhat, rstd, w_output))
    got_i, dm = lax.optimization_barrier((got_i, dm))
    rounds.end(dh1, dob, dm)
    rounds.add("inner", reduction(keep_i, got_i))
    rounds.begin()
    small, d, send, keep = att_call(lengths, me, small, (q, k, v, rounds.hold(dm), lse, x, mixed, dob))
    rounds.end(d, send)
    rounds.add("vectors", vector_sum(small))
    (got,) = rounds.begin([send])
    d_x = dx_call(rounds.hold(dh1), d, w_query, w_key, w_value)
    got, d_x = lax.optimization_barrier((got, d_x))
    rounds.end(got)
    rounds.add("attn", reduction(keep, got))
    for _ in range(4):
        rounds.begin()
        rounds.end()
    rounds.begin()
    vec = small_call(rounds.hold(rounds.results["vectors"]), w_inner.shape[1])
    rounds.end(vec[0])
    rounds.begin()
    (d_w_outer,) = unpack("outer", rounds.hold(rounds.results["outer"]), ORDERS)
    rounds.end(d_w_outer)
    rounds.begin()
    (d_w_inner,) = unpack("inner", rounds.hold(rounds.results["inner"]), ORDERS)
    rounds.end(d_w_inner)
    rounds.begin()
    rounds.end()
    d_w_query, d_w_key, d_w_value, d_w_output = unpack("attn", rounds.results["attn"], ORDERS)
    return (
        out.reshape(seqs, length, width), d_x.reshape(seqs, length, width),
        d_w_query, vec[0], d_w_key, d_w_value, vec[1], d_w_output, vec[2], vec[3], vec[4],
        d_w_inner, vec[5], d_w_outer, vec[6], vec[7], vec[8],
    )


def solution(mesh):
    rows = P(AXES, None, None)
    return jax.shard_map(
        body, mesh=mesh, in_specs=(rows, P(AXES), rows) + (P(),) * 15, out_specs=(rows, rows) + (P(),) * 15, check_vma=False
    )
```

```python
import functools
import math
import jax
import jax.numpy as jnp
from jax import lax
from jax.experimental import pallas as pl
from jax.experimental.pallas import tpu as pltpu
from jax.sharding import PartitionSpec as P

H = 12
EPS = 1e-12
f32 = jnp.float32
bf16 = jnp.bfloat16
sd = jax.ShapeDtypeStruct
ANY = pl.BlockSpec(memory_space=pl.ANY)
HBM = pl.BlockSpec(memory_space=pltpu.HBM)
VMEM = pl.BlockSpec(memory_space=pltpu.VMEM)
SMEM = pl.BlockSpec(memory_space=pltpu.SMEM)
CHUNK = 384
HALF = CHUNK // 2


def params(mib=60):
    return pltpu.CompilerParams(vmem_limit_bytes=mib * 1024 * 1024)


def cost(flops, nbytes=1 << 20):
    return pl.CostEstimate(flops=int(flops), transcendentals=0, bytes_accessed=int(nbytes))


def nn(a, b):
    return lax.dot_general(a, b, (((1,), (0,)), ((), ())), preferred_element_type=f32)


def nt(a, b):
    return lax.dot_general(a, b, (((1,), (1,)), ((), ())), preferred_element_type=f32)


def tn(a, b):
    return lax.dot_general(a, b, (((0,), (0,)), ((), ())), preferred_element_type=f32)


def own_place():
    dp = lax.axis_index("dp")
    return lax.axis_index("seq"), dp & 7, (dp >> 3) & 1


def row_mean(v):
    return jnp.mean(v, -1, keepdims=True)


def ds(start, size, align=None):
    return pl.ds(pl.multiple_of(start, align or size), size)


FWD_IN = ("x", "wq", "wk", "wv", "wo", "wi", "w2", "dout")
FWD_OUT = ("q", "k", "v", "mixed", "xhat", "rstd", "fin", "out", "dffn")


def row(ref):
    return ref[...].reshape(1, ref.shape[0])


def both(low, v):
    zero = jnp.zeros_like(v)
    return jnp.concatenate([jnp.where(low, v, zero), jnp.where(low, zero, v)], 0)


def pairs_of(width, size):
    return [slice(2 * size * p, 2 * size * (p + 1)) for p in range(width // (2 * size))]


def attention(lens, q, k, v, mixed, lse):
    rows, width = q.shape
    seqs = lens.shape[0]
    length = rows // seqs
    size = width // H
    low = lax.broadcasted_iota(jnp.int32, (length, 2 * size), 1) < size
    pos = lax.broadcasted_iota(jnp.int32, (2, length, 1), 1)

    def chain(s, _):
        r = ds(s * length, length, 32)
        live = pos < lens[s]
        cols = pairs_of(width, size)
        scores = [nt(both(low, k[r, c]), q[r, c]) for c in cols]
        for p, c in enumerate(cols):
            st = jnp.where(live, scores[p].reshape(2, length, length), -1e9)
            top = jnp.max(st, 1, keepdims=True)
            e = jnp.exp(st - top)
            total = jnp.sum(e, 1, keepdims=True)
            lse[s, pl.ds(2 * p, 2), :] = (top + jnp.log(total)).reshape(2, length)
            prob = (e * (1.0 / total)).astype(bf16).reshape(2 * length, length)
            mixed[r, c] = tn(prob, both(low, v[r, c])).astype(bf16)
        return 0

    lax.fori_loop(0, seqs, chain, 0)


def put_blocks(outs, grad, chunk0, me, rows_are_chunks):
    for i in range(2):
        for n, out in enumerate(outs):
            half = (me[0] ^ (1 - n)) * CHUNK
            for t in range(2):
                if rows_are_chunks:
                    value = grad[i * CHUNK + t * HALF : i * CHUNK + (t + 1) * HALF, ds(half, CHUNK)]
                else:
                    value = grad[ds(half + t * HALF, HALF), i * CHUNK : (i + 1) * CHUNK]
                out[((chunk0 + i) ^ me[1]) * 2 + (t ^ me[2])] = value.astype(bf16)


def put_side(out, grad, chunk0, me):
    for i in range(2):
        for t in range(2):
            value = grad[t * HALF : (t + 1) * HALF, i * CHUNK : (i + 1) * CHUNK]
            out[((chunk0 + i) ^ me[1]) * 2 + (t ^ me[2])] = value.astype(bf16)


def pair_part(n, me):
    return pl.ds(4 * (n ^ (me[1] >> 1)), 4)


def fwd_kernel(*refs):
    lens, me = refs[:2]
    bq, bv, bo, g1, s1, bi, b2, g2, s2 = refs[2:11]
    src = dict(zip(FWD_IN, refs[11:19]))
    lse, small = refs[19:21]
    dst = dict(zip(FWD_OUT, refs[21:30]))
    dpre_h = refs[30]
    block_h = refs[31:35]
    rest = refs[35:]
    vin = dict(zip(FWD_IN, rest[:8]))
    vout = dict(zip(FWD_OUT, rest[8:17]))
    dpre = rest[17]
    block = rest[18:22]
    hid, slope, acc, both_grad, sem_in, sem_out, sem_ff, sem_block = rest[22:]
    rows, width = vin["x"].shape
    ff = vin["wi"].shape[1]
    seqs = lens.shape[0]
    length = rows // seqs

    def load(name):
        return pltpu.make_async_copy(src[name], vin[name], sem_in.at[FWD_IN.index(name)])

    def store(name):
        return pltpu.make_async_copy(vout[name], dst[name], sem_out.at[FWD_OUT.index(name)])

    x, q, k, v, mixed = vin["x"], vout["q"], vout["k"], vout["v"], vout["mixed"]
    for name in ("x", "wq", "wk"):
        load(name).start()
    load("x").wait()
    load("wq").wait()
    load("wv").start()
    load("wo").start()
    q[...] = ((nn(x[...], vin["wq"][...]) + row(bq)).astype(bf16).astype(f32) * 0.125).astype(bf16)
    store("q").start()
    load("wk").wait()
    load("wi").start()
    k[...] = nn(x[...], vin["wk"][...]).astype(bf16)
    store("k").start()
    load("wv").wait()
    load("w2").start()
    load("dout").start()
    v[...] = (nn(x[...], vin["wv"][...]) + row(bv)).astype(bf16)
    store("v").start()
    attention(lens, q, k, v, mixed, lse)
    store("mixed").start()
    load("wo").wait()
    xhat, rstd, fin = vout["xhat"], vout["rstd"], vout["fin"]
    acc[...] = nn(mixed[...], vin["wo"][...])
    R = length
    gain1, shift1, bias_o = row(g1), row(s1), row(bo)

    def norm_one(n, _):
        r = ds(n * R, R, 32)
        h = acc[r, :] + bias_o + x[r, :].astype(f32)
        centre = h - row_mean(h)
        scale = lax.rsqrt(row_mean(centre * centre) + EPS)
        unit = centre * scale
        xhat[r, :] = unit
        rstd[r, :] = scale
        fin[r, :] = (unit * gain1 + shift1).astype(bf16)
        return 0

    lax.fori_loop(0, rows // R, norm_one, 0)
    store("rstd").start()
    store("fin").start()
    store("xhat").start()
    wi, w2 = vin["wi"], vin["w2"]
    load("wi").wait()
    load("w2").wait()
    RB = 320
    part_ff = ff // width

    def feed(n, _):
        c = ds(n * width, width)
        bias_i = bi[ds(n * width, width)].reshape(1, width)
        for i in range(rows // RB):
            r = slice(i * RB, (i + 1) * RB)
            u = nn(fin[r, :], wi[:, c]) + bias_i
            cdf = 0.5 * lax.erf(u * 0.7071067811865476) + 0.5
            hid[r, c] = (u * cdf).astype(bf16)
            slope[r, c] = (cdf + u * jnp.exp(-0.5 * (u * u)) * 0.3989422804014327).astype(bf16)
            part = nn(hid[r, c], w2[c, :])
            acc[r, :] = jnp.where(n == 0, part, acc[r, :] + part)
        return 0

    lax.fori_loop(0, part_ff, feed, 0)
    load("dout").wait()
    dout, out, dffn = vin["dout"], vout["out"], vout["dffn"]
    small[...] = jnp.zeros_like(small)
    gain2, shift2, bias_2 = row(g2), row(s2), row(b2)
    pos = lax.broadcasted_iota(jnp.int32, (R, 1), 0)

    def norm_two(n, _):
        r = ds(n * R, R, 32)
        keep = jnp.where(pos < lens[n], 1.0, 0.0).astype(f32)
        h = xhat[r, :] * gain1 + shift1 + (acc[r, :] + bias_2).astype(bf16).astype(f32)
        centre = h - row_mean(h)
        scale = lax.rsqrt(row_mean(centre * centre) + EPS)
        unit = centre * scale
        out[r, :] = ((unit * gain2 + shift2) * keep).astype(bf16)
        g = dout[r, :].astype(f32) * keep
        e = g * gain2
        low = (scale * (e - row_mean(e) - unit * row_mean(e * unit))).astype(bf16)
        dffn[r, :] = low
        small[0:1, :] += jnp.sum(g * unit, 0, keepdims=True)
        small[1:2, :] += jnp.sum(g, 0, keepdims=True)
        small[2:3, :] += jnp.sum(low.astype(f32), 0, keepdims=True)
        return 0

    lax.fori_loop(0, seqs, norm_two, 0)
    store("dffn").start()
    store("out").start()
    def block_copy(i, n):
        part = pair_part(n, me)
        return pltpu.make_async_copy(block[i].at[part], block_h[i].at[part], sem_block.at[i, n])

    def dpre_copy(n):
        c = ds(n * width, width)
        return pltpu.make_async_copy(dpre.at[:, c], dpre_h.at[:, c], sem_ff.at[n])

    def grads(n, _):
        c = ds(n * width, width)
        both_grad[...] = tn(hid[:, c], dffn[...])
        put_blocks(block[0:2], both_grad, 2 * n, me, True)
        block_copy(0, n).start()
        block_copy(1, n).start()
        d = (nt(dffn[...], w2[c, :]) * slope[:, c].astype(f32)).astype(bf16)
        dpre[:, c] = d
        dpre_copy(n).start()
        small[pl.ds(8 + n, 1), :] = jnp.sum(d.astype(f32), 0, keepdims=True)
        both_grad[...] = tn(fin[...], dpre[:, c])
        put_blocks(block[2:4], both_grad, 2 * n, me, False)
        block_copy(2, n).start()
        block_copy(3, n).start()
        return 0

    lax.fori_loop(0, part_ff, grads, 0)
    for name in FWD_OUT:
        store(name).wait()
    for n in range(part_ff):
        dpre_copy(n).wait()
        for i in range(4):
            block_copy(i, n).wait()


def forward(lens, me, vectors, arrays):
    rows, width = arrays[0].shape
    ff = arrays[5].shape[1]
    seqs = lens.shape[0]
    like = lambda shape, dtype=bf16: sd(shape, dtype)
    thin = like((rows, width))
    outs = [thin, thin, thin, thin, like((rows, width), f32), like((rows, 1), f32), thin, thin, thin]
    wide = [like((rows, ff))] + [like((16, HALF, CHUNK))] * 4
    dma = pltpu.SemaphoreType.DMA
    return pl.pallas_call(
        fwd_kernel,
        in_specs=[SMEM, SMEM] + [VMEM] * 9 + [HBM] * 8,
        out_specs=[VMEM, VMEM] + [HBM] * 14,
        out_shape=[like((seqs, H, rows // seqs), f32), like((16, width), f32)] + outs + wide,
        scratch_shapes=[pltpu.VMEM(a.shape, a.dtype) for a in arrays]
        + [pltpu.VMEM(o.shape, o.dtype) for o in outs + wide]
        + [pltpu.VMEM((rows, ff), bf16), pltpu.VMEM((rows, ff), bf16), pltpu.VMEM((rows, width), f32)]
        + [pltpu.VMEM((width, width), f32), dma((8,)), dma((9,)), dma((ff // width,)), dma((4, ff // width))],
        compiler_params=params(),
        cost_estimate=cost(28e9),
        name="forward",
    )(lens, me, *vectors, *arrays)


def attention_bwd(lens, q, k, v, dm, lse, d, small):
    rows, width = q.shape
    seqs = lens.shape[0]
    length = rows // seqs
    size = width // H
    low = lax.broadcasted_iota(jnp.int32, (length, 2 * size), 1) < size
    pos = lax.broadcasted_iota(jnp.int32, (2, length, 1), 1)

    def chain(s, _):
        r = ds(s * length, length, 32)
        live = pos < lens[s]
        cols = pairs_of(width, size)
        first = []
        for c in cols:
            k2 = both(low, k[r, c])
            first.append((k2, nt(k2, q[r, c]), nt(both(low, v[r, c]), dm[r, c])))
        for p, c in enumerate(cols):
            k2, st, dprob = first[p]
            st = jnp.where(live, st.reshape(2, length, length), -1e9)
            dprob = dprob.reshape(2, length, length)
            prob = jnp.exp(st - lse[s, pl.ds(2 * p, 2), :].reshape(2, 1, length))
            delta = jnp.sum(prob * dprob, 1, keepdims=True)
            dst = (prob * (dprob - delta)).astype(bf16).reshape(2 * length, length)
            dv = nn(prob.astype(bf16).reshape(2 * length, length), dm[r, c])
            dk = nn(dst, q[r, c])
            dq = (tn(dst, k2) * 0.125).astype(bf16)
            dv = jnp.where(low, dv[:length], dv[length:]).astype(bf16)
            d[r, c] = dq
            d[r, slice(width + c.start, width + c.stop)] = jnp.where(low, dk[:length], dk[length:]).astype(bf16)
            d[r, slice(2 * width + c.start, 2 * width + c.stop)] = dv
            small[6:7, c] += jnp.sum(dq.astype(f32), 0, keepdims=True)
            small[7:8, c] += jnp.sum(dv.astype(f32), 0, keepdims=True)
        return 0

    lax.fori_loop(0, seqs, chain, 0)


MID_IN = ("dffn", "xhat", "rstd", "wo")


def mid_kernel(*refs):
    g1, small1, dpre_h, wi_h = refs[:4]
    src = dict(zip(MID_IN, refs[4:8]))
    small, dh1_h, dob_h, dm_h = refs[8:12]
    dpre, wi = refs[12:14]
    vin = dict(zip(MID_IN, refs[14:18]))
    dh1, dob, dm, acc, sem_ff, sem_in, sem_out = refs[18:]
    rows, width = acc.shape
    part_ff = dpre.shape[1] // width
    R = 160

    def load(name):
        return pltpu.make_async_copy(src[name], vin[name], sem_in.at[MID_IN.index(name)])

    def ff_copies(n):
        c = ds(n * width, width)
        return (
            pltpu.make_async_copy(dpre_h.at[:, c], dpre.at[:, c], sem_ff.at[0, n]),
            pltpu.make_async_copy(wi_h.at[:, c], wi.at[:, c], sem_ff.at[1, n]),
        )

    for n in range(part_ff):
        for one in ff_copies(n):
            one.start()
    for name in MID_IN:
        load(name).start()
    def products(n, _):
        c = ds(n * width, width)
        for one in ff_copies(n):
            one.wait()
        part = nt(dpre[:, c], wi[:, c])
        acc[...] = jnp.where(n == 0, part, acc[...] + part)
        return 0

    lax.fori_loop(0, part_ff, products, 0)
    small[...] = small1[...]
    gain1 = row(g1)
    dffn, xhat, rstd = vin["dffn"], vin["xhat"], vin["rstd"]
    for name in ("dffn", "xhat", "rstd"):
        load(name).wait()

    def norm_one(i, _):
        r = ds(i * R, R, 32)
        g = dffn[r, :].astype(f32) + acc[r, :].astype(bf16).astype(f32)
        unit = xhat[r, :]
        e = g * gain1
        v = rstd[r, :] * (e - row_mean(e) - unit * row_mean(e * unit))
        dh1[r, :] = v
        low = v.astype(bf16)
        dob[r, :] = low
        small[3:4, :] += jnp.sum(g * unit, 0, keepdims=True)
        small[4:5, :] += jnp.sum(g, 0, keepdims=True)
        small[5:6, :] += jnp.sum(low.astype(f32), 0, keepdims=True)
        return 0

    lax.fori_loop(0, rows // R, norm_one, 0)
    stores = [pltpu.make_async_copy(a, b, sem_out.at[n]) for n, (a, b) in enumerate(((dh1, dh1_h), (dob, dob_h), (dm, dm_h)))]
    stores[0].start()
    stores[1].start()
    load("wo").wait()
    dm[...] = nt(dob[...], vin["wo"][...]).astype(bf16)
    stores[2].start()
    for one in stores:
        one.wait()


def mid_call(g1, small1, dpre, wi, arrays):
    rows, width = arrays[0].shape
    ff = wi.shape[1]
    dma = pltpu.SemaphoreType.DMA
    vm = lambda a: pltpu.VMEM(a.shape, a.dtype)
    outs = [sd((rows, width), f32), sd((rows, width), bf16), sd((rows, width), bf16)]
    return pl.pallas_call(
        mid_kernel,
        in_specs=[VMEM, VMEM] + [HBM] * 6,
        out_specs=[VMEM] + [HBM] * 3,
        out_shape=[sd((16, width), f32)] + outs,
        scratch_shapes=[vm(dpre), vm(wi)] + [vm(a) for a in arrays] + [vm(o) for o in outs]
        + [pltpu.VMEM((rows, width), f32), dma((2, ff // width)), dma((4,)), dma((3,))],
        compiler_params=params(44),
        cost_estimate=cost(10e9),
        name="mid_bwd",
    )(g1, small1, dpre, wi, *arrays)


ATT_IN = ("q", "k", "v", "dm", "lse", "x", "mixed", "dob")


def att_kernel(*refs):
    lens, me, small1 = refs[:3]
    src = dict(zip(ATT_IN, refs[3:11]))
    small, d_h = refs[11:13]
    block_h = refs[13:15]
    rest = refs[15:]
    vin = dict(zip(ATT_IN, rest[:8]))
    d = rest[8]
    block = rest[9:11]
    sem_in, sem_out, sem_block = rest[11:]
    width = d.shape[1] // 4

    def load(name):
        if name == "dob":
            return pltpu.make_async_copy(src[name], d.at[:, 3 * width : 4 * width], sem_in.at[7])
        return pltpu.make_async_copy(src[name], vin[name], sem_in.at[ATT_IN.index(name)])

    for name in ATT_IN:
        load(name).start()
    small[...] = small1[...]
    for name in ("q", "k", "v", "dm", "lse"):
        load(name).wait()
    attention_bwd(lens, vin["q"], vin["k"], vin["v"], vin["dm"], vin["lse"], d, small)
    load("dob").wait()
    d_copy = pltpu.make_async_copy(d, d_h, sem_out.at[0])
    d_copy.start()
    load("x").wait()
    load("mixed").wait()
    def block_copy(i, n):
        part = pair_part(n, me)
        return pltpu.make_async_copy(block[i].at[part], block_h[i].at[part], sem_block.at[i, n])

    sides = (ds((1 - me[0]) * CHUNK, CHUNK), ds(me[0] * CHUNK, CHUNK))

    for n in range(4):
        left = vin["mixed" if n == 3 else "x"]
        for i, side in enumerate(sides):
            put_side(block[i], tn(left[:, side], d[:, n * width : (n + 1) * width]), 2 * n, me)
            block_copy(i, n).start()
    d_copy.wait()
    for n in range(4):
        for i in range(2):
            block_copy(i, n).wait()


def att_call(lens, me, small1, arrays):
    rows, width = arrays[0].shape
    dma = pltpu.SemaphoreType.DMA
    vm = lambda a: pltpu.VMEM(a.shape, a.dtype)
    outs = [sd((rows, 4 * width), bf16)] + [sd((16, HALF, CHUNK), bf16)] * 2
    return pl.pallas_call(
        att_kernel,
        in_specs=[SMEM, SMEM, VMEM] + [HBM] * 8,
        out_specs=[VMEM] + [HBM] * 3,
        out_shape=[sd((16, width), f32)] + outs,
        scratch_shapes=[vm(a) for a in arrays[:7]] + [pltpu.VMEM((8, 128), bf16)] + [vm(o) for o in outs]
        + [dma((8,)), dma((1,)), dma((2, 4))],
        compiler_params=params(50),
        cost_estimate=cost(12e9),
        name="att_bwd",
    )(lens, me, small1, *arrays)


def dx_kernel(dh1_h, d_h, wq_h, wk_h, wv_h, o_h, dh1, d, wq, wk, wv, o, sem, sem_out):
    width = dh1.shape[1]
    loads = []
    for n, (w_h, w) in enumerate(((wq_h, wq), (wk_h, wk), (wv_h, wv))):
        c = slice(n * width, (n + 1) * width)
        loads.append(pltpu.make_async_copy(d_h.at[:, c], d.at[:, c], sem.at[2 * n]))
        loads.append(pltpu.make_async_copy(w_h, w, sem.at[2 * n + 1]))
    loads.insert(2, pltpu.make_async_copy(dh1_h, dh1, sem.at[6]))
    for one in loads:
        one.start()
    loads[0].wait()
    loads[1].wait()
    part = nt(d[:, :width], wq[...])
    loads[2].wait()
    o[...] = dh1[...] + part
    loads[3].wait()
    loads[4].wait()
    o[...] = o[...] + nt(d[:, width : 2 * width], wk[...])
    loads[5].wait()
    loads[6].wait()
    half = dh1.shape[0] // 2
    stores = []
    for i in range(2):
        r = slice(i * half, (i + 1) * half)
        o[r, :] = o[r, :] + nt(d[r, 2 * width : 3 * width], wv[...])
        stores.append(pltpu.make_async_copy(o.at[r, :], o_h.at[r, :], sem_out.at[i]))
        stores[i].start()
    for one in stores:
        one.wait()


def dx_call(dh1, d, wq, wk, wv):
    rows, width = dh1.shape
    dma = pltpu.SemaphoreType.DMA
    return pl.pallas_call(
        dx_kernel,
        in_specs=[HBM] * 5,
        out_specs=HBM,
        out_shape=sd((rows, width), f32),
        scratch_shapes=[
            pltpu.VMEM((rows, width), f32), pltpu.VMEM((rows, 3 * width), bf16), pltpu.VMEM(wq.shape, bf16),
            pltpu.VMEM(wq.shape, bf16), pltpu.VMEM(wq.shape, bf16), pltpu.VMEM((rows, width), f32), dma((7,)), dma((2,)),
        ],
        compiler_params=params(40),
        cost_estimate=cost(5e9),
        name="dx",
    )(dh1, d, wq, wk, wv)


def bit(value, name):
    return (value >> "xya".index(name)) & 1


def unpack_kernel(kind, orders, halves, *refs):
    me = own_place()
    colors = len(orders)
    per = 2 * len(halves)
    n_in = per * colors
    src = refs[:n_in]
    if halves == (1,):
        refs = refs[:n_in] + refs[n_in + 4 :]
    n_out = 4 if kind == "attn" else 1
    outs = refs[n_in : n_in + n_out]
    ins = refs[n_in + n_out : 2 * n_in + n_out]
    buf, sem_in, sem = refs[2 * n_in + n_out :]
    sizes = [src[per * n].shape[1] for n in range(colors)]
    slots = buf.shape[0]

    order_in = [n for first in range(2) for n in range(n_in) if n % 2 == first]
    loads = [pltpu.make_async_copy(src[n], ins[n], sem_in.at[n]) for n in range(n_in)]
    for n in order_in:
        loads[n].start()
    waited = set()

    def copies(step):
        chunk = step ^ me[1]
        slot = step % slots
        if kind == "outer":
            return [(None, pltpu.make_async_copy(buf.at[slot], outs[0].at[ds(chunk * CHUNK, CHUNK), :], sem.at[slot]))]
        if kind == "inner":
            return [(None, pltpu.make_async_copy(buf.at[slot], outs[0].at[:, ds(chunk * CHUNK, CHUNK)], sem.at[slot]))]
        rows = pl.ds(0, 2 * CHUNK) if len(halves) == 2 else ds((halves[0] ^ me[0]) * CHUNK, CHUNK)
        cols = ds((chunk % 2) * CHUNK, CHUNK)
        return [
            (chunk // 2 == m, pltpu.make_async_copy(buf.at[slot, rows], outs[m].at[rows, cols], sem.at[slot]))
            for m in range(4)
        ]

    def each(step, act):
        for cond, one in copies(step):
            if cond is None:
                act(one)
            else:
                pl.when(cond)(functools.partial(act, one))

    for step in range(8):
        slot = step % slots
        if step >= slots:
            each(step - slots, lambda one: one.wait())
        for half in halves:
            place = (half ^ me[0]) * CHUNK
            for n in range(colors):
                order, size, first = orders[n], sizes[n], sum(sizes[:n])
                at = per * n + (2 * half if len(halves) == 2 else 0) + bit(step, order[0])
                if at not in waited:
                    waited.add(at)
                    loads[at].wait()
                for t in range(2):
                    bits = [t if c == "b" else bit(step, c) for c in order]
                    where = bits[1] * 4 + bits[2] * 2 + bits[3]
                    start = (t ^ me[2]) * HALF + first
                    value = ins[at][where].astype(f32)
                    if kind == "outer":
                        buf[slot, ds(start, size, 16), ds(place, CHUNK)] = value
                    else:
                        buf[slot, ds(place + start, size, 16), :] = value
        each(step, lambda one: one.start())
    for step in range(8 - slots, 8):
        each(step, lambda one: one.wait())


def unpack(kind, pieces, orders, halves=(0, 1), into=()):
    colors = len(orders)
    width = 2 * CHUNK
    if kind == "outer":
        out_shape = [sd((8 * CHUNK, width), f32)]
    elif kind == "inner":
        out_shape = [sd((width, 8 * CHUNK), f32)]
    else:
        out_shape = [sd((width, width), f32)] * 4
    buf = (4, CHUNK, width) if kind == "outer" else (4, width, CHUNK)
    dma = pltpu.SemaphoreType.DMA
    return pl.pallas_call(
        functools.partial(unpack_kernel, kind, orders, halves),
        in_specs=[ANY] * len(pieces) + [HBM] * len(into),
        out_specs=[HBM] * len(out_shape),
        out_shape=out_shape,
        scratch_shapes=[pltpu.VMEM(v.shape, v.dtype) for v in pieces]
        + [pltpu.VMEM(buf, f32), dma((len(pieces),)), dma((4,))],
        compiler_params=params(22),
        cost_estimate=cost(4e9),
        name="unpack_" + kind,
        input_output_aliases={len(pieces) + n: n for n in range(len(into))},
    )(*pieces, *into)


SMALL_ROWS = (6, 7, 5, 3, 4, 8, 2, 0, 1)


def small_kernel(total, *outs):
    half = total.shape[1]
    for at, out in zip(SMALL_ROWS, outs):
        for n in range(out.shape[0] // half):
            line = at + n // 2 + (n % 2) * (total.shape[0] // 2)
            out[pl.ds(n * half, half)] = total[line : line + 1, :].reshape(half)


def small_call(total, ff):
    width = 2 * total.shape[1]
    sizes = [ff if at == 8 else width for at in SMALL_ROWS]
    return pl.pallas_call(
        small_kernel,
        in_specs=[VMEM],
        out_specs=[VMEM] * 9,
        out_shape=[sd((n,), f32) for n in sizes],
        compiler_params=params(4),
        cost_estimate=cost(1e9),
        name="vectors",
    )(total)


AXES = ("dp", "seq")
DP_BIT = {"x": 0, "y": 1, "a": 2, "b": 3}


def swap(value, name):
    dp = lax.axis_size("dp")
    seq = lax.axis_size("seq")
    flip = 1 if name == "c" else seq << (name if isinstance(name, int) else DP_BIT[name])
    return lax.ppermute(value, AXES, [(i, i ^ flip) for i in range(dp * seq)])


ORDERS = ("xyab", "yaxb", "axyb")


def pick(value, at, n):
    return lax.index_in_dim(value, n, at, keepdims=False)


def cut(value, sizes):
    return [value[..., sum(sizes[:n]) : sum(sizes[: n + 1]), :] for n in range(len(sizes))]


EVEN = (64, 64, 64)
LEAN = (80, 64, 48)


def reduction(keep, got, down=EVEN, up=EVEN):
    shape = (2, 2, 2, 2, HALF, CHUNK)
    keeps = cut(keep.reshape(shape), down)
    gots = cut(got.reshape(shape), down)
    dims = ["ayxb"] * 3
    for level in range(3):
        places = [d.index(o[level]) for d, o in zip(dims, ORDERS)]
        sends = [pick(k, at, 1) + pick(g, at, 1) for k, g, at in zip(keeps, gots, places)]
        keeps = [pick(k, at, 0) + pick(g, at, 0) for k, g, at in zip(keeps, gots, places)]
        dims = [d.replace(o[level], "") for d, o in zip(dims, ORDERS)]
        gots = yield [(o[level], v) for o, v in zip(ORDERS, sends)]
    own = jnp.concatenate([k + g for k, g in zip(keeps, gots)], -2)
    (got,) = yield [("b", own)]
    own = own + jnp.concatenate([got[1:], got[:1]])
    for extra in range(4, lax.axis_size("dp").bit_length() - 1):
        own = own + swap(own, extra)
    owns = cut(own, up)
    for level in (2, 1):
        gots = yield [(o[level], v) for o, v in zip(ORDERS, owns)]
        owns = [jnp.stack(v) for v in zip(owns, gots)]
    owns = [v.reshape((8,) + v.shape[-2:]) for v in owns]
    gots = yield [(o[0], v) for o, v in zip(ORDERS, owns)] + [("c", v) for v in owns]
    near, far = gots[:3], gots[3:]
    others = yield [("c", v) for v in near], (owns, near)
    return [v for four in zip(owns, near, far, others) for v in four]


def vector_sum(small):
    half = small.shape[1] // 2
    value = jnp.concatenate([small[:, :half], small[:, half:]])
    links = ["c"] + list("axyb") + list(range(4, lax.axis_size("dp").bit_length() - 1))
    for link in links:
        sent = value.astype(bf16)
        if isinstance(link, int):
            got = swap(sent, link)
        else:
            (got,) = yield [(link, sent)]
        value = sent.astype(f32) + got.astype(f32)
    return value


def unroll(v):
    return v.reshape((-1, v.shape[-1]))


class Rounds:
    def __init__(self):
        self.flows = {}
        self.results = {}
        self.parts = {}
        self.wanted = {}
        self.mark = ()

    def add(self, name, flow):
        self.flows[name] = flow
        self.wanted[name] = next(flow)

    def hold(self, value):
        return lax.optimization_barrier((value,) + self.mark)[0]

    def begin(self, extra=(), skip=()):
        self.order = [(name, n) for name in self.wanted if name not in skip for n in range(len(self.wanted[name]))]
        links = {}
        alone = {}
        for name, n in self.order:
            link, value = self.wanted[name][n]
            if link == "c":
                alone[name, n] = value
            else:
                links.setdefault(link, []).append((name, n))
        merged = {}
        for link, keys in links.items():
            values = [self.wanted[k][n][1] for k, n in keys]
            merged[link] = values[0] if len(values) == 1 else jnp.concatenate([unroll(v) for v in values])
        merged, alone, extra = lax.optimization_barrier((merged, alone, tuple(extra)))
        self.mark = tuple(merged.values())
        self.got = {}
        for link in "baxy":
            if link not in links:
                continue
            keys = links[link]
            got = swap(merged[link], link)
            if len(keys) == 1:
                self.got[keys[0]] = got
                continue
            row = 0
            for k, n in keys:
                shape = self.wanted[k][n][1].shape
                count = math.prod(shape[:-1])
                self.got[k, n] = got[row : row + count].reshape(shape)
                row += count
        for key, value in alone.items():
            self.got[key] = swap(value, "c")
        return [swap(v, "c") for v in extra]

    def end(self, *beside):
        got, _ = lax.optimization_barrier((self.got, tuple(beside)))
        for name in list(self.flows):
            if name not in self.wanted or (name, 0) not in got:
                continue
            values = [got[name, n] for n in range(len(self.wanted[name]))]
            try:
                wanted = self.flows[name].send(values)
                if isinstance(wanted, tuple):
                    wanted, self.parts[name] = wanted
                self.wanted[name] = wanted
            except StopIteration as stop:
                self.results[name] = stop.value
                del self.flows[name], self.wanted[name]


def body(chains_in, lengths, d_out, w_query, b_query, w_key, w_value, b_value, w_output, b_output, gain_one, shift_one,
         w_inner, b_inner, w_outer, b_outer, gain_two, shift_two):
    seqs, length, width = chains_in.shape
    rows = seqs * length
    place = lax.axis_index("dp") * 2 + lax.axis_index("seq")
    me = (place >> jnp.array([0, 1, 4], jnp.int32)) & jnp.array([1, 7, 1], jnp.int32)
    x = chains_in.reshape(rows, width)
    lse, small, q, k, v, mixed, xhat, rstd, fin, out, dffn, dpre, send_o, keep_o, send_i, keep_i = forward(
        lengths, me, (b_query, b_value, b_output, gain_one, shift_one, b_inner, b_outer, gain_two, shift_two),
        (x, w_query, w_key, w_value, w_output, w_inner, w_outer, d_out.reshape(rows, width)),
    )
    rounds = Rounds()
    got_o, got_i = rounds.begin([send_o, send_i])
    rounds.add("outer", reduction(keep_o, got_o))
    rounds.begin()
    small, dh1, dob, dm = mid_call(gain_one, small, rounds.hold(dpre), w_inner, (dffn, xhat, rstd, w_output))
    got_i, dm = lax.optimization_barrier((got_i, dm))
    rounds.end(dh1, dob, dm)
    rounds.add("inner", reduction(keep_i, got_i))
    rounds.begin()
    small, d, send, keep = att_call(lengths, me, small, (q, k, v, rounds.hold(dm), lse, x, mixed, dob))
    rounds.end(d, send)
    rounds.add("vectors", vector_sum(small))
    (got,) = rounds.begin([send])
    d_x = dx_call(rounds.hold(dh1), d, w_query, w_key, w_value)
    got, d_x = lax.optimization_barrier((got, d_x))
    rounds.end(got)
    rounds.add("attn", reduction(keep, got))
    for _ in range(4):
        rounds.begin()
        rounds.end()
    rounds.begin()
    vec = small_call(rounds.hold(rounds.results["vectors"]), w_inner.shape[1])
    rounds.end(vec[0])
    rounds.begin()
    (d_w_outer,) = unpack("outer", rounds.hold(rounds.results["outer"]), ORDERS)
    rounds.end(d_w_outer)
    rounds.begin()
    (d_w_inner,) = unpack("inner", rounds.hold(rounds.results["inner"]), ORDERS)
    rounds.end(d_w_inner)
    rounds.begin()
    owns, nears = rounds.hold(rounds.parts["attn"])
    grads = unpack("attn", [v for two in zip(owns, nears) for v in two], ORDERS, (0,))
    rounds.end()
    pieces = rounds.results["attn"]
    far = [v for n in range(3) for v in pieces[4 * n + 2 : 4 * n + 4]]
    d_w_query, d_w_key, d_w_value, d_w_output = unpack("attn", far, ORDERS, (1,), grads)
    return (
        out.reshape(seqs, length, width), d_x.reshape(seqs, length, width),
        d_w_query, vec[0], d_w_key, d_w_value, vec[1], d_w_output, vec[2], vec[3], vec[4],
        d_w_inner, vec[5], d_w_outer, vec[6], vec[7], vec[8],
    )


def solution(mesh):
    rows = P(AXES, None, None)
    return jax.shard_map(
        body, mesh=mesh, in_specs=(rows, P(AXES), rows) + (P(),) * 15, out_specs=(rows, rows) + (P(),) * 15, check_vma=False
    )
```

```python
import functools
import math
import jax
import jax.numpy as jnp
from jax import lax
from jax.experimental import pallas as pl
from jax.experimental.pallas import tpu as pltpu
from jax.sharding import PartitionSpec as P

H = 12
EPS = 1e-12
f32 = jnp.float32
bf16 = jnp.bfloat16
sd = jax.ShapeDtypeStruct
ANY = pl.BlockSpec(memory_space=pl.ANY)
HBM = pl.BlockSpec(memory_space=pltpu.HBM)
VMEM = pl.BlockSpec(memory_space=pltpu.VMEM)
SMEM = pl.BlockSpec(memory_space=pltpu.SMEM)
CHUNK = 384
HALF = CHUNK // 2


def params(mib=60):
    return pltpu.CompilerParams(vmem_limit_bytes=mib * 1024 * 1024)


def cost(flops, nbytes=1 << 20):
    return pl.CostEstimate(flops=int(flops), transcendentals=0, bytes_accessed=int(nbytes))


def nn(a, b):
    return lax.dot_general(a, b, (((1,), (0,)), ((), ())), preferred_element_type=f32)


def nt(a, b):
    return lax.dot_general(a, b, (((1,), (1,)), ((), ())), preferred_element_type=f32)


def tn(a, b):
    return lax.dot_general(a, b, (((0,), (0,)), ((), ())), preferred_element_type=f32)


def own_place():
    dp = lax.axis_index("dp")
    return lax.axis_index("seq"), dp & 7, (dp >> 3) & 1


def row_mean(v):
    return jnp.mean(v, -1, keepdims=True)


def ds(start, size, align=None):
    return pl.ds(pl.multiple_of(start, align or size), size)


FWD_IN = ("x", "wq", "wk", "wv", "wo", "wi", "w2", "dout")
FWD_OUT = ("q", "k", "v", "mixed", "xhat", "rstd", "fin", "out", "dffn")


def row(ref):
    return ref[...].reshape(1, ref.shape[0])


def both(low, v):
    zero = jnp.zeros_like(v)
    return jnp.concatenate([jnp.where(low, v, zero), jnp.where(low, zero, v)], 0)


def pairs_of(width, size):
    return [slice(2 * size * p, 2 * size * (p + 1)) for p in range(width // (2 * size))]


def attention(lens, q, k, v, mixed, lse):
    rows, width = q.shape
    seqs = lens.shape[0]
    length = rows // seqs
    size = width // H
    low = lax.broadcasted_iota(jnp.int32, (length, 2 * size), 1) < size
    pos = lax.broadcasted_iota(jnp.int32, (2, length, 1), 1)

    def chain(s, _):
        r = ds(s * length, length, 32)
        live = pos < lens[s]
        cols = pairs_of(width, size)
        scores = [nt(both(low, k[r, c]), q[r, c]) for c in cols]
        for p, c in enumerate(cols):
            st = jnp.where(live, scores[p].reshape(2, length, length), -1e9)
            top = jnp.max(st, 1, keepdims=True)
            e = jnp.exp(st - top)
            total = jnp.sum(e, 1, keepdims=True)
            lse[s, pl.ds(2 * p, 2), :] = (top + jnp.log(total)).reshape(2, length)
            prob = (e * (1.0 / total)).astype(bf16).reshape(2 * length, length)
            mixed[r, c] = tn(prob, both(low, v[r, c])).astype(bf16)
        return 0

    lax.fori_loop(0, seqs, chain, 0)


def put_blocks(outs, grad, chunk0, me, rows_are_chunks):
    for i in range(2):
        for n, out in enumerate(outs):
            half = (me[0] ^ (1 - n)) * CHUNK
            for t in range(2):
                if rows_are_chunks:
                    value = grad[i * CHUNK + t * HALF : i * CHUNK + (t + 1) * HALF, ds(half, CHUNK)]
                else:
                    value = grad[ds(half + t * HALF, HALF), i * CHUNK : (i + 1) * CHUNK]
                out[((chunk0 + i) ^ me[1]) * 2 + (t ^ me[2])] = value.astype(bf16)


def put_side(out, grad, chunk0, me):
    for i in range(2):
        for t in range(2):
            value = grad[t * HALF : (t + 1) * HALF, i * CHUNK : (i + 1) * CHUNK]
            out[((chunk0 + i) ^ me[1]) * 2 + (t ^ me[2])] = value.astype(bf16)


def pair_part(n, me):
    return pl.ds(4 * (n ^ (me[1] >> 1)), 4)


def fwd_kernel(*refs):
    lens, me = refs[:2]
    bq, bv, bo, g1, s1, bi, b2, g2, s2 = refs[2:11]
    src = dict(zip(FWD_IN, refs[11:19]))
    lse, small = refs[19:21]
    dst = dict(zip(FWD_OUT, refs[21:30]))
    dpre_h = refs[30]
    block_h = refs[31:35]
    rest = refs[35:]
    vin = dict(zip(FWD_IN, rest[:8]))
    vout = dict(zip(FWD_OUT, rest[8:17]))
    dpre = rest[17]
    block = rest[18:22]
    hid, slope, acc, both_grad, sem_in, sem_out, sem_ff, sem_block = rest[22:]
    rows, width = vin["x"].shape
    ff = vin["wi"].shape[1]
    seqs = lens.shape[0]
    length = rows // seqs

    def load(name):
        return pltpu.make_async_copy(src[name], vin[name], sem_in.at[FWD_IN.index(name)])

    def store(name):
        return pltpu.make_async_copy(vout[name], dst[name], sem_out.at[FWD_OUT.index(name)])

    x, q, k, v, mixed = vin["x"], vout["q"], vout["k"], vout["v"], vout["mixed"]
    for name in ("x", "wq", "wk"):
        load(name).start()
    load("x").wait()
    load("wq").wait()
    load("wv").start()
    load("wo").start()
    q[...] = ((nn(x[...], vin["wq"][...]) + row(bq)).astype(bf16).astype(f32) * 0.125).astype(bf16)
    store("q").start()
    load("wk").wait()
    load("wi").start()
    k[...] = nn(x[...], vin["wk"][...]).astype(bf16)
    store("k").start()
    load("wv").wait()
    load("w2").start()
    load("dout").start()
    v[...] = (nn(x[...], vin["wv"][...]) + row(bv)).astype(bf16)
    store("v").start()
    attention(lens, q, k, v, mixed, lse)
    store("mixed").start()
    load("wo").wait()
    xhat, rstd, fin = vout["xhat"], vout["rstd"], vout["fin"]
    acc[...] = nn(mixed[...], vin["wo"][...])
    R = length
    gain1, shift1, bias_o = row(g1), row(s1), row(bo)

    def norm_one(n, _):
        r = ds(n * R, R, 32)
        h = acc[r, :] + bias_o + x[r, :].astype(f32)
        centre = h - row_mean(h)
        scale = lax.rsqrt(row_mean(centre * centre) + EPS)
        unit = centre * scale
        xhat[r, :] = unit
        rstd[r, :] = scale
        fin[r, :] = (unit * gain1 + shift1).astype(bf16)
        return 0

    lax.fori_loop(0, rows // R, norm_one, 0)
    store("rstd").start()
    store("fin").start()
    store("xhat").start()
    wi, w2 = vin["wi"], vin["w2"]
    load("wi").wait()
    load("w2").wait()
    RB = 320
    part_ff = ff // width

    def feed(n, _):
        c = ds(n * width, width)
        bias_i = bi[ds(n * width, width)].reshape(1, width)
        for i in range(rows // RB):
            r = slice(i * RB, (i + 1) * RB)
            u = nn(fin[r, :], wi[:, c]) + bias_i
            cdf = 0.5 * lax.erf(u * 0.7071067811865476) + 0.5
            hid[r, c] = (u * cdf).astype(bf16)
            slope[r, c] = (cdf + u * jnp.exp(-0.5 * (u * u)) * 0.3989422804014327).astype(bf16)
            part = nn(hid[r, c], w2[c, :])
            acc[r, :] = jnp.where(n == 0, part, acc[r, :] + part)
        return 0

    lax.fori_loop(0, part_ff, feed, 0)
    load("dout").wait()
    dout, out, dffn = vin["dout"], vout["out"], vout["dffn"]
    small[...] = jnp.zeros_like(small)
    gain2, shift2, bias_2 = row(g2), row(s2), row(b2)
    pos = lax.broadcasted_iota(jnp.int32, (R, 1), 0)

    def norm_two(n, _):
        r = ds(n * R, R, 32)
        keep = jnp.where(pos < lens[n], 1.0, 0.0).astype(f32)
        h = xhat[r, :] * gain1 + shift1 + (acc[r, :] + bias_2).astype(bf16).astype(f32)
        centre = h - row_mean(h)
        scale = lax.rsqrt(row_mean(centre * centre) + EPS)
        unit = centre * scale
        out[r, :] = ((unit * gain2 + shift2) * keep).astype(bf16)
        g = dout[r, :].astype(f32) * keep
        e = g * gain2
        low = (scale * (e - row_mean(e) - unit * row_mean(e * unit))).astype(bf16)
        dffn[r, :] = low
        small[0:1, :] += jnp.sum(g * unit, 0, keepdims=True)
        small[1:2, :] += jnp.sum(g, 0, keepdims=True)
        small[2:3, :] += jnp.sum(low.astype(f32), 0, keepdims=True)
        return 0

    lax.fori_loop(0, seqs, norm_two, 0)
    store("dffn").start()
    store("out").start()
    def block_copy(i, n):
        part = pair_part(n, me)
        return pltpu.make_async_copy(block[i].at[part], block_h[i].at[part], sem_block.at[i, n])

    def dpre_copy(n):
        c = ds(n * width, width)
        return pltpu.make_async_copy(dpre.at[:, c], dpre_h.at[:, c], sem_ff.at[n])

    def grads(n, _):
        c = ds(n * width, width)
        both_grad[...] = tn(hid[:, c], dffn[...])
        put_blocks(block[0:2], both_grad, 2 * n, me, True)
        block_copy(0, n).start()
        block_copy(1, n).start()
        d = (nt(dffn[...], w2[c, :]) * slope[:, c].astype(f32)).astype(bf16)
        dpre[:, c] = d
        dpre_copy(n).start()
        small[pl.ds(8 + n, 1), :] = jnp.sum(d.astype(f32), 0, keepdims=True)
        both_grad[...] = tn(fin[...], dpre[:, c])
        put_blocks(block[2:4], both_grad, 2 * n, me, False)
        block_copy(2, n).start()
        block_copy(3, n).start()
        return 0

    lax.fori_loop(0, part_ff, grads, 0)
    for name in FWD_OUT:
        store(name).wait()
    for n in range(part_ff):
        dpre_copy(n).wait()
        for i in range(4):
            block_copy(i, n).wait()


def forward(lens, me, vectors, arrays):
    rows, width = arrays[0].shape
    ff = arrays[5].shape[1]
    seqs = lens.shape[0]
    like = lambda shape, dtype=bf16: sd(shape, dtype)
    thin = like((rows, width))
    outs = [thin, thin, thin, thin, like((rows, width), f32), like((rows, 1), f32), thin, thin, thin]
    wide = [like((rows, ff))] + [like((16, HALF, CHUNK))] * 4
    dma = pltpu.SemaphoreType.DMA
    return pl.pallas_call(
        fwd_kernel,
        in_specs=[SMEM, SMEM] + [VMEM] * 9 + [HBM] * 8,
        out_specs=[VMEM, VMEM] + [HBM] * 14,
        out_shape=[like((seqs, H, rows // seqs), f32), like((16, width), f32)] + outs + wide,
        scratch_shapes=[pltpu.VMEM(a.shape, a.dtype) for a in arrays]
        + [pltpu.VMEM(o.shape, o.dtype) for o in outs + wide]
        + [pltpu.VMEM((rows, ff), bf16), pltpu.VMEM((rows, ff), bf16), pltpu.VMEM((rows, width), f32)]
        + [pltpu.VMEM((width, width), f32), dma((8,)), dma((9,)), dma((ff // width,)), dma((4, ff // width))],
        compiler_params=params(),
        cost_estimate=cost(28e9),
        name="forward",
    )(lens, me, *vectors, *arrays)


def attention_bwd(lens, q, k, v, dm, lse, d, small):
    rows, width = q.shape
    seqs = lens.shape[0]
    length = rows // seqs
    size = width // H
    low = lax.broadcasted_iota(jnp.int32, (length, 2 * size), 1) < size
    pos = lax.broadcasted_iota(jnp.int32, (2, length, 1), 1)

    def chain(s, _):
        r = ds(s * length, length, 32)
        live = pos < lens[s]
        cols = pairs_of(width, size)
        first = []
        for c in cols:
            k2 = both(low, k[r, c])
            first.append((k2, nt(k2, q[r, c]), nt(both(low, v[r, c]), dm[r, c])))
        for p, c in enumerate(cols):
            k2, st, dprob = first[p]
            st = jnp.where(live, st.reshape(2, length, length), -1e9)
            dprob = dprob.reshape(2, length, length)
            prob = jnp.exp(st - lse[s, pl.ds(2 * p, 2), :].reshape(2, 1, length))
            delta = jnp.sum(prob * dprob, 1, keepdims=True)
            dst = (prob * (dprob - delta)).astype(bf16).reshape(2 * length, length)
            dv = nn(prob.astype(bf16).reshape(2 * length, length), dm[r, c])
            dk = nn(dst, q[r, c])
            dq = (tn(dst, k2) * 0.125).astype(bf16)
            dv = jnp.where(low, dv[:length], dv[length:]).astype(bf16)
            d[r, c] = dq
            d[r, slice(width + c.start, width + c.stop)] = jnp.where(low, dk[:length], dk[length:]).astype(bf16)
            d[r, slice(2 * width + c.start, 2 * width + c.stop)] = dv
            small[6:7, c] += jnp.sum(dq.astype(f32), 0, keepdims=True)
            small[7:8, c] += jnp.sum(dv.astype(f32), 0, keepdims=True)
        return 0

    lax.fori_loop(0, seqs, chain, 0)


MID_IN = ("dffn", "xhat", "rstd", "wo")


def mid_kernel(*refs):
    g1, small1, dpre_h, wi_h = refs[:4]
    src = dict(zip(MID_IN, refs[4:8]))
    small, dh1_h, dob_h, dm_h = refs[8:12]
    dpre, wi = refs[12:14]
    vin = dict(zip(MID_IN, refs[14:18]))
    dh1, dob, dm, acc, sem_ff, sem_in, sem_out = refs[18:]
    rows, width = acc.shape
    part_ff = dpre.shape[1] // width
    R = 160

    def load(name):
        return pltpu.make_async_copy(src[name], vin[name], sem_in.at[MID_IN.index(name)])

    def ff_copies(n):
        c = ds(n * width, width)
        return (
            pltpu.make_async_copy(dpre_h.at[:, c], dpre.at[:, c], sem_ff.at[0, n]),
            pltpu.make_async_copy(wi_h.at[:, c], wi.at[:, c], sem_ff.at[1, n]),
        )

    for n in range(part_ff):
        for one in ff_copies(n):
            one.start()
    for name in MID_IN:
        load(name).start()
    def products(n, _):
        c = ds(n * width, width)
        for one in ff_copies(n):
            one.wait()
        part = nt(dpre[:, c], wi[:, c])
        acc[...] = jnp.where(n == 0, part, acc[...] + part)
        return 0

    lax.fori_loop(0, part_ff, products, 0)
    small[...] = small1[...]
    gain1 = row(g1)
    dffn, xhat, rstd = vin["dffn"], vin["xhat"], vin["rstd"]
    for name in ("dffn", "xhat", "rstd"):
        load(name).wait()

    def norm_one(i, _):
        r = ds(i * R, R, 32)
        g = dffn[r, :].astype(f32) + acc[r, :].astype(bf16).astype(f32)
        unit = xhat[r, :]
        e = g * gain1
        v = rstd[r, :] * (e - row_mean(e) - unit * row_mean(e * unit))
        dh1[r, :] = v
        low = v.astype(bf16)
        dob[r, :] = low
        small[3:4, :] += jnp.sum(g * unit, 0, keepdims=True)
        small[4:5, :] += jnp.sum(g, 0, keepdims=True)
        small[5:6, :] += jnp.sum(low.astype(f32), 0, keepdims=True)
        return 0

    lax.fori_loop(0, rows // R, norm_one, 0)
    stores = [pltpu.make_async_copy(a, b, sem_out.at[n]) for n, (a, b) in enumerate(((dh1, dh1_h), (dob, dob_h), (dm, dm_h)))]
    stores[0].start()
    stores[1].start()
    load("wo").wait()
    dm[...] = nt(dob[...], vin["wo"][...]).astype(bf16)
    stores[2].start()
    for one in stores:
        one.wait()


def mid_call(g1, small1, dpre, wi, arrays):
    rows, width = arrays[0].shape
    ff = wi.shape[1]
    dma = pltpu.SemaphoreType.DMA
    vm = lambda a: pltpu.VMEM(a.shape, a.dtype)
    outs = [sd((rows, width), f32), sd((rows, width), bf16), sd((rows, width), bf16)]
    return pl.pallas_call(
        mid_kernel,
        in_specs=[VMEM, VMEM] + [HBM] * 6,
        out_specs=[VMEM] + [HBM] * 3,
        out_shape=[sd((16, width), f32)] + outs,
        scratch_shapes=[vm(dpre), vm(wi)] + [vm(a) for a in arrays] + [vm(o) for o in outs]
        + [pltpu.VMEM((rows, width), f32), dma((2, ff // width)), dma((4,)), dma((3,))],
        compiler_params=params(44),
        cost_estimate=cost(10e9),
        name="mid_bwd",
    )(g1, small1, dpre, wi, *arrays)


ATT_IN = ("q", "k", "v", "dm", "lse", "x", "mixed", "dob")


def att_kernel(*refs):
    lens, me, small1 = refs[:3]
    src = dict(zip(ATT_IN, refs[3:11]))
    small, d_h = refs[11:13]
    block_h = refs[13:15]
    rest = refs[15:]
    vin = dict(zip(ATT_IN, rest[:8]))
    d = rest[8]
    block = rest[9:11]
    sem_in, sem_out, sem_block = rest[11:]
    width = d.shape[1] // 4

    def load(name):
        if name == "dob":
            return pltpu.make_async_copy(src[name], d.at[:, 3 * width : 4 * width], sem_in.at[7])
        return pltpu.make_async_copy(src[name], vin[name], sem_in.at[ATT_IN.index(name)])

    for name in ATT_IN:
        load(name).start()
    small[...] = small1[...]
    for name in ("q", "k", "v", "dm", "lse"):
        load(name).wait()
    attention_bwd(lens, vin["q"], vin["k"], vin["v"], vin["dm"], vin["lse"], d, small)
    load("dob").wait()
    d_copy = pltpu.make_async_copy(d, d_h, sem_out.at[0])
    d_copy.start()
    load("x").wait()
    load("mixed").wait()
    def block_copy(i, n):
        part = pair_part(n, me)
        return pltpu.make_async_copy(block[i].at[part], block_h[i].at[part], sem_block.at[i, n])

    sides = (ds((1 - me[0]) * CHUNK, CHUNK), ds(me[0] * CHUNK, CHUNK))

    for n in range(4):
        left = vin["mixed" if n == 3 else "x"]
        for i, side in enumerate(sides):
            put_side(block[i], tn(left[:, side], d[:, n * width : (n + 1) * width]), 2 * n, me)
            block_copy(i, n).start()
    d_copy.wait()
    for n in range(4):
        for i in range(2):
            block_copy(i, n).wait()


def att_call(lens, me, small1, arrays):
    rows, width = arrays[0].shape
    dma = pltpu.SemaphoreType.DMA
    vm = lambda a: pltpu.VMEM(a.shape, a.dtype)
    outs = [sd((rows, 4 * width), bf16)] + [sd((16, HALF, CHUNK), bf16)] * 2
    return pl.pallas_call(
        att_kernel,
        in_specs=[SMEM, SMEM, VMEM] + [HBM] * 8,
        out_specs=[VMEM] + [HBM] * 3,
        out_shape=[sd((16, width), f32)] + outs,
        scratch_shapes=[vm(a) for a in arrays[:7]] + [pltpu.VMEM((8, 128), bf16)] + [vm(o) for o in outs]
        + [dma((8,)), dma((1,)), dma((2, 4))],
        compiler_params=params(50),
        cost_estimate=cost(12e9),
        name="att_bwd",
    )(lens, me, small1, *arrays)


def dx_kernel(dh1_h, d_h, wq_h, wk_h, wv_h, o_h, dh1, d, wq, wk, wv, o, sem, sem_out):
    width = dh1.shape[1]
    loads = []
    for n, (w_h, w) in enumerate(((wq_h, wq), (wk_h, wk), (wv_h, wv))):
        c = slice(n * width, (n + 1) * width)
        loads.append(pltpu.make_async_copy(d_h.at[:, c], d.at[:, c], sem.at[2 * n]))
        loads.append(pltpu.make_async_copy(w_h, w, sem.at[2 * n + 1]))
    loads.insert(2, pltpu.make_async_copy(dh1_h, dh1, sem.at[6]))
    for one in loads:
        one.start()
    loads[0].wait()
    loads[1].wait()
    part = nt(d[:, :width], wq[...])
    loads[2].wait()
    o[...] = dh1[...] + part
    loads[3].wait()
    loads[4].wait()
    o[...] = o[...] + nt(d[:, width : 2 * width], wk[...])
    loads[5].wait()
    loads[6].wait()
    half = dh1.shape[0] // 2
    stores = []
    for i in range(2):
        r = slice(i * half, (i + 1) * half)
        o[r, :] = o[r, :] + nt(d[r, 2 * width : 3 * width], wv[...])
        stores.append(pltpu.make_async_copy(o.at[r, :], o_h.at[r, :], sem_out.at[i]))
        stores[i].start()
    for one in stores:
        one.wait()


def dx_call(dh1, d, wq, wk, wv):
    rows, width = dh1.shape
    dma = pltpu.SemaphoreType.DMA
    return pl.pallas_call(
        dx_kernel,
        in_specs=[HBM] * 5,
        out_specs=HBM,
        out_shape=sd((rows, width), f32),
        scratch_shapes=[
            pltpu.VMEM((rows, width), f32), pltpu.VMEM((rows, 3 * width), bf16), pltpu.VMEM(wq.shape, bf16),
            pltpu.VMEM(wq.shape, bf16), pltpu.VMEM(wq.shape, bf16), pltpu.VMEM((rows, width), f32), dma((7,)), dma((2,)),
        ],
        compiler_params=params(42),
        cost_estimate=cost(5e9),
        name="dx",
    )(dh1, d, wq, wk, wv)


def bit(value, name):
    return (value >> "xya".index(name)) & 1


def unpack_kernel(kind, orders, halves, *refs):
    me = own_place()
    colors = len(orders)
    per = 2 * len(halves)
    n_in = per * colors
    src = refs[:n_in]
    if halves == (1,):
        refs = refs[:n_in] + refs[n_in + 4 :]
    n_out = 4 if kind == "attn" else 1
    outs = refs[n_in : n_in + n_out]
    ins = refs[n_in + n_out : 2 * n_in + n_out]
    buf, sem_in, sem = refs[2 * n_in + n_out :]
    sizes = [src[per * n].shape[1] for n in range(colors)]
    slots = buf.shape[0]

    order_in = [n for first in range(2) for n in range(n_in) if n % 2 == first]
    loads = [pltpu.make_async_copy(src[n], ins[n], sem_in.at[n]) for n in range(n_in)]
    for n in order_in:
        loads[n].start()
    waited = set()

    def copies(step):
        chunk = step ^ me[1]
        slot = step % slots
        if kind == "outer":
            return [(None, pltpu.make_async_copy(buf.at[slot], outs[0].at[ds(chunk * CHUNK, CHUNK), :], sem.at[slot]))]
        if kind == "inner":
            return [(None, pltpu.make_async_copy(buf.at[slot], outs[0].at[:, ds(chunk * CHUNK, CHUNK)], sem.at[slot]))]
        rows = pl.ds(0, 2 * CHUNK) if len(halves) == 2 else ds((halves[0] ^ me[0]) * CHUNK, CHUNK)
        cols = ds((chunk % 2) * CHUNK, CHUNK)
        return [
            (chunk // 2 == m, pltpu.make_async_copy(buf.at[slot, rows], outs[m].at[rows, cols], sem.at[slot]))
            for m in range(4)
        ]

    def each(step, act):
        for cond, one in copies(step):
            if cond is None:
                act(one)
            else:
                pl.when(cond)(functools.partial(act, one))

    for step in range(8):
        slot = step % slots
        if step >= slots:
            each(step - slots, lambda one: one.wait())
        for half in halves:
            place = (half ^ me[0]) * CHUNK
            for n in range(colors):
                order, size, first = orders[n], sizes[n], sum(sizes[:n])
                at = per * n + (2 * half if len(halves) == 2 else 0) + bit(step, order[0])
                if at not in waited:
                    waited.add(at)
                    loads[at].wait()
                for t in range(2):
                    bits = [t if c == "b" else bit(step, c) for c in order]
                    where = bits[1] * 4 + bits[2] * 2 + bits[3]
                    start = (t ^ me[2]) * HALF + first
                    value = ins[at][where].astype(f32)
                    if kind == "outer":
                        buf[slot, ds(start, size, 16), ds(place, CHUNK)] = value
                    else:
                        buf[slot, ds(place + start, size, 16), :] = value
        each(step, lambda one: one.start())
    for step in range(8 - slots, 8):
        each(step, lambda one: one.wait())


def unpack(kind, pieces, orders, halves=(0, 1), into=()):
    colors = len(orders)
    width = 2 * CHUNK
    if kind == "outer":
        out_shape = [sd((8 * CHUNK, width), f32)]
    elif kind == "inner":
        out_shape = [sd((width, 8 * CHUNK), f32)]
    else:
        out_shape = [sd((width, width), f32)] * 4
    buf = (4, CHUNK, width) if kind == "outer" else (4, width, CHUNK)
    dma = pltpu.SemaphoreType.DMA
    return pl.pallas_call(
        functools.partial(unpack_kernel, kind, orders, halves),
        in_specs=[ANY] * len(pieces) + [HBM] * len(into),
        out_specs=[HBM] * len(out_shape),
        out_shape=out_shape,
        scratch_shapes=[pltpu.VMEM(v.shape, v.dtype) for v in pieces]
        + [pltpu.VMEM(buf, f32), dma((len(pieces),)), dma((4,))],
        compiler_params=params(26),
        cost_estimate=cost(4e9),
        name="unpack_" + kind,
        input_output_aliases={len(pieces) + n: n for n in range(len(into))},
    )(*pieces, *into)


SMALL_ROWS = (6, 7, 5, 3, 4, 8, 2, 0, 1)


def small_kernel(total, *outs):
    half = total.shape[1]
    for at, out in zip(SMALL_ROWS, outs):
        for n in range(out.shape[0] // half):
            line = at + n // 2 + (n % 2) * (total.shape[0] // 2)
            out[pl.ds(n * half, half)] = total[line : line + 1, :].reshape(half)


def small_call(total, ff):
    width = 2 * total.shape[1]
    sizes = [ff if at == 8 else width for at in SMALL_ROWS]
    return pl.pallas_call(
        small_kernel,
        in_specs=[VMEM],
        out_specs=[VMEM] * 9,
        out_shape=[sd((n,), f32) for n in sizes],
        compiler_params=params(4),
        cost_estimate=cost(1e9),
        name="vectors",
    )(total)


AXES = ("dp", "seq")
DP_BIT = {"x": 0, "y": 1, "a": 2, "b": 3}


def swap(value, name):
    dp = lax.axis_size("dp")
    seq = lax.axis_size("seq")
    flip = 1 if name == "c" else seq << (name if isinstance(name, int) else DP_BIT[name])
    return lax.ppermute(value, AXES, [(i, i ^ flip) for i in range(dp * seq)])


ORDERS = ("xyab", "yaxb", "axyb")


def pick(value, at, n):
    return lax.index_in_dim(value, n, at, keepdims=False)


def cut(value, sizes):
    return [value[..., sum(sizes[:n]) : sum(sizes[: n + 1]), :] for n in range(len(sizes))]


EVEN = (64, 64, 64)
LEAN = (80, 64, 48)


def reduction(keep, got, down=EVEN, up=EVEN):
    shape = (2, 2, 2, 2, HALF, CHUNK)
    keeps = cut(keep.reshape(shape), down)
    gots = cut(got.reshape(shape), down)
    dims = ["ayxb"] * 3
    for level in range(3):
        places = [d.index(o[level]) for d, o in zip(dims, ORDERS)]
        sends = [pick(k, at, 1) + pick(g, at, 1) for k, g, at in zip(keeps, gots, places)]
        keeps = [pick(k, at, 0) + pick(g, at, 0) for k, g, at in zip(keeps, gots, places)]
        dims = [d.replace(o[level], "") for d, o in zip(dims, ORDERS)]
        gots = yield [(o[level], v) for o, v in zip(ORDERS, sends)]
    own = jnp.concatenate([k + g for k, g in zip(keeps, gots)], -2)
    (got,) = yield [("b", own)]
    own = own + jnp.concatenate([got[1:], got[:1]])
    for extra in range(4, lax.axis_size("dp").bit_length() - 1):
        own = own + swap(own, extra)
    owns = cut(own, up)
    for level in (2, 1):
        gots = yield [(o[level], v) for o, v in zip(ORDERS, owns)]
        owns = [jnp.stack(v) for v in zip(owns, gots)]
    owns = [v.reshape((8,) + v.shape[-2:]) for v in owns]
    gots = yield [(o[0], v) for o, v in zip(ORDERS, owns)] + [("c", v) for v in owns]
    near, far = gots[:3], gots[3:]
    others = yield [("c", v) for v in near], (owns, near)
    return [v for four in zip(owns, near, far, others) for v in four]


def vector_sum(small):
    half = small.shape[1] // 2
    value = jnp.concatenate([small[:, :half], small[:, half:]])
    links = ["c"] + list("axyb") + list(range(4, lax.axis_size("dp").bit_length() - 1))
    for link in links:
        sent = value.astype(bf16)
        if isinstance(link, int):
            got = swap(sent, link)
        else:
            (got,) = yield [(link, sent)]
        value = sent.astype(f32) + got.astype(f32)
    return value


def unroll(v):
    return v.reshape((-1, v.shape[-1]))


class Rounds:
    def __init__(self):
        self.flows = {}
        self.results = {}
        self.parts = {}
        self.wanted = {}
        self.mark = ()

    def add(self, name, flow):
        self.flows[name] = flow
        self.wanted[name] = next(flow)

    def hold(self, value):
        return lax.optimization_barrier((value,) + self.mark)[0]

    def begin(self, extra=(), skip=()):
        self.order = [(name, n) for name in self.wanted if name not in skip for n in range(len(self.wanted[name]))]
        links = {}
        alone = {}
        for name, n in self.order:
            link, value = self.wanted[name][n]
            if link == "c":
                alone[name, n] = value
            else:
                links.setdefault(link, []).append((name, n))
        merged = {}
        for link, keys in links.items():
            values = [self.wanted[k][n][1] for k, n in keys]
            merged[link] = values[0] if len(values) == 1 else jnp.concatenate([unroll(v) for v in values])
        merged, alone, extra = lax.optimization_barrier((merged, alone, tuple(extra)))
        self.mark = tuple(merged.values())
        self.got = {}
        for link in "baxy":
            if link not in links:
                continue
            keys = links[link]
            got = swap(merged[link], link)
            if len(keys) == 1:
                self.got[keys[0]] = got
                continue
            row = 0
            for k, n in keys:
                shape = self.wanted[k][n][1].shape
                count = math.prod(shape[:-1])
                self.got[k, n] = got[row : row + count].reshape(shape)
                row += count
        for key, value in alone.items():
            self.got[key] = swap(value, "c")
        return [swap(v, "c") for v in extra]

    def end(self, *beside):
        got, _ = lax.optimization_barrier((self.got, tuple(beside)))
        for name in list(self.flows):
            if name not in self.wanted or (name, 0) not in got:
                continue
            values = [got[name, n] for n in range(len(self.wanted[name]))]
            try:
                wanted = self.flows[name].send(values)
                if isinstance(wanted, tuple):
                    wanted, self.parts[name] = wanted
                self.wanted[name] = wanted
            except StopIteration as stop:
                self.results[name] = stop.value
                del self.flows[name], self.wanted[name]


def body(chains_in, lengths, d_out, w_query, b_query, w_key, w_value, b_value, w_output, b_output, gain_one, shift_one,
         w_inner, b_inner, w_outer, b_outer, gain_two, shift_two):
    seqs, length, width = chains_in.shape
    rows = seqs * length
    place = lax.axis_index("dp") * 2 + lax.axis_index("seq")
    me = (place >> jnp.array([0, 1, 4], jnp.int32)) & jnp.array([1, 7, 1], jnp.int32)
    x = chains_in.reshape(rows, width)
    lse, small, q, k, v, mixed, xhat, rstd, fin, out, dffn, dpre, send_o, keep_o, send_i, keep_i = forward(
        lengths, me, (b_query, b_value, b_output, gain_one, shift_one, b_inner, b_outer, gain_two, shift_two),
        (x, w_query, w_key, w_value, w_output, w_inner, w_outer, d_out.reshape(rows, width)),
    )
    rounds = Rounds()
    got_o, got_i = rounds.begin([send_o, send_i])
    rounds.add("outer", reduction(keep_o, got_o))
    rounds.begin()
    small, dh1, dob, dm = mid_call(gain_one, small, rounds.hold(dpre), w_inner, (dffn, xhat, rstd, w_output))
    got_i, dm = lax.optimization_barrier((got_i, dm))
    rounds.end(dh1, dob, dm)
    rounds.add("inner", reduction(keep_i, got_i))
    rounds.begin()
    small, d, send, keep = att_call(lengths, me, small, (q, k, v, rounds.hold(dm), lse, x, mixed, dob))
    rounds.end(d, send)
    rounds.add("vectors", vector_sum(small))
    (got,) = rounds.begin([send])
    d_x = dx_call(rounds.hold(dh1), d, w_query, w_key, w_value)
    got, d_x = lax.optimization_barrier((got, d_x))
    rounds.end(got)
    rounds.add("attn", reduction(keep, got))
    for _ in range(4):
        rounds.begin()
        rounds.end()
    rounds.begin()
    vec = small_call(rounds.hold(rounds.results["vectors"]), w_inner.shape[1])
    rounds.end(vec[0])
    rounds.begin()
    (d_w_outer,) = unpack("outer", rounds.hold(rounds.results["outer"]), ORDERS)
    rounds.end(d_w_outer)
    rounds.begin()
    (d_w_inner,) = unpack("inner", rounds.hold(rounds.results["inner"]), ORDERS)
    rounds.end(d_w_inner)
    rounds.begin()
    owns, nears = rounds.hold(rounds.parts["attn"])
    grads = unpack("attn", [v for two in zip(owns, nears) for v in two], ORDERS, (0,))
    rounds.end()
    pieces = rounds.results["attn"]
    far = [v for n in range(3) for v in pieces[4 * n + 2 : 4 * n + 4]]
    d_w_query, d_w_key, d_w_value, d_w_output = unpack("attn", far, ORDERS, (1,), grads)
    return (
        out.reshape(seqs, length, width), d_x.reshape(seqs, length, width),
        d_w_query, vec[0], d_w_key, d_w_value, vec[1], d_w_output, vec[2], vec[3], vec[4],
        d_w_inner, vec[5], d_w_outer, vec[6], vec[7], vec[8],
    )


def solution(mesh):
    rows = P(AXES, None, None)
    return jax.shard_map(
        body, mesh=mesh, in_specs=(rows, P(AXES), rows) + (P(),) * 15, out_specs=(rows, rows) + (P(),) * 15, check_vma=False
    )
```
